8 devices in a mesh: data: 8 (over z, y, x, core).
Axes of the slice: x: 2, y: 2, z: 1, core: 2. Of those that a mesh axis runs over, the one named last changes fastest.
Arguments:
- x_in: bfloat16 [32, 128, 384], P('data')
- g_out: bfloat16 [32, 128, 384], P('data')
- step_emb: bfloat16 [6, 384], replicated
- w_q: bfloat16 [384, 6, 64], replicated
- w_k: bfloat16 [384, 6, 64], replicated
- w_v: bfloat16 [384, 6, 64], replicated
- w_o: bfloat16 [6, 64, 384], replicated
- w_up: bfloat16 [384, 1536], replicated
- w_down: bfloat16 [1536, 384], replicated
Outputs:
- output 1: float32 [384, 6, 64], replicated
- output 2: float32 [384, 6, 64], replicated
- output 3: float32 [384, 6, 64], replicated
- output 4: float32 [6, 64, 384], replicated
- output 5: float32 [384, 1536], replicated
- output 6: float32 [1536, 384], replicated
- output 7: bfloat16 [32, 128, 384], P('data')
All inputs are finite; a program needn't handle non-finite values.
Results may differ from the reference program's by a relative error of at most 0.02.
Values are sent between devices in bfloat16 or wider.
A program may use at most 1 GiB of HBM per device.

```python
import math
import functools
import jax
import jax.numpy as jnp
from jax import lax

D = 384
FF = 1536
HEADS = 6
SEQ = 128
LAYERS = 6
BATCH = 32
HEAD = D // HEADS
NORM_EPS = 1e-6


def setup_inputs(seed: int = 0) -> dict:
    sub_keys = jax.random.split(jax.random.key(seed), 9)
    out_gain = 2.0 / math.sqrt(LAYERS)
    x_in = jax.random.normal(sub_keys[0], (BATCH, SEQ, D), jnp.float32)
    g_out = jax.random.normal(sub_keys[1], (BATCH, SEQ, D), jnp.float32)
    step_emb = jax.random.normal(sub_keys[2], (LAYERS, D), jnp.float32) / math.sqrt(LAYERS)
    w_q = jax.random.normal(sub_keys[3], (D, HEADS, HEAD), jnp.float32) * D ** -0.5
    w_k = jax.random.normal(sub_keys[4], (D, HEADS, HEAD), jnp.float32) * D ** -0.5
    w_v = jax.random.normal(sub_keys[5], (D, HEADS, HEAD), jnp.float32) * D ** -0.5
    w_o = jax.random.normal(sub_keys[6], (HEADS, HEAD, D), jnp.float32) * (D ** -0.5 * out_gain)
    w_up = jax.random.normal(sub_keys[7], (D, FF), jnp.float32) * D ** -0.5
    w_down = jax.random.normal(sub_keys[8], (FF, D), jnp.float32) * (FF ** -0.5 * out_gain)
    return {
        'x_in': x_in.astype(jnp.bfloat16),
        'g_out': g_out.astype(jnp.bfloat16),
        'step_emb': step_emb.astype(jnp.bfloat16),
        'w_q': w_q.astype(jnp.bfloat16),
        'w_k': w_k.astype(jnp.bfloat16),
        'w_v': w_v.astype(jnp.bfloat16),
        'w_o': w_o.astype(jnp.bfloat16),
        'w_up': w_up.astype(jnp.bfloat16),
        'w_down': w_down.astype(jnp.bfloat16),
    }


def rms_norm(x_val):
    x_f32 = x_val.astype(jnp.float32)
    return (x_f32 * lax.rsqrt(jnp.mean(x_f32 * x_f32, axis=-1, keepdims=True) + NORM_EPS)).astype(jnp.bfloat16)


def shared_block(weight_set, x_prev, step_vec):
    w_q, w_k, w_v, w_o, w_up, w_down = weight_set
    x_cur = x_prev + step_vec
    u_norm = rms_norm(x_cur).astype(jnp.float32)
    q_heads = jnp.einsum('sd,dhe->she', u_norm, w_q).astype(jnp.bfloat16)
    k_heads = jnp.einsum('sd,dhe->she', u_norm, w_k).astype(jnp.bfloat16)
    v_heads = jnp.einsum('sd,dhe->she', u_norm, w_v).astype(jnp.bfloat16)
    scores = jnp.einsum('qhe,khe->hqk', q_heads.astype(jnp.float32), k_heads.astype(jnp.float32)).astype(jnp.bfloat16)
    prob_mat = jax.nn.softmax(scores.astype(jnp.float32) * HEAD ** -0.5, axis=-1).astype(jnp.bfloat16)
    mix_heads = jnp.einsum('hqk,khe->qhe', prob_mat.astype(jnp.float32), v_heads.astype(jnp.float32)).astype(jnp.bfloat16)
    attn_out = jnp.einsum('qhe,hed->qd', mix_heads.astype(jnp.float32), w_o).astype(jnp.bfloat16)
    h_mid = x_cur + attn_out
    m_norm = rms_norm(h_mid).astype(jnp.float32)
    z_up = jnp.dot(m_norm, w_up, preferred_element_type=jnp.float32).astype(jnp.bfloat16)
    g_act = jax.nn.gelu(z_up.astype(jnp.float32), approximate=True).astype(jnp.bfloat16)
    y_down = jnp.dot(g_act.astype(jnp.float32), w_down, preferred_element_type=jnp.float32).astype(jnp.bfloat16)
    return h_mid + y_down


def run_stack(weight_set, x_seq, step_emb):
    def layer_step(x_cur, step_vec):
        return jax.checkpoint(shared_block)(weight_set, x_cur, step_vec), None
    x_out, unused = lax.scan(layer_step, x_seq, step_emb)
    return x_out


def reference(x_in, g_out, step_emb, w_q, w_k, w_v, w_o, w_up, w_down):
    weight_set = tuple(w.astype(jnp.float32) for w in (w_q, w_k, w_v, w_o, w_up, w_down))

    def seq_grads(grad_acc, seq_pair):
        x_seq, g_seq = seq_pair
        x_out, pull_back = jax.vjp(functools.partial(run_stack, step_emb=step_emb), weight_set, x_seq)
        d_weights, d_x = pull_back(g_seq)
        return tuple(a + b for a, b in zip(grad_acc, d_weights)), d_x

    zero_acc = tuple(jnp.zeros_like(w) for w in weight_set)
    grad_sums, grad_x = lax.scan(seq_grads, zero_acc, (x_in, g_out))
    return (grad_sums[0], grad_sums[1], grad_sums[2], grad_sums[3], grad_sums[4], grad_sums[5], grad_x)
```

```python
import functools
import math

import jax
import jax.numpy as jnp
from jax import lax
from jax.experimental import pallas as pl
from jax.experimental.pallas import tpu as pltpu
from jax.sharding import PartitionSpec as P

EPS = 1e-6
F32 = jnp.float32
BF16 = jnp.bfloat16
LOG2E = math.log2(math.e)
GC0 = math.sqrt(2.0 / math.pi)
GC1 = GC0 * 0.044715
NT = (((1,), (1,)), ((), ()))
TN = (((0,), (0,)), ((), ()))


def mm(a, b):
    return jnp.dot(a, b, preferred_element_type=F32)


def mmg(a, b, dims):
    return lax.dot_general(a, b, dims, preferred_element_type=F32)


def blocks(total, size):
    return [(s, min(size, total - s)) for s in range(0, total, size)]


def rms_scale(xf):
    return lax.rsqrt(jnp.mean(xf * xf, axis=-1, keepdims=True) + EPS)


def norm_back(xf, r, dy):
    inner = jnp.mean(xf * dy, axis=-1, keepdims=True)
    return dy * r - xf * (r * r * r * inner)


def block_kernel(n_seq, seq, n_layers, n_heads,
                 x_ref, g_ref, emb_ref, wq_ref, wk_ref, wv_ref, wo_ref, wup_ref, wdn_ref,
                 gq_ref, gk_ref, gv_ref, go_ref, gup_ref, gdn_ref, dx_ref,
                 wqkv_s, wqkvt_s, wot_s, wupt_s, wdnt_s,
                 x_s, qkv_s, p_s, mix_s, h_s, z_s,
                 u_s, g_s, dup_s, dn_s, dmix_s, dqkv_s, d_s, dmid_s):
    tok, dm = d_s.shape
    ff = wup_ref.shape[1]
    hd = dm // n_heads
    pw = 2 * hd
    n_pair = n_heads // 2
    scale = hd ** -0.5
    RB = 64
    NB = 256
    rows = blocks(tok, RB)

    for i, w in enumerate((wq_ref, wk_ref, wv_ref)):
        wt = w[...]
        wqkvt_s[i * dm:(i + 1) * dm, :] = wt
        wqkv_s[:, i * dm:(i + 1) * dm] = wt.T
    wot_s[...] = wo_ref[...].T
    wupt_s[...] = wup_ref[...].T
    wdnt_s[...] = wdn_ref[...].T
    for ref in (gq_ref, gk_ref, gv_ref, go_ref, gup_ref, gdn_ref):
        ref[...] = jnp.zeros(ref.shape, F32)

    low = lax.broadcasted_iota(jnp.int32, (seq, pw), 1) < hd

    def stack(a):
        zero = jnp.zeros_like(a)
        return jnp.concatenate([jnp.where(low, a, zero), jnp.where(low, zero, a)], axis=0)

    def halves(a):
        return a[:, :seq], a[:, seq:]

    d_s[...] = x_ref[...]

    def fwd(l, carry):
        emb = emb_ref[l]
        for r0, rn in rows:
            rs = slice(r0, r0 + rn)
            xb = (d_s[rs, :].astype(F32) + emb).astype(BF16)
            x_s[l, rs, :] = xb
            xf = xb.astype(F32)
            u_s[rs, :] = (xf * rms_scale(xf)).astype(BF16)
        for n0, nn in blocks(3 * dm, NB):
            ns = slice(n0, n0 + nn)
            qkv_s[l, :, ns] = mm(u_s[...], wqkv_s[:, ns]).astype(BF16)
        for s in range(n_seq):
            rs = slice(s * seq, (s + 1) * seq)
            for j in range(n_pair):
                c = j * pw
                q = qkv_s[l, rs, c:c + pw]
                k = stack(qkv_s[l, rs, dm + c:dm + c + pw])
                v = stack(qkv_s[l, rs, 2 * dm + c:2 * dm + c + pw])
                sc = mmg(q, k, NT).astype(BF16).astype(F32)
                ps = []
                for half in halves(sc):
                    top = jnp.max(half, axis=-1, keepdims=True)
                    e = jnp.exp2((half - top) * (scale * LOG2E))
                    ps.append(e * (1.0 / jnp.sum(e, axis=-1, keepdims=True)))
                p = jnp.concatenate(ps, axis=1)
                p_s[l, s * n_pair + j] = p
                mix_s[l, rs, c:c + pw] = mm(p.astype(BF16), v).astype(BF16)
        for n0, nn in blocks(dm, NB):
            ns = slice(n0, n0 + nn)
            o = mm(mix_s[l], wo_ref[:, ns]).astype(BF16)
            h_s[l, :, ns] = (x_s[l, :, ns].astype(F32) + o.astype(F32)).astype(BF16)
        for r0, rn in rows:
            rs = slice(r0, r0 + rn)
            hf = h_s[l, rs, :].astype(F32)
            u_s[rs, :] = (hf * rms_scale(hf)).astype(BF16)
        for n0, nn in blocks(ff, NB):
            ns = slice(n0, n0 + nn)
            zb = mm(u_s[...], wup_ref[:, ns]).astype(BF16)
            z_s[l, :, ns] = zb
            for r0, rn in rows:
                z = zb[r0:r0 + rn].astype(F32)
                t = jnp.tanh(z * (GC0 + GC1 * (z * z)))
                hz = 0.5 * z
                g_s[r0:r0 + rn, ns] = (hz + hz * t).astype(BF16)
        for n0, nn in blocks(dm, NB):
            ns = slice(n0, n0 + nn)
            y = mm(g_s[...], wdn_ref[:, ns]).astype(BF16)
            d_s[:, ns] = (h_s[l, :, ns].astype(F32) + y.astype(F32)).astype(BF16)
        return carry

    lax.fori_loop(0, n_layers, fwd, 0)
    d_s[...] = g_ref[...]

    def bwd(i, carry):
        l = n_layers - 1 - i
        for n0, nn in blocks(ff, NB):
            ns = slice(n0, n0 + nn)
            da = mm(d_s[...], wdnt_s[:, ns]).astype(BF16)
            for r0, rn in rows:
                rs = slice(r0, r0 + rn)
                z = z_s[l, rs, ns].astype(F32)
                z2 = z * z
                t = jnp.tanh(z * (GC0 + GC1 * z2))
                hz = 0.5 * z
                g_s[rs, ns] = (hz + hz * t).astype(BF16)
                dg = (0.5 + 0.5 * t) + hz * (1.0 - t * t) * (GC0 + 3.0 * GC1 * z2)
                dup_s[rs, ns] = (da[rs].astype(F32) * dg).astype(BF16)
        for n0, nn in blocks(ff, NB):
            gdn_ref[n0:n0 + nn, :] += mmg(g_s[:, n0:n0 + nn], d_s[...], TN)
        for n0, nn in blocks(dm, NB):
            ns = slice(n0, n0 + nn)
            dn_s[:, ns] = mm(dup_s[...], wupt_s[:, ns]).astype(BF16)
        for r0, rn in rows:
            rs = slice(r0, r0 + rn)
            hf = h_s[l, rs, :].astype(F32)
            r = rms_scale(hf)
            u_s[rs, :] = (hf * r).astype(BF16)
            dh = norm_back(hf, r, dn_s[rs, :].astype(F32)).astype(BF16)
            dmid_s[rs, :] = (d_s[rs, :].astype(F32) + dh.astype(F32)).astype(BF16)
        for n0, nn in blocks(ff, NB):
            ns = slice(n0, n0 + nn)
            gup_ref[:, ns] += mmg(u_s[...], dup_s[:, ns], TN)
        for n0, nn in blocks(dm, NB):
            ns = slice(n0, n0 + nn)
            dmix_s[:, ns] = mm(dmid_s[...], wot_s[:, ns]).astype(BF16)
        go_ref[...] += mmg(mix_s[l], dmid_s[...], TN)
        for s in range(n_seq):
            rs = slice(s * seq, (s + 1) * seq)
            for j in range(n_pair):
                c = j * pw
                q = stack(qkv_s[l, rs, c:c + pw])
                k = stack(qkv_s[l, rs, dm + c:dm + c + pw])
                v = stack(qkv_s[l, rs, 2 * dm + c:2 * dm + c + pw])
                dmx = dmix_s[rs, c:c + pw]
                p = p_s[l, s * n_pair + j]
                dp = mmg(dmx, v, NT).astype(BF16).astype(F32)
                dss = []
                for ph, dph in zip(halves(p), halves(dp)):
                    inner = jnp.sum(ph * dph, axis=-1, keepdims=True)
                    dss.append((ph * (dph - inner) * scale).astype(BF16))
                ds = jnp.concatenate(dss, axis=1)
                dst = jnp.concatenate(dss, axis=0)
                pst = jnp.concatenate([a.astype(BF16) for a in halves(p)], axis=0)
                dqkv_s[rs, c:c + pw] = mm(ds, k).astype(BF16)
                dqkv_s[rs, dm + c:dm + c + pw] = mmg(dst, q, TN).astype(BF16)
                dqkv_s[rs, 2 * dm + c:2 * dm + c + pw] = mmg(pst, stack(dmx), TN).astype(BF16)
        for n0, nn in blocks(dm, NB):
            ns = slice(n0, n0 + nn)
            dn_s[:, ns] = mm(dqkv_s[...], wqkvt_s[:, ns]).astype(BF16)
        for r0, rn in rows:
            rs = slice(r0, r0 + rn)
            xf = x_s[l, rs, :].astype(F32)
            r = rms_scale(xf)
            u_s[rs, :] = (xf * r).astype(BF16)
            dh = norm_back(xf, r, dn_s[rs, :].astype(F32)).astype(BF16)
            d_s[rs, :] = (dmid_s[rs, :].astype(F32) + dh.astype(F32)).astype(BF16)
        for i3, ref in enumerate((gq_ref, gk_ref, gv_ref)):
            ref[...] += mmg(dqkv_s[:, i3 * dm:(i3 + 1) * dm], u_s[...], TN)
        return carry

    lax.fori_loop(0, n_layers, bwd, 0)
    dx_ref[...] = d_s[...]


def solution(mesh):
    batch_spec = P('data', None, None)

    def per_device(x_loc, g_loc, step_emb, w_q, w_k, w_v, w_o, w_up, w_down):
        n_seq, seq, dm = x_loc.shape
        n_layers = step_emb.shape[0]
        n_heads, hd = w_q.shape[1:]
        ff = w_up.shape[1]
        tok = n_seq * seq
        n_pair = n_heads // 2
        wts = [w.transpose(1, 2, 0).reshape(n_heads * hd, dm) for w in (w_q, w_k, w_v)]
        vm = pl.BlockSpec(memory_space=pltpu.VMEM)
        sq = jax.ShapeDtypeStruct((dm, dm), F32)
        outs = pl.pallas_call(
            functools.partial(block_kernel, n_seq, seq, n_layers, n_heads),
            out_shape=(sq, sq, sq, sq, jax.ShapeDtypeStruct((dm, ff), F32), jax.ShapeDtypeStruct((ff, dm), F32),
                       jax.ShapeDtypeStruct((tok, dm), BF16)),
            in_specs=[vm] * 9,
            out_specs=[vm] * 7,
            scratch_shapes=[
                pltpu.VMEM((dm, 3 * dm), BF16),
                pltpu.VMEM((3 * dm, dm), BF16),
                pltpu.VMEM((dm, dm), BF16),
                pltpu.VMEM((ff, dm), BF16),
                pltpu.VMEM((dm, ff), BF16),
                pltpu.VMEM((n_layers, tok, dm), BF16),
                pltpu.VMEM((n_layers, tok, 3 * dm), BF16),
                pltpu.VMEM((n_layers, n_seq * n_pair, seq, 2 * seq), F32),
                pltpu.VMEM((n_layers, tok, dm), BF16),
                pltpu.VMEM((n_layers, tok, dm), BF16),
                pltpu.VMEM((n_layers, tok, ff), BF16),
                pltpu.VMEM((tok, dm), BF16),
                pltpu.VMEM((tok, ff), BF16),
                pltpu.VMEM((tok, ff), BF16),
                pltpu.VMEM((tok, dm), BF16),
                pltpu.VMEM((tok, dm), BF16),
                pltpu.VMEM((tok, 3 * dm), BF16),
                pltpu.VMEM((tok, dm), BF16),
                pltpu.VMEM((tok, dm), BF16),
            ],
            compiler_params=pltpu.CompilerParams(vmem_limit_bytes=67043328),
        )(x_loc.reshape(tok, dm), g_loc.reshape(tok, dm), step_emb.astype(F32)[:, None, :],
          *wts, w_o.reshape(n_heads * hd, dm), w_up, w_down)
        sums = lax.psum(tuple(outs[:6]), 'data')
        heads = [a.reshape(n_heads, hd, dm).transpose(2, 0, 1) for a in sums[:3]]
        return (*heads, sums[3].reshape(n_heads, hd, dm), sums[4], sums[5], outs[6].reshape(n_seq, seq, dm))

    return jax.shard_map(per_device, mesh=mesh, in_specs=(batch_spec, batch_spec, P(), P(), P(), P(), P(), P(), P()), out_specs=(P(), P(), P(), P(), P(), P(), batch_spec), check_vma=False)
```

```python
import functools
import math

import jax
import jax.numpy as jnp
from jax import lax
from jax.experimental import pallas as pl
from jax.experimental.pallas import tpu as pltpu
from jax.sharding import PartitionSpec as P

EPS = 1e-6
F32 = jnp.float32
BF16 = jnp.bfloat16
MESH = pl.DeviceIdType.MESH
LOG2E = math.log2(math.e)
GC0 = math.sqrt(2.0 / math.pi)
GC1 = GC0 * 0.044715
NT = (((1,), (1,)), ((), ()))
TN = (((0,), (0,)), ((), ()))


def mm(a, b):
    return jnp.dot(a, b, preferred_element_type=F32)


def mmg(a, b, dims):
    return lax.dot_general(a, b, dims, preferred_element_type=F32)


def blocks(total, size):
    return [(s, min(size, total - s)) for s in range(0, total, size)]


def rms_scale(xf):
    return lax.rsqrt(jnp.mean(xf * xf, axis=-1, keepdims=True) + EPS)


def norm_back(xf, r, dy):
    inner = jnp.mean(xf * dy, axis=-1, keepdims=True)
    return dy * r - xf * (r * r * r * inner)


def block_kernel(n_seq, seq, n_layers, n_heads,
                 x_ref, g_ref, emb_ref, wq_ref, wk_ref, wv_ref, wo_ref, wup_ref, wdn_ref,
                 gq_ref, gk_ref, gv_ref, go_ref, gup_ref, gdn_ref, dx_ref,
                 wqkv_s, wqkvt_s, wot_s, wupt_s, wdnt_s,
                 x_s, qkv_s, p_s, mix_s, h_s, z_s,
                 u_s, g_s, dup_s, dn_s, dmix_s, dqkv_s, d_s, dmid_s):
    tok, dm = d_s.shape
    ff = wup_ref.shape[1]
    hd = dm // n_heads
    pw = 2 * hd
    n_pair = n_heads // 2
    scale = hd ** -0.5
    RB = 64
    NB = 256
    rows = blocks(tok, RB)

    for i, w in enumerate((wq_ref, wk_ref, wv_ref)):
        wt = w[...]
        wqkvt_s[i * dm:(i + 1) * dm, :] = wt
        wqkv_s[:, i * dm:(i + 1) * dm] = wt.T
    wot_s[...] = wo_ref[...].T
    wupt_s[...] = wup_ref[...].T
    wdnt_s[...] = wdn_ref[...].T
    for ref in (gq_ref, gk_ref, gv_ref, go_ref, gup_ref, gdn_ref):
        ref[...] = jnp.zeros(ref.shape, F32)

    low = lax.broadcasted_iota(jnp.int32, (seq, pw), 1) < hd

    def stack(a):
        zero = jnp.zeros_like(a)
        return jnp.concatenate([jnp.where(low, a, zero), jnp.where(low, zero, a)], axis=0)

    def halves(a):
        return a[:, :seq], a[:, seq:]

    d_s[...] = x_ref[...]

    def fwd(l, carry):
        emb = emb_ref[l]
        for r0, rn in rows:
            rs = slice(r0, r0 + rn)
            xb = (d_s[rs, :].astype(F32) + emb).astype(BF16)
            x_s[l, rs, :] = xb
            xf = xb.astype(F32)
            u_s[rs, :] = (xf * rms_scale(xf)).astype(BF16)
        for n0, nn in blocks(3 * dm, NB):
            ns = slice(n0, n0 + nn)
            qkv_s[l, :, ns] = mm(u_s[...], wqkv_s[:, ns]).astype(BF16)
        for s in range(n_seq):
            rs = slice(s * seq, (s + 1) * seq)
            for j in range(n_pair):
                c = j * pw
                q = qkv_s[l, rs, c:c + pw]
                k = stack(qkv_s[l, rs, dm + c:dm + c + pw])
                v = stack(qkv_s[l, rs, 2 * dm + c:2 * dm + c + pw])
                sc = mmg(q, k, NT).astype(BF16).astype(F32)
                ps = []
                for half in halves(sc):
                    top = jnp.max(half, axis=-1, keepdims=True)
                    e = jnp.exp2((half - top) * (scale * LOG2E))
                    ps.append(e * (1.0 / jnp.sum(e, axis=-1, keepdims=True)))
                p = jnp.concatenate(ps, axis=1)
                p_s[l, s * n_pair + j] = p
                mix_s[l, rs, c:c + pw] = mm(p.astype(BF16), v).astype(BF16)
        for n0, nn in blocks(dm, NB):
            ns = slice(n0, n0 + nn)
            o = mm(mix_s[l], wo_ref[:, ns]).astype(BF16)
            h_s[l, :, ns] = (x_s[l, :, ns].astype(F32) + o.astype(F32)).astype(BF16)
        for r0, rn in rows:
            rs = slice(r0, r0 + rn)
            hf = h_s[l, rs, :].astype(F32)
            u_s[rs, :] = (hf * rms_scale(hf)).astype(BF16)
        for n0, nn in blocks(ff, NB):
            ns = slice(n0, n0 + nn)
            zb = mm(u_s[...], wup_ref[:, ns]).astype(BF16)
            z_s[l, :, ns] = zb
            for r0, rn in rows:
                z = zb[r0:r0 + rn].astype(F32)
                t = jnp.tanh(z * (GC0 + GC1 * (z * z)))
                hz = 0.5 * z
                g_s[r0:r0 + rn, ns] = (hz + hz * t).astype(BF16)
        for n0, nn in blocks(dm, NB):
            ns = slice(n0, n0 + nn)
            y = mm(g_s[...], wdn_ref[:, ns]).astype(BF16)
            d_s[:, ns] = (h_s[l, :, ns].astype(F32) + y.astype(F32)).astype(BF16)
        return carry

    lax.fori_loop(0, n_layers, fwd, 0)
    d_s[...] = g_ref[...]

    def bwd(i, carry):
        l = n_layers - 1 - i
        for n0, nn in blocks(ff, NB):
            ns = slice(n0, n0 + nn)
            da = mm(d_s[...], wdnt_s[:, ns]).astype(BF16)
            for r0, rn in rows:
                rs = slice(r0, r0 + rn)
                z = z_s[l, rs, ns].astype(F32)
                z2 = z * z
                t = jnp.tanh(z * (GC0 + GC1 * z2))
                hz = 0.5 * z
                g_s[rs, ns] = (hz + hz * t).astype(BF16)
                dg = (0.5 + 0.5 * t) + hz * (1.0 - t * t) * (GC0 + 3.0 * GC1 * z2)
                dup_s[rs, ns] = (da[rs].astype(F32) * dg).astype(BF16)
        for n0, nn in blocks(ff, NB):
            gdn_ref[n0:n0 + nn, :] += mmg(g_s[:, n0:n0 + nn], d_s[...], TN)
        for n0, nn in blocks(dm, NB):
            ns = slice(n0, n0 + nn)
            dn_s[:, ns] = mm(dup_s[...], wupt_s[:, ns]).astype(BF16)
        for r0, rn in rows:
            rs = slice(r0, r0 + rn)
            hf = h_s[l, rs, :].astype(F32)
            r = rms_scale(hf)
            u_s[rs, :] = (hf * r).astype(BF16)
            dh = norm_back(hf, r, dn_s[rs, :].astype(F32)).astype(BF16)
            dmid_s[rs, :] = (d_s[rs, :].astype(F32) + dh.astype(F32)).astype(BF16)
        for n0, nn in blocks(ff, NB):
            ns = slice(n0, n0 + nn)
            gup_ref[:, ns] += mmg(u_s[...], dup_s[:, ns], TN)
        for n0, nn in blocks(dm, NB):
            ns = slice(n0, n0 + nn)
            dmix_s[:, ns] = mm(dmid_s[...], wot_s[:, ns]).astype(BF16)
        go_ref[...] += mmg(mix_s[l], dmid_s[...], TN)
        for s in range(n_seq):
            rs = slice(s * seq, (s + 1) * seq)
            for j in range(n_pair):
                c = j * pw
                q = stack(qkv_s[l, rs, c:c + pw])
                k = stack(qkv_s[l, rs, dm + c:dm + c + pw])
                v = stack(qkv_s[l, rs, 2 * dm + c:2 * dm + c + pw])
                dmx = dmix_s[rs, c:c + pw]
                p = p_s[l, s * n_pair + j]
                dp = mmg(dmx, v, NT).astype(BF16).astype(F32)
                dss = []
                for ph, dph in zip(halves(p), halves(dp)):
                    inner = jnp.sum(ph * dph, axis=-1, keepdims=True)
                    dss.append((ph * (dph - inner) * scale).astype(BF16))
                ds = jnp.concatenate(dss, axis=1)
                dst = jnp.concatenate(dss, axis=0)
                pst = jnp.concatenate([a.astype(BF16) for a in halves(p)], axis=0)
                dqkv_s[rs, c:c + pw] = mm(ds, k).astype(BF16)
                dqkv_s[rs, dm + c:dm + c + pw] = mmg(dst, q, TN).astype(BF16)
                dqkv_s[rs, 2 * dm + c:2 * dm + c + pw] = mmg(pst, stack(dmx), TN).astype(BF16)
        for n0, nn in blocks(dm, NB):
            ns = slice(n0, n0 + nn)
            dn_s[:, ns] = mm(dqkv_s[...], wqkvt_s[:, ns]).astype(BF16)
        for r0, rn in rows:
            rs = slice(r0, r0 + rn)
            xf = x_s[l, rs, :].astype(F32)
            r = rms_scale(xf)
            u_s[rs, :] = (xf * r).astype(BF16)
            dh = norm_back(xf, r, dn_s[rs, :].astype(F32)).astype(BF16)
            d_s[rs, :] = (dmid_s[rs, :].astype(F32) + dh.astype(F32)).astype(BF16)
        for i3, ref in enumerate((gq_ref, gk_ref, gv_ref)):
            ref[...] += mmg(dqkv_s[:, i3 * dm:(i3 + 1) * dm], u_s[...], TN)
        return carry

    lax.fori_loop(0, n_layers, bwd, 0)
    dx_ref[...] = d_s[...]


def reduce_kernel(n_chunk, gq_ref, gk_ref, gv_ref, go_ref, gup_ref, gdn_ref,
                  oq_ref, ok_ref, ov_ref, oo_ref, oup_ref, odn_ref,
                  acc, r0, ra, rb, ra2, rb2, in_sem, out_sem, ssem, rsem, free_sem):
    dm = acc.shape[1]
    me = lax.axis_index('data')
    c = lax.rem(me, 2)
    x = lax.rem(lax.div(me, 2), 2)
    y = lax.div(me, 4)
    cp = me + 1 - 2 * c
    xp = me + 2 - 4 * x
    yp = me + 4 - 8 * y

    def views(dn, up, o, q, k, v):
        n = dn.shape[0] // dm
        return ([dn.at[i * dm:(i + 1) * dm, :] for i in range(n)]
                + [up.at[:, i * dm:(i + 1) * dm] for i in range(n)] + [o, q, k, v])

    ins = views(gdn_ref, gup_ref, go_ref, gq_ref, gk_ref, gv_ref)
    outs = views(odn_ref, oup_ref, oo_ref, oq_ref, ok_ref, ov_ref)
    loads = [pltpu.make_async_copy(src, acc.at[i], in_sem.at[i]) for i, src in enumerate(ins)]
    for ld in loads:
        ld.start()

    barrier = pltpu.get_barrier_semaphore()
    for p in (cp, xp, yp):
        pl.semaphore_signal(barrier, inc=1, device_id=(p,), device_id_type=MESH)
    pl.semaphore_wait(barrier, 3)

    h0, h1, h2, h3 = dm // 2, dm // 4, dm // 8, dm // 16
    own = c * h0
    oth = (1 - c) * h0
    a0, a0n = own + x * h2, own + (1 - x) * h2
    b0, b0n = own + h1 + y * h2, own + h1 + (1 - y) * h2
    a1, a1n = a0 + y * h3, a0 + (1 - y) * h3
    b1, b1n = b0 + x * h3, b0 + (1 - x) * h3

    def part(k, off, n):
        return acc.at[k, pl.ds(pl.multiple_of(off, 8), n), :]

    def send(j, src, dst, dev):
        def at(k):
            return pltpu.make_async_remote_copy(
                src_ref=src(k), dst_ref=dst(k), send_sem=ssem.at[j, k], recv_sem=rsem.at[j, k],
                device_id=(dev,), device_id_type=MESH)
        return at

    def rows_of(off, n):
        return lambda k: part(k, off, n)

    def slot(ref, n):
        return lambda k: ref.at[k, 0:n, :]

    cs = [
        send(0, rows_of(oth, h0), slot(r0, h0), cp),
        send(1, rows_of(a0n, h2), slot(ra, h2), xp),
        send(2, rows_of(b0n, h2), slot(rb, h2), yp),
        send(3, rows_of(a1n, h3), slot(ra2, h3), yp),
        send(4, rows_of(b1n, h3), slot(rb2, h3), xp),
        send(5, rows_of(a1, h3), slot(ra, h3), yp),
        send(6, rows_of(b1, h3), slot(rb, h3), xp),
        send(7, rows_of(a1, h3), rows_of(a1, h3), xp),
        send(8, rows_of(b1, h3), rows_of(b1, h3), yp),
        send(9, slot(ra, h3), rows_of(a1n, h3), xp),
        send(10, slot(rb, h3), rows_of(b1n, h3), yp),
        send(11, rows_of(own, h0), rows_of(own, h0), cp),
    ]

    def add(k, off, n, src):
        sl = pl.ds(pl.multiple_of(off, 8), n)
        acc[k, sl, :] = acc[k, sl, :] + src[k]

    def loop(fn):
        lax.fori_loop(0, n_chunk, lambda k, t: (fn(k), t)[1], 0)

    for i, ld in enumerate(loads):
        ld.wait()
        cs[0](i).start()

    def s1(k):
        cs[0](k).wait_recv()
        add(k, own, h0, r0)
        cs[1](k).start()
        cs[2](k).start()

    def s2(k):
        cs[1](k).wait()
        add(k, a0, h2, ra)
        cs[2](k).wait()
        add(k, b0, h2, rb)
        cs[3](k).start()
        cs[4](k).start()

    def g2(k):
        cs[3](k).wait_recv()
        add(k, a1, h3, ra2)
        cs[4](k).wait_recv()
        add(k, b1, h3, rb2)
        for j in (5, 6, 7, 8):
            cs[j](k).start()

    def g1(k):
        cs[5](k).wait_recv()
        cs[9](k).start()
        cs[6](k).wait_recv()
        cs[10](k).start()
        cs[3](k).wait_send()
        acc[k, pl.ds(pl.multiple_of(a1n, 8), h3), :] = ra[k, 0:h3, :]
        cs[4](k).wait_send()
        acc[k, pl.ds(pl.multiple_of(b1n, 8), h3), :] = rb[k, 0:h3, :]

    def g0(k):
        for j in (7, 8, 9, 10):
            cs[j](k).wait_recv()
        cs[11](k).start()

    loop(s1)
    loop(s2)
    loop(lambda k: cs[0](k).wait_send())
    pl.semaphore_signal(free_sem, inc=1, device_id=(cp,), device_id_type=MESH)
    loop(g2)
    loop(g1)
    pl.semaphore_wait(free_sem, 1)
    loop(g0)
    stores = [pltpu.make_async_copy(acc.at[i], dst, out_sem.at[i]) for i, dst in enumerate(outs)]
    for i, st in enumerate(stores):
        cs[11](i).wait_recv()
        st.start()

    def finish(k):
        for j in range(5, 12):
            cs[j](k).wait_send()

    loop(finish)
    for st in stores:
        st.wait()


def all_reduce(grads):
    dm, ff = grads[4].shape
    n_chunk = 4 + 2 * (ff // dm)
    anyspec = pl.BlockSpec(memory_space=pl.ANY)
    return pl.pallas_call(
        functools.partial(reduce_kernel, n_chunk),
        out_shape=tuple(jax.ShapeDtypeStruct(g.shape, F32) for g in grads),
        in_specs=[anyspec] * 6,
        out_specs=[anyspec] * 6,
        scratch_shapes=[
            pltpu.VMEM((n_chunk, dm, dm), F32),
            pltpu.VMEM((n_chunk, dm // 2, dm), F32),
            pltpu.VMEM((n_chunk, dm // 8, dm), F32),
            pltpu.VMEM((n_chunk, dm // 8, dm), F32),
            pltpu.VMEM((n_chunk, dm // 16, dm), F32),
            pltpu.VMEM((n_chunk, dm // 16, dm), F32),
            pltpu.SemaphoreType.DMA((n_chunk,)),
            pltpu.SemaphoreType.DMA((n_chunk,)),
            pltpu.SemaphoreType.DMA((12, n_chunk)),
            pltpu.SemaphoreType.DMA((12, n_chunk)),
            pltpu.SemaphoreType.REGULAR,
        ],
        compiler_params=pltpu.CompilerParams(collective_id=0, has_side_effects=True, vmem_limit_bytes=40 * 2 ** 20),
    )(*grads)


def solution(mesh):
    batch_spec = P('data', None, None)

    def per_device(x_loc, g_loc, step_emb, w_q, w_k, w_v, w_o, w_up, w_down):
        n_seq, seq, dm = x_loc.shape
        n_layers = step_emb.shape[0]
        n_heads, hd = w_q.shape[1:]
        ff = w_up.shape[1]
        tok = n_seq * seq
        n_pair = n_heads // 2
        wts = [w.transpose(1, 2, 0).reshape(n_heads * hd, dm) for w in (w_q, w_k, w_v)]
        vm = pl.BlockSpec(memory_space=pltpu.VMEM)
        sq = jax.ShapeDtypeStruct((dm, dm), F32)
        outs = pl.pallas_call(
            functools.partial(block_kernel, n_seq, seq, n_layers, n_heads),
            out_shape=(sq, sq, sq, sq, jax.ShapeDtypeStruct((dm, ff), F32), jax.ShapeDtypeStruct((ff, dm), F32),
                       jax.ShapeDtypeStruct((tok, dm), BF16)),
            in_specs=[vm] * 9,
            out_specs=[vm] * 7,
            scratch_shapes=[
                pltpu.VMEM((dm, 3 * dm), BF16),
                pltpu.VMEM((3 * dm, dm), BF16),
                pltpu.VMEM((dm, dm), BF16),
                pltpu.VMEM((ff, dm), BF16),
                pltpu.VMEM((dm, ff), BF16),
                pltpu.VMEM((n_layers, tok, dm), BF16),
                pltpu.VMEM((n_layers, tok, 3 * dm), BF16),
                pltpu.VMEM((n_layers, n_seq * n_pair, seq, 2 * seq), F32),
                pltpu.VMEM((n_layers, tok, dm), BF16),
                pltpu.VMEM((n_layers, tok, dm), BF16),
                pltpu.VMEM((n_layers, tok, ff), BF16),
                pltpu.VMEM((tok, dm), BF16),
                pltpu.VMEM((tok, ff), BF16),
                pltpu.VMEM((tok, ff), BF16),
                pltpu.VMEM((tok, dm), BF16),
                pltpu.VMEM((tok, dm), BF16),
                pltpu.VMEM((tok, 3 * dm), BF16),
                pltpu.VMEM((tok, dm), BF16),
                pltpu.VMEM((tok, dm), BF16),
            ],
            compiler_params=pltpu.CompilerParams(vmem_limit_bytes=67043328),
        )(x_loc.reshape(tok, dm), g_loc.reshape(tok, dm), step_emb.astype(F32)[:, None, :],
          *wts, w_o.reshape(n_heads * hd, dm), w_up, w_down)
        sums = all_reduce(tuple(outs[:6]))
        heads = [a.reshape(n_heads, hd, dm).transpose(2, 0, 1) for a in sums[:3]]
        return (*heads, sums[3].reshape(n_heads, hd, dm), sums[4], sums[5], outs[6].reshape(n_seq, seq, dm))

    return jax.shard_map(per_device, mesh=mesh, in_specs=(batch_spec, batch_spec, P(), P(), P(), P(), P(), P(), P()), out_specs=(P(), P(), P(), P(), P(), P(), batch_spec), check_vma=False)
```

```python
import functools
import math

import jax
import jax.numpy as jnp
from jax import lax
from jax.experimental import pallas as pl
from jax.experimental.pallas import tpu as pltpu
from jax.sharding import PartitionSpec as P

EPS = 1e-6
F32 = jnp.float32
BF16 = jnp.bfloat16
MESH = pl.DeviceIdType.MESH
LOG2E = math.log2(math.e)
GC0 = math.sqrt(2.0 / math.pi)
GC1 = GC0 * 0.044715
NT = (((1,), (1,)), ((), ()))
TN = (((0,), (0,)), ((), ()))
VMEM_LIMIT = 58851328


def mm(a, b):
    return jnp.dot(a, b, preferred_element_type=F32)


def mmg(a, b, dims):
    return lax.dot_general(a, b, dims, preferred_element_type=F32)


def blocks(total, size):
    return [(s, min(size, total - s)) for s in range(0, total, size)]


def rms_scale(xf):
    return lax.rsqrt(jnp.mean(xf * xf, axis=-1, keepdims=True) + EPS)


def norm_back(xf, r, dy):
    inner = jnp.mean(xf * dy, axis=-1, keepdims=True)
    return dy * r - xf * (r * r * r * inner)


def block_kernel(n_seq, seq, n_layers, n_heads,
                 x_hbm, g_hbm, emb_ref, wq_hbm, wk_hbm, wv_hbm, wo_hbm, wup_hbm, wdn_hbm,
                 acc, dx_ref,
                 wqkv_s, wqkvt_s, wo_s, wot_s, wup_s, wupt_s, wdn_s, wdnt_s, emb_s,
                 x_s, qkv_s, p_s, mix_s, h_s, z_s,
                 u_s, g_s, dup_s, dn_s, dqkv_s, d_s, dmid_s, st_s,
                 r0, ra, rb, ra2, rb2, in_sem, ssem, rsem, free_sem):
    tok, dm = d_s.shape
    ff = wup_s.shape[1]
    hd = dm // n_heads
    pw = 2 * hd
    n_pair = n_heads // 2
    n_dn = ff // dm
    n_chunk = 2 * n_dn + 4
    k_o, k_q = 2 * n_dn, 2 * n_dn + 1
    scale = hd ** -0.5
    NB = 256
    rows = blocks(tok, 64)
    rows_b = blocks(tok, 32)

    me = lax.axis_index('data')
    c = lax.rem(me, 2)
    x = lax.rem(lax.div(me, 2), 2)
    y = lax.div(me, 4)
    cp = me + 1 - 2 * c
    xp = me + 2 - 4 * x
    yp = me + 4 - 8 * y
    barrier = pltpu.get_barrier_semaphore()
    for p in (cp, xp, yp):
        pl.semaphore_signal(barrier, inc=1, device_id=(p,), device_id_type=MESH)

    loads = [pltpu.make_async_copy(src, dst, in_sem.at[i]) for i, (src, dst) in enumerate((
        (wq_hbm, wqkvt_s.at[0:dm, :]), (wk_hbm, wqkvt_s.at[dm:2 * dm, :]), (wv_hbm, wqkvt_s.at[2 * dm:3 * dm, :]),
        (x_hbm, d_s), (wo_hbm, wo_s), (wup_hbm, wup_s), (wdn_hbm, wdn_s), (g_hbm, dmid_s)))]
    for ld in loads:
        ld.start()
    emb = emb_ref[...].astype(F32)
    for l in range(n_layers):
        emb_s[l] = emb[l:l + 1]
    acc[...] = jnp.zeros(acc.shape, F32)
    for i in range(3):
        loads[i].wait()
        wqkv_s[:, i * dm:(i + 1) * dm] = wqkvt_s[i * dm:(i + 1) * dm, :].T
    for ld in loads[3:]:
        ld.wait()
    wot_s[...] = wo_s[...].T
    wupt_s[...] = wup_s[...].T
    wdnt_s[...] = wdn_s[...].T

    low = lax.broadcasted_iota(jnp.int32, (seq, pw), 1) < hd

    def stack(a):
        zero = jnp.zeros_like(a)
        return jnp.concatenate([jnp.where(low, a, zero), jnp.where(low, zero, a)], axis=0)

    def halves(a):
        return a[:seq], a[seq:]

    def beside(a):
        return jnp.concatenate(halves(a), axis=1)

    def seq_rows(s):
        return slice(s * seq, (s + 1) * seq)

    def fwd(l, carry):
        emb_l = emb_s[l]
        for r_0, rn in rows:
            rs = slice(r_0, r_0 + rn)
            xb = (d_s[rs, :].astype(F32) + emb_l).astype(BF16)
            x_s[l, rs, :] = xb
            xf = xb.astype(F32)
            u_s[rs, :] = (xf * rms_scale(xf)).astype(BF16)
        for n0, nn in blocks(3 * dm, NB):
            ns = slice(n0, n0 + nn)
            qkv_s[l, :, ns] = mm(u_s[...], wqkv_s[:, ns]).astype(BF16)

        def scores(s):
            rs = seq_rows(s)
            for j in range(n_pair):
                cc = j * pw
                k = stack(qkv_s[l, rs, dm + cc:dm + cc + pw])
                st_s[s * n_pair + j] = mmg(k, qkv_s[l, rs, cc:cc + pw], NT).astype(BF16)

        def soft(s):
            for j in range(n_pair):
                for i, half in enumerate(halves(st_s[s * n_pair + j])):
                    sf = half.astype(F32)
                    top = jnp.max(sf, axis=0, keepdims=True)
                    e = jnp.exp2((sf - top) * (scale * LOG2E))
                    pr = e * (1.0 / jnp.sum(e, axis=0, keepdims=True))
                    p_s[l, s * n_pair + j, i * seq:(i + 1) * seq, :] = pr

        def mix(s):
            rs = seq_rows(s)
            for j in range(n_pair):
                cc = j * pw
                v = stack(qkv_s[l, rs, 2 * dm + cc:2 * dm + cc + pw])
                pb = p_s[l, s * n_pair + j].astype(BF16)
                mix_s[l, rs, cc:cc + pw] = mmg(pb, v, TN).astype(BF16)

        for s in range(n_seq + 2):
            if s < n_seq:
                scores(s)
            if 1 <= s <= n_seq:
                soft(s - 1)
            if s >= 2:
                mix(s - 2)
        for n0, nn in blocks(dm, NB):
            ns = slice(n0, n0 + nn)
            o = mm(mix_s[l], wo_s[:, ns]).astype(BF16)
            h_s[l, :, ns] = (x_s[l, :, ns].astype(F32) + o.astype(F32)).astype(BF16)
        for r_0, rn in rows:
            rs = slice(r_0, r_0 + rn)
            hf = h_s[l, rs, :].astype(F32)
            u_s[rs, :] = (hf * rms_scale(hf)).astype(BF16)
        for n0, nn in blocks(ff, NB):
            ns = slice(n0, n0 + nn)
            zb = mm(u_s[...], wup_s[:, ns]).astype(BF16)
            z_s[l, :, ns] = zb
            for r_0, rn in rows:
                z = zb[r_0:r_0 + rn].astype(F32)
                cdf = 0.5 + 0.5 * jnp.tanh(z * (GC0 + GC1 * (z * z)))
                g_s[r_0:r_0 + rn, ns] = (z * cdf).astype(BF16)
        for n0, nn in blocks(dm, NB):
            ns = slice(n0, n0 + nn)
            yd = mm(g_s[...], wdn_s[:, ns]).astype(BF16)
            d_s[:, ns] = (h_s[l, :, ns].astype(F32) + yd.astype(F32)).astype(BF16)
        return carry

    lax.fori_loop(0, n_layers, fwd, 0)
    d_s[...] = dmid_s[...]

    def bwd(l, hook):
        fb = blocks(ff, NB)

        def dact(i):
            n0, nn = fb[i]
            ns = slice(n0, n0 + nn)
            dup_s[:, ns] = mm(d_s[...], wdnt_s[:, ns]).astype(BF16)

        def gelu_back(i):
            n0, nn = fb[i]
            ns = slice(n0, n0 + nn)
            for r_0, rn in rows_b:
                rs = slice(r_0, r_0 + rn)
                z = z_s[l, rs, ns].astype(F32)
                z2 = z * z
                cdf = 0.5 + 0.5 * jnp.tanh(z * (GC0 + GC1 * z2))
                g = z * cdf
                g_s[rs, ns] = g.astype(BF16)
                dg = cdf + (g * (1.0 - cdf)) * (2.0 * GC0 + 6.0 * GC1 * z2)
                dup_s[rs, ns] = (dup_s[rs, ns].astype(F32) * dg).astype(BF16)

        def wg_down(i):
            n0, nn = fb[i]
            res = mmg(g_s[:, n0:n0 + nn], d_s[...], TN)
            for t in range(0, nn, 128):
                r = n0 + t
                acc[r // dm, r % dm:r % dm + 128, :] += res[t:t + 128]

        def wg_up(i):
            n0, nn = fb[i]
            res = mmg(u_s[...], dup_s[:, n0:n0 + nn], TN)
            for t in range(0, nn, 128):
                r = n0 + t
                acc[n_dn + r // dm, :, r % dm:r % dm + 128] += res[:, t:t + 128]

        def wg_qkv(i):
            acc[k_q + i] += mmg(dqkv_s[:, i * dm:(i + 1) * dm], u_s[...], TN)

        dact(0)
        for r_0, rn in rows:
            rs = slice(r_0, r_0 + rn)
            hf = h_s[l, rs, :].astype(F32)
            u_s[rs, :] = (hf * rms_scale(hf)).astype(BF16)
        for i in range(len(fb)):
            if i + 1 < len(fb):
                dact(i + 1)
            gelu_back(i)
            if i >= 1:
                wg_down(i - 1)
        wg_down(len(fb) - 1)
        hook(0)
        for n0, nn in blocks(dm, NB):
            ns = slice(n0, n0 + nn)
            dn_s[:, ns] = mm(dup_s[...], wupt_s[:, ns]).astype(BF16)
        for i, (r_0, rn) in enumerate(rows_b):
            rs = slice(r_0, r_0 + rn)
            hf = h_s[l, rs, :].astype(F32)
            dh = norm_back(hf, rms_scale(hf), dn_s[rs, :].astype(F32)).astype(BF16)
            dmid_s[rs, :] = (d_s[rs, :].astype(F32) + dh.astype(F32)).astype(BF16)
            if i % 4 == 3 and i // 4 < 2:
                wg_up(i // 4)
        hook(1)
        for n0, nn in blocks(dm, NB):
            ns = slice(n0, n0 + nn)
            dn_s[:, ns] = mm(dmid_s[...], wot_s[:, ns]).astype(BF16)

        def dprob(s):
            rs = seq_rows(s)
            for j in range(n_pair):
                cc = j * pw
                v = stack(qkv_s[l, rs, 2 * dm + cc:2 * dm + cc + pw])
                st_s[s * n_pair + j] = mmg(v, dn_s[rs, cc:cc + pw], NT).astype(BF16)

        def dscore(s):
            for j in range(n_pair):
                i = s * n_pair + j
                for hh in range(2):
                    hs = slice(hh * seq, (hh + 1) * seq)
                    pf = p_s[l, i, hs, :]
                    dp = st_s[i, hs, :].astype(F32)
                    inner = jnp.sum(pf * dp, axis=0, keepdims=True)
                    st_s[i, hs, :] = (pf * (dp - inner) * scale).astype(BF16)

        def dqkv(s):
            rs = seq_rows(s)
            for j in range(n_pair):
                i = s * n_pair + j
                cc = j * pw
                dst = st_s[i]
                q = stack(qkv_s[l, rs, cc:cc + pw])
                k = stack(qkv_s[l, rs, dm + cc:dm + cc + pw])
                dmx = stack(dn_s[rs, cc:cc + pw])
                dqkv_s[rs, cc:cc + pw] = mmg(dst, k, TN).astype(BF16)
                dqkv_s[rs, dm + cc:dm + cc + pw] = mm(beside(dst), q).astype(BF16)
                pb = p_s[l, i].astype(BF16)
                dqkv_s[rs, 2 * dm + cc:2 * dm + cc + pw] = mm(beside(pb), dmx).astype(BF16)

        for s in range(n_seq + 2):
            if s < n_seq:
                dprob(s)
                wg_up(2 + s)
            if 1 <= s <= n_seq:
                dscore(s - 1)
            if s == 2:
                acc[k_o] += mmg(mix_s[l], dmid_s[...], TN)
            if s >= 2:
                dqkv(s - 2)
            if s == n_seq - 1:
                hook(2)
        hook(3)
        for r_0, rn in rows:
            rs = slice(r_0, r_0 + rn)
            xf = x_s[l, rs, :].astype(F32)
            u_s[rs, :] = (xf * rms_scale(xf)).astype(BF16)
        for n0, nn in blocks(dm, NB):
            ns = slice(n0, n0 + nn)
            dn_s[:, ns] = mm(dqkv_s[...], wqkvt_s[:, ns]).astype(BF16)
        for i, (r_0, rn) in enumerate(rows_b):
            rs = slice(r_0, r_0 + rn)
            xf = x_s[l, rs, :].astype(F32)
            dh = norm_back(xf, rms_scale(xf), dn_s[rs, :].astype(F32)).astype(BF16)
            d_s[rs, :] = (dmid_s[rs, :].astype(F32) + dh.astype(F32)).astype(BF16)
            if i % 4 == 3 and i // 4 < 3:
                wg_qkv(i // 4)
        hook(4)

    def bwd_body(i, carry):
        bwd(n_layers - 1 - i, lambda n: None)
        return carry

    lax.fori_loop(0, n_layers - 1, bwd_body, 0)
    pl.semaphore_wait(barrier, 3)

    h0, h1, h2, h3 = dm // 2, dm // 4, dm // 8, dm // 16
    own = c * h0
    oth = (1 - c) * h0
    a0, a0n = own + x * h2, own + (1 - x) * h2
    b0, b0n = own + h1 + y * h2, own + h1 + (1 - y) * h2
    a1, a1n = a0 + y * h3, a0 + (1 - y) * h3
    b1, b1n = b0 + x * h3, b0 + (1 - x) * h3

    def part(k, off, n):
        return acc.at[k, pl.ds(pl.multiple_of(off, 8), n), :]

    def send(j, src, dst, dev):
        def at(k):
            return pltpu.make_async_remote_copy(
                src_ref=src(k), dst_ref=dst(k), send_sem=ssem.at[j, k], recv_sem=rsem.at[j, k],
                device_id=(dev,), device_id_type=MESH)
        return at

    def rows_of(off, n):
        return lambda k: part(k, off, n)

    def slot(ref, n):
        return lambda k: ref.at[k, 0:n, :]

    cs = [
        send(0, rows_of(oth, h0), slot(r0, h0), cp),
        send(1, rows_of(a0n, h2), slot(ra, h2), xp),
        send(2, rows_of(b0n, h2), slot(rb, h2), yp),
        send(3, rows_of(a1n, h3), slot(ra2, h3), yp),
        send(4, rows_of(b1n, h3), slot(rb2, h3), xp),
        send(5, rows_of(a1, h3), slot(ra, h3), yp),
        send(6, rows_of(b1, h3), slot(rb, h3), xp),
        send(7, rows_of(a1, h3), rows_of(a1, h3), xp),
        send(8, rows_of(b1, h3), rows_of(b1, h3), yp),
        send(9, slot(ra, h3), rows_of(a1n, h3), xp),
        send(10, slot(rb, h3), rows_of(b1n, h3), yp),
        send(11, rows_of(own, h0), rows_of(own, h0), cp),
    ]

    def add(k, off, n, src):
        sl = pl.ds(pl.multiple_of(off, 8), n)
        acc[k, sl, :] = acc[k, sl, :] + src[k]

    def loop(fn, lo=0, hi=n_chunk):
        lax.fori_loop(lo, hi, lambda k, t: (fn(k), t)[1], 0)

    def s0(k):
        cs[0](k).start()

    def s1(k):
        cs[0](k).wait_recv()
        add(k, own, h0, r0)
        cs[1](k).start()
        cs[2](k).start()

    def s2(k):
        cs[1](k).wait()
        add(k, a0, h2, ra)
        cs[2](k).wait()
        add(k, b0, h2, rb)
        cs[3](k).start()
        cs[4](k).start()

    def g2(k):
        cs[3](k).wait_recv()
        add(k, a1, h3, ra2)
        cs[4](k).wait_recv()
        add(k, b1, h3, rb2)
        for j in (5, 6, 7, 8):
            cs[j](k).start()

    def g1(k):
        cs[5](k).wait_recv()
        cs[9](k).start()
        cs[6](k).wait_recv()
        cs[10](k).start()
        cs[3](k).wait_send()
        acc[k, pl.ds(pl.multiple_of(a1n, 8), h3), :] = ra[k, 0:h3, :]
        cs[4](k).wait_send()
        acc[k, pl.ds(pl.multiple_of(b1n, 8), h3), :] = rb[k, 0:h3, :]

    def g0(k):
        for j in (7, 8, 9, 10):
            cs[j](k).wait_recv()
        cs[11](k).start()

    def finish(k):
        cs[11](k).wait_recv()
        for j in range(5, 12):
            cs[j](k).wait_send()

    def hook(n):
        if n == 0:
            loop(s0, 0, n_dn)
        elif n == 1:
            loop(s1, 0, n_dn)
        elif n == 2:
            loop(s0, n_dn, k_o + 1)
        elif n == 3:
            loop(s1, n_dn, k_o + 1)
        elif n == 4:
            loop(s0, k_q, n_chunk)

    bwd(0, hook)
    dx_ref[...] = d_s[...]
    loop(s1, k_q, n_chunk)
    loop(s2)
    loop(lambda k: cs[0](k).wait_send())
    pl.semaphore_signal(free_sem, inc=1, device_id=(cp,), device_id_type=MESH)
    loop(g2)
    loop(g1)
    pl.semaphore_wait(free_sem, 1)
    loop(g0)
    loop(finish)


def store_kernel(acc, dx_ref, oq, ok, ov, oo, oup, odn, odx, sem):
    dm = acc.shape[1]
    n = odn.shape[0] // dm
    dst = ([odn.at[i * dm:(i + 1) * dm, :] for i in range(n)]
           + [oup.at[:, i * dm:(i + 1) * dm] for i in range(n)] + [oo, oq, ok, ov])
    cps = [pltpu.make_async_copy(acc.at[i], d, sem.at[i]) for i, d in enumerate(dst)]
    cps.append(pltpu.make_async_copy(dx_ref, odx, sem.at[len(dst)]))
    for cc in cps:
        cc.start()
    for cc in cps:
        cc.wait()


def solution(mesh):
    batch_spec = P('data', None, None)

    def per_device(x_loc, g_loc, step_emb, w_q, w_k, w_v, w_o, w_up, w_down):
        n_seq, seq, dm = x_loc.shape
        n_layers = step_emb.shape[0]
        n_heads, hd = w_q.shape[1:]
        ff = w_up.shape[1]
        tok = n_seq * seq
        n_pair = n_heads // 2
        n_chunk = 4 + 2 * (ff // dm)
        wts = [w.transpose(1, 2, 0).reshape(n_heads * hd, dm) for w in (w_q, w_k, w_v)]
        vm = pl.BlockSpec(memory_space=pltpu.VMEM)
        hb = pl.BlockSpec(memory_space=pl.ANY)
        acc, dx = pl.pallas_call(
            functools.partial(block_kernel, n_seq, seq, n_layers, n_heads),
            out_shape=(pltpu.VMEM((n_chunk, dm, dm), F32), pltpu.VMEM((tok, dm), BF16)),
            in_specs=[hb, hb, vm] + [hb] * 6,
            out_specs=[vm] * 2,
            scratch_shapes=[
                pltpu.VMEM((dm, 3 * dm), BF16),
                pltpu.VMEM((3 * dm, dm), BF16),
                pltpu.VMEM((dm, dm), BF16),
                pltpu.VMEM((dm, dm), BF16),
                pltpu.VMEM((dm, ff), BF16),
                pltpu.VMEM((ff, dm), BF16),
                pltpu.VMEM((ff, dm), BF16),
                pltpu.VMEM((dm, ff), BF16),
                pltpu.VMEM((n_layers, 1, dm), F32),
                pltpu.VMEM((n_layers, tok, dm), BF16),
                pltpu.VMEM((n_layers, tok, 3 * dm), BF16),
                pltpu.VMEM((n_layers, n_seq * n_pair, 2 * seq, seq), F32),
                pltpu.VMEM((n_layers, tok, dm), BF16),
                pltpu.VMEM((n_layers, tok, dm), BF16),
                pltpu.VMEM((n_layers, tok, ff), BF16),
                pltpu.VMEM((tok, dm), BF16),
                pltpu.VMEM((tok, ff), BF16),
                pltpu.VMEM((tok, ff), BF16),
                pltpu.VMEM((tok, dm), BF16),
                pltpu.VMEM((tok, 3 * dm), BF16),
                pltpu.VMEM((tok, dm), BF16),
                pltpu.VMEM((tok, dm), BF16),
                pltpu.VMEM((n_seq * n_pair, 2 * seq, seq), BF16),
                pltpu.VMEM((n_chunk, dm // 2, dm), F32),
                pltpu.VMEM((n_chunk, dm // 8, dm), F32),
                pltpu.VMEM((n_chunk, dm // 8, dm), F32),
                pltpu.VMEM((n_chunk, dm // 16, dm), F32),
                pltpu.VMEM((n_chunk, dm // 16, dm), F32),
                pltpu.SemaphoreType.DMA((8,)),
                pltpu.SemaphoreType.DMA((12, n_chunk)),
                pltpu.SemaphoreType.DMA((12, n_chunk)),
                pltpu.SemaphoreType.REGULAR,
            ],
            compiler_params=pltpu.CompilerParams(
                collective_id=0, has_side_effects=True, vmem_limit_bytes=VMEM_LIMIT),
        )(x_loc.reshape(tok, dm), g_loc.reshape(tok, dm), step_emb,
          *wts, w_o.reshape(n_heads * hd, dm), w_up, w_down)
        sq = jax.ShapeDtypeStruct((dm, dm), F32)
        gq, gk, gv, go, gup, gdn, gx = pl.pallas_call(
            store_kernel,
            out_shape=(sq, sq, sq, sq, jax.ShapeDtypeStruct((dm, ff), F32), jax.ShapeDtypeStruct((ff, dm), F32),
                       jax.ShapeDtypeStruct((tok, dm), BF16)),
            in_specs=[vm] * 2,
            out_specs=[hb] * 7,
            scratch_shapes=[pltpu.SemaphoreType.DMA((n_chunk + 1,))],
            compiler_params=pltpu.CompilerParams(vmem_limit_bytes=2 ** 20),
        )(acc, dx)
        heads = [a.reshape(n_heads, hd, dm).transpose(2, 0, 1) for a in (gq, gk, gv)]
        return (*heads, go.reshape(n_heads, hd, dm), gup, gdn, gx.reshape(n_seq, seq, dm))

    return jax.shard_map(per_device, mesh=mesh, in_specs=(batch_spec, batch_spec, P(), P(), P(), P(), P(), P(), P()), out_specs=(P(), P(), P(), P(), P(), P(), batch_spec), check_vma=False)
```

```python
import functools
import math

import jax
import jax.numpy as jnp
from jax import lax
from jax.experimental import pallas as pl
from jax.experimental.pallas import tpu as pltpu
from jax.sharding import PartitionSpec as P

EPS = 1e-6
F32 = jnp.float32
BF16 = jnp.bfloat16
MESH = pl.DeviceIdType.MESH
LOG2E = math.log2(math.e)
GC0 = math.sqrt(2.0 / math.pi)
GC1 = GC0 * 0.044715
NT = (((1,), (1,)), ((), ()))
TN = (((0,), (0,)), ((), ()))
VMEM_LIMIT = 58851328
BLOCK = 256


def mm(a, b):
    return jnp.dot(a, b, preferred_element_type=F32)


def mmg(a, b, dims):
    return lax.dot_general(a, b, dims, preferred_element_type=F32)


def blocks(total, size):
    return [(s, min(size, total - s)) for s in range(0, total, size)]


def rms_scale(xf):
    return lax.rsqrt(jnp.mean(xf * xf, axis=-1, keepdims=True) + EPS)


def norm_back(xf, r, dy):
    inner = jnp.mean(xf * dy, axis=-1, keepdims=True)
    return dy * r - xf * (r * r * r * inner)


def block_kernel(n_seq, seq, n_layers, n_heads,
                 x_hbm, g_hbm, emb_ref, wq_hbm, wk_hbm, wv_hbm, wo_hbm, wup_hbm, wdn_hbm,
                 acc, dx_ref,
                 wqkv_s, wqkvt_s, wo_s, wot_s, wup_s, wupt_s, wdn_s, wdnt_s, emb_s,
                 x_s, qkv_s, p_s, mix_s, h_s, z_s,
                 u_s, g_s, da_s, yp_s, dn_s, d_s, dmid_s, st_s,
                 r0, ra, rb, ra2, rb2, in_sem, ssem, rsem, free_sem):
    tok, dm = d_s.shape
    ff = wup_s.shape[1]
    fb = blocks(ff, BLOCK)
    hd = dm // n_heads
    pw = 2 * hd
    n_pair = n_heads // 2
    n_dn = ff // dm
    n_chunk = 2 * n_dn + 4
    k_o, k_q = 2 * n_dn, 2 * n_dn + 1
    scale = hd ** -0.5
    NB = BLOCK
    rows = blocks(tok, 64)
    rows_b = blocks(tok, 32)

    me = lax.axis_index('data')
    c = lax.rem(me, 2)
    x = lax.rem(lax.div(me, 2), 2)
    y = lax.div(me, 4)
    cp = me + 1 - 2 * c
    xp = me + 2 - 4 * x
    yp = me + 4 - 8 * y
    barrier = pltpu.get_barrier_semaphore()
    for p in (cp, xp, yp):
        pl.semaphore_signal(barrier, inc=1, device_id=(p,), device_id_type=MESH)

    loads = [pltpu.make_async_copy(src, dst, in_sem.at[i]) for i, (src, dst) in enumerate((
        (wq_hbm, wqkvt_s.at[0:dm, :]), (wk_hbm, wqkvt_s.at[dm:2 * dm, :]), (wv_hbm, wqkvt_s.at[2 * dm:3 * dm, :]),
        (x_hbm, d_s), (wo_hbm, wo_s), (wup_hbm, wup_s), (wdn_hbm, wdn_s), (g_hbm, dmid_s.at[0])))]
    for ld in loads:
        ld.start()
    emb = emb_ref[...].astype(F32)
    for l in range(n_layers):
        emb_s[l] = emb[l:l + 1]
    acc[0:n_dn] = jnp.zeros((n_dn, dm, dm), F32)
    for i in range(3):
        loads[i].wait()
        wqkv_s[:, i * dm:(i + 1) * dm] = wqkvt_s[i * dm:(i + 1) * dm, :].T
    for ld in loads[3:]:
        ld.wait()
    wot_s[...] = wo_s[...].T

    low = lax.broadcasted_iota(jnp.int32, (seq, pw), 1) < hd

    def stack(a):
        zero = jnp.zeros_like(a)
        return jnp.concatenate([jnp.where(low, a, zero), jnp.where(low, zero, a)], axis=0)

    def halves(a):
        return a[:seq], a[seq:]

    def beside(a):
        return jnp.concatenate(halves(a), axis=1)

    def seq_rows(s):
        return slice(s * seq, (s + 1) * seq)

    def fwd(l, carry):
        emb_l = emb_s[l]
        tl = ff // n_layers
        ts = pl.ds(pl.multiple_of(l * tl, tl), tl)
        wupt_s[ts, :] = wup_s[:, ts].T
        wdnt_s[:, ts] = wdn_s[ts, :].T
        for r_0, rn in rows:
            rs = slice(r_0, r_0 + rn)
            xb = (d_s[rs, :].astype(F32) + emb_l).astype(BF16)
            x_s[l, rs, :] = xb
            xf = xb.astype(F32)
            u_s[rs, :] = (xf * rms_scale(xf)).astype(BF16)
        for n0, nn in blocks(3 * dm, NB):
            ns = slice(n0, n0 + nn)
            qkv_s[l, :, ns] = mm(u_s[...], wqkv_s[:, ns]).astype(BF16)

        def scores(s):
            rs = seq_rows(s)
            for j in range(n_pair):
                cc = j * pw
                k = stack(qkv_s[l, rs, dm + cc:dm + cc + pw])
                st_s[s * n_pair + j] = mmg(k, qkv_s[l, rs, cc:cc + pw], NT).astype(BF16)

        def soft(s):
            for j in range(n_pair):
                for i, half in enumerate(halves(st_s[s * n_pair + j])):
                    sf = half.astype(F32)
                    top = jnp.max(sf, axis=0, keepdims=True)
                    e = jnp.exp2((sf - top) * (scale * LOG2E))
                    pr = e * (1.0 / jnp.sum(e, axis=0, keepdims=True))
                    p_s[l, s * n_pair + j, i * seq:(i + 1) * seq, :] = pr

        def mix(s):
            rs = seq_rows(s)
            for j in range(n_pair):
                cc = j * pw
                v = stack(qkv_s[l, rs, 2 * dm + cc:2 * dm + cc + pw])
                pb = p_s[l, s * n_pair + j].astype(BF16)
                mix_s[l, rs, cc:cc + pw] = mmg(pb, v, TN).astype(BF16)

        for s in range(n_seq + 2):
            if s < n_seq:
                scores(s)
            if 1 <= s <= n_seq:
                soft(s - 1)
            if s >= 2:
                mix(s - 2)
        for n0, nn in blocks(dm, NB):
            ns = slice(n0, n0 + nn)
            o = mm(mix_s[l], wo_s[:, ns]).astype(BF16)
            h_s[l, :, ns] = (x_s[l, :, ns].astype(F32) + o.astype(F32)).astype(BF16)
        for r_0, rn in rows:
            rs = slice(r_0, r_0 + rn)
            hf = h_s[l, rs, :].astype(F32)
            u_s[rs, :] = (hf * rms_scale(hf)).astype(BF16)
        def up(i):
            n0, nn = fb[i]
            ns = slice(n0, n0 + nn)
            z_s[l, :, ns] = mm(u_s[...], wup_s[:, ns]).astype(BF16)

        def gelu(i):
            n0, nn = fb[i]
            ns = slice(n0, n0 + nn)
            for r_0, rn in rows:
                rs = slice(r_0, r_0 + rn)
                z = z_s[l, rs, ns].astype(F32)
                cdf = 0.5 + 0.5 * jnp.tanh(z * (GC0 + GC1 * (z * z)))
                g_s[rs, ns] = (z * cdf).astype(BF16)

        half = len(fb) // 2 * BLOCK
        up(0)
        for i in range(len(fb)):
            if i + 1 < len(fb):
                up(i + 1)
            gelu(i)
            if i + 1 == len(fb) - 1:
                for n0, nn in blocks(dm, NB):
                    ns = slice(n0, n0 + nn)
                    yp_s[:, ns] = mm(g_s[:, :half], wdn_s[:half, ns])
        for n0, nn in blocks(dm, NB):
            ns = slice(n0, n0 + nn)
            yd = (yp_s[:, ns] + mm(g_s[:, half:], wdn_s[half:, ns])).astype(BF16)
            d_s[:, ns] = (h_s[l, :, ns].astype(F32) + yd.astype(F32)).astype(BF16)
        return carry

    lax.fori_loop(0, n_layers, fwd, 0)
    d_s[...] = dmid_s[0]

    def gelu_phase(l, after):
        def dact(i):
            n0, nn = fb[i]
            da_s[i % 2] = mm(d_s[...], wdnt_s[:, n0:n0 + nn]).astype(BF16)

        def gelu_back(i):
            n0, nn = fb[i]
            ns = slice(n0, n0 + nn)
            for r_0, rn in rows_b:
                rs = slice(r_0, r_0 + rn)
                z = z_s[l, rs, ns].astype(F32)
                z2 = z * z
                cdf = 0.5 + 0.5 * jnp.tanh(z * (GC0 + GC1 * z2))
                g = z * cdf
                g_s[rs, ns] = g.astype(BF16)
                dg = cdf + (g * (1.0 - cdf)) * (2.0 * GC0 + 6.0 * GC1 * z2)
                z_s[l, rs, ns] = (da_s[i % 2, rs, :].astype(F32) * dg).astype(BF16)

        def wg_down(i):
            n0, nn = fb[i]
            res = mmg(g_s[:, n0:n0 + nn], d_s[...], TN)
            for t in range(0, nn, 128):
                r = n0 + t
                acc[r // dm, r % dm:r % dm + 128, :] += res[t:t + 128]

        dact(0)
        for i in range(len(fb)):
            if i + 1 < len(fb):
                dact(i + 1)
            gelu_back(i)
            if i >= 1:
                wg_down(i - 1)
                after(i - 1)
        wg_down(len(fb) - 1)
        after(len(fb) - 1)

    def mid_phase(l):
        for n0, nn in blocks(dm, NB):
            ns = slice(n0, n0 + nn)
            dn_s[:, ns] = mm(z_s[l], wupt_s[:, ns]).astype(BF16)
        for r_0, rn in rows_b:
            rs = slice(r_0, r_0 + rn)
            hf = h_s[l, rs, :].astype(F32)
            r = rms_scale(hf)
            dh = norm_back(hf, r, dn_s[rs, :].astype(F32)).astype(BF16)
            h_s[l, rs, :] = (hf * r).astype(BF16)
            dmid_s[l, rs, :] = (d_s[rs, :].astype(F32) + dh.astype(F32)).astype(BF16)

    def attn_phase(l):
        for n0, nn in blocks(dm, NB):
            ns = slice(n0, n0 + nn)
            dn_s[:, ns] = mm(dmid_s[l], wot_s[:, ns]).astype(BF16)

        def dprob(s):
            rs = seq_rows(s)
            for j in range(n_pair):
                cc = j * pw
                v = stack(qkv_s[l, rs, 2 * dm + cc:2 * dm + cc + pw])
                st_s[s * n_pair + j] = mmg(v, dn_s[rs, cc:cc + pw], NT).astype(BF16)

        def dscore(s):
            for j in range(n_pair):
                i = s * n_pair + j
                for hh in range(2):
                    hs = slice(hh * seq, (hh + 1) * seq)
                    pf = p_s[l, i, hs, :]
                    dp = st_s[i, hs, :].astype(F32)
                    inner = jnp.sum(pf * dp, axis=0, keepdims=True)
                    st_s[i, hs, :] = (pf * (dp - inner) * scale).astype(BF16)

        def dqkv(s):
            rs = seq_rows(s)
            for j in range(n_pair):
                i = s * n_pair + j
                cc = j * pw
                dst = st_s[i]
                q = stack(qkv_s[l, rs, cc:cc + pw])
                k = stack(qkv_s[l, rs, dm + cc:dm + cc + pw])
                dmx = stack(dn_s[rs, cc:cc + pw])
                qkv_s[l, rs, cc:cc + pw] = mmg(dst, k, TN).astype(BF16)
                qkv_s[l, rs, dm + cc:dm + cc + pw] = mm(beside(dst), q).astype(BF16)
                pb = p_s[l, i].astype(BF16)
                qkv_s[l, rs, 2 * dm + cc:2 * dm + cc + pw] = mm(beside(pb), dmx).astype(BF16)

        for s in range(n_seq + 2):
            if s < n_seq:
                dprob(s)
            if 1 <= s <= n_seq:
                dscore(s - 1)
            if s >= 2:
                dqkv(s - 2)

    def in_phase(l):
        for n0, nn in blocks(dm, NB):
            ns = slice(n0, n0 + nn)
            dn_s[:, ns] = mm(qkv_s[l], wqkvt_s[:, ns]).astype(BF16)
        for r_0, rn in rows_b:
            rs = slice(r_0, r_0 + rn)
            xf = x_s[l, rs, :].astype(F32)
            r = rms_scale(xf)
            dh = norm_back(xf, r, dn_s[rs, :].astype(F32)).astype(BF16)
            x_s[l, rs, :] = (xf * r).astype(BF16)
            d_s[rs, :] = (dmid_s[l, rs, :].astype(F32) + dh.astype(F32)).astype(BF16)

    def bwd_body(i, carry):
        l = n_layers - 1 - i
        gelu_phase(l, lambda n: None)
        mid_phase(l)
        attn_phase(l)
        in_phase(l)
        return carry

    lax.fori_loop(0, n_layers - 1, bwd_body, 0)
    pl.semaphore_wait(barrier, 3)

    h0, h1, h2, h3 = dm // 2, dm // 4, dm // 8, dm // 16
    own = c * h0
    oth = (1 - c) * h0
    a0, a0n = own + x * h2, own + (1 - x) * h2
    b0, b0n = own + h1 + y * h2, own + h1 + (1 - y) * h2
    a1, a1n = a0 + y * h3, a0 + (1 - y) * h3
    b1, b1n = b0 + x * h3, b0 + (1 - x) * h3

    def part(k, off, n):
        return acc.at[k, pl.ds(pl.multiple_of(off, 8), n), :]

    def send(j, src, dst, dev):
        def at(k):
            return pltpu.make_async_remote_copy(
                src_ref=src(k), dst_ref=dst(k), send_sem=ssem.at[j, k], recv_sem=rsem.at[j, k],
                device_id=(dev,), device_id_type=MESH)
        return at

    def rows_of(off, n):
        return lambda k: part(k, off, n)

    def slot(ref, n):
        return lambda k: ref.at[k, 0:n, :]

    cs = [
        send(0, rows_of(oth, h0), slot(r0, h0), cp),
        send(1, rows_of(a0n, h2), slot(ra, h2), xp),
        send(2, rows_of(b0n, h2), slot(rb, h2), yp),
        send(3, rows_of(a1n, h3), slot(ra2, h3), yp),
        send(4, rows_of(b1n, h3), slot(rb2, h3), xp),
        send(5, rows_of(a1, h3), slot(ra, h3), yp),
        send(6, rows_of(b1, h3), slot(rb, h3), xp),
        send(7, rows_of(a1, h3), rows_of(a1, h3), xp),
        send(8, rows_of(b1, h3), rows_of(b1, h3), yp),
        send(9, slot(ra, h3), rows_of(a1n, h3), xp),
        send(10, slot(rb, h3), rows_of(b1n, h3), yp),
        send(11, rows_of(own, h0), rows_of(own, h0), cp),
    ]

    def add(k, off, n, src):
        sl = pl.ds(pl.multiple_of(off, 8), n)
        acc[k, sl, :] = acc[k, sl, :] + src[k]

    def loop(fn, lo=0, hi=n_chunk):
        lax.fori_loop(lo, hi, lambda k, t: (fn(k), t)[1], 0)

    def s0(k):
        cs[0](k).start()

    def s1(k):
        cs[0](k).wait_recv()
        add(k, own, h0, r0)
        cs[1](k).start()
        cs[2](k).start()

    def s2(k):
        cs[1](k).wait()
        add(k, a0, h2, ra)
        cs[2](k).wait()
        add(k, b0, h2, rb)
        cs[3](k).start()
        cs[4](k).start()

    def g2(k):
        cs[3](k).wait_recv()
        add(k, a1, h3, ra2)
        cs[4](k).wait_recv()
        add(k, b1, h3, rb2)
        for j in (5, 6, 7, 8):
            cs[j](k).start()

    def g1(k):
        cs[5](k).wait_recv()
        cs[9](k).start()
        cs[6](k).wait_recv()
        cs[10](k).start()
        cs[3](k).wait_send()
        acc[k, pl.ds(pl.multiple_of(a1n, 8), h3), :] = ra[k, 0:h3, :]
        cs[4](k).wait_send()
        acc[k, pl.ds(pl.multiple_of(b1n, 8), h3), :] = rb[k, 0:h3, :]

    def g0(k):
        for j in (7, 8, 9, 10):
            cs[j](k).wait_recv()
        cs[11](k).start()

    def finish(k):
        cs[11](k).wait_recv()
        for j in range(5, 12):
            cs[j](k).wait_send()

    first = n_layers - 1

    def put(l, k, sl, val):
        if l == first:
            acc[(k, *sl)] = val
        else:
            acc[(k, *sl)] += val

    def wg_up(l, m):
        for n0, nn in fb:
            res = mmg(m, z_s[l, :, n0:n0 + nn], TN)
            for t in range(0, nn, 128):
                r = n0 + t
                put(l, n_dn + r // dm, (slice(None), slice(r % dm, r % dm + 128)), res[:, t:t + 128])

    def wg_o(l):
        put(l, k_o, (slice(None), slice(None)), mmg(mix_s[l], dmid_s[l], TN))

    def wg_qkv(l):
        for i in range(3):
            put(l, k_q + i, (slice(None), slice(None)), mmg(qkv_s[l, :, i * dm:(i + 1) * dm], x_s[l], TN))

    def after(i):
        done = min((i + 1) * BLOCK // dm, n_dn)
        prev = i * BLOCK // dm
        for k in range(prev, done):
            s0(k)
        if i >= 1:
            for k in range((i - 1) * BLOCK // dm, prev):
                s1(k)

    for r_0, rn in rows:
        rs = slice(r_0, r_0 + rn)
        hf = h_s[0, rs, :].astype(F32)
        u_s[rs, :] = (hf * rms_scale(hf)).astype(BF16)
    gelu_phase(0, after)
    order = list(range(first, -1, -1))
    for i, l in enumerate(order):
        wg_up(l, h_s[l] if l else u_s[...])
        if i == 0:
            loop(s1, n_dn - 1, n_dn)
        if i >= 3:
            loop(s2, i - 3, i - 2)
    loop(s0, n_dn, 2 * n_dn)
    loop(s2, 3, n_dn)
    mid_phase(0)
    loop(s1, n_dn, 2 * n_dn)
    attn_phase(0)
    loop(g2, 0, n_dn)
    in_phase(0)
    dx_ref[...] = d_s[...]
    loop(s2, n_dn, 2 * n_dn)
    for l in order:
        wg_o(l)
    loop(s0, k_o, k_o + 1)
    loop(g1, 0, n_dn)
    for i, l in enumerate(order):
        wg_qkv(l)
        if i == 1:
            loop(s1, k_o, k_o + 1)
        if i == 3:
            loop(g2, n_dn, 2 * n_dn)
    loop(s0, k_q, n_chunk)
    loop(s1, k_q, n_chunk)
    loop(lambda k: cs[0](k).wait_send())
    pl.semaphore_signal(free_sem, inc=1, device_id=(cp,), device_id_type=MESH)
    loop(g1, n_dn, 2 * n_dn)
    loop(s2, 2 * n_dn, n_chunk)
    pl.semaphore_wait(free_sem, 1)
    loop(g0, 0, n_dn)
    loop(g2, 2 * n_dn, n_chunk)
    loop(g0, n_dn, 2 * n_dn)
    loop(g1, 2 * n_dn, n_chunk)
    loop(g0, 2 * n_dn, n_chunk)
    loop(finish)


def store_kernel(acc, dx_ref, oq, ok, ov, oo, oup, odn, odx, sem):
    dm = acc.shape[1]
    n = odn.shape[0] // dm
    dst = ([odn.at[i * dm:(i + 1) * dm, :] for i in range(n)]
           + [oup.at[:, i * dm:(i + 1) * dm] for i in range(n)] + [oo, oq, ok, ov])
    cps = [pltpu.make_async_copy(acc.at[i], d, sem.at[i]) for i, d in enumerate(dst)]
    cps.append(pltpu.make_async_copy(dx_ref, odx, sem.at[len(dst)]))
    for cc in cps:
        cc.start()
    for cc in cps:
        cc.wait()


def solution(mesh):
    batch_spec = P('data', None, None)

    def per_device(x_loc, g_loc, step_emb, w_q, w_k, w_v, w_o, w_up, w_down):
        n_seq, seq, dm = x_loc.shape
        n_layers = step_emb.shape[0]
        n_heads, hd = w_q.shape[1:]
        ff = w_up.shape[1]
        tok = n_seq * seq
        n_pair = n_heads // 2
        n_chunk = 4 + 2 * (ff // dm)
        wts = [w.transpose(1, 2, 0).reshape(n_heads * hd, dm) for w in (w_q, w_k, w_v)]
        vm = pl.BlockSpec(memory_space=pltpu.VMEM)
        hb = pl.BlockSpec(memory_space=pl.ANY)
        acc, dx = pl.pallas_call(
            functools.partial(block_kernel, n_seq, seq, n_layers, n_heads),
            out_shape=(pltpu.VMEM((n_chunk, dm, dm), F32), pltpu.VMEM((tok, dm), BF16)),
            in_specs=[hb, hb, vm] + [hb] * 6,
            out_specs=[vm] * 2,
            scratch_shapes=[
                pltpu.VMEM((dm, 3 * dm), BF16),
                pltpu.VMEM((3 * dm, dm), BF16),
                pltpu.VMEM((dm, dm), BF16),
                pltpu.VMEM((dm, dm), BF16),
                pltpu.VMEM((dm, ff), BF16),
                pltpu.VMEM((ff, dm), BF16),
                pltpu.VMEM((ff, dm), BF16),
                pltpu.VMEM((dm, ff), BF16),
                pltpu.VMEM((n_layers, 1, dm), F32),
                pltpu.VMEM((n_layers, tok, dm), BF16),
                pltpu.VMEM((n_layers, tok, 3 * dm), BF16),
                pltpu.VMEM((n_layers, n_seq * n_pair, 2 * seq, seq), F32),
                pltpu.VMEM((n_layers, tok, dm), BF16),
                pltpu.VMEM((n_layers, tok, dm), BF16),
                pltpu.VMEM((n_layers, tok, ff), BF16),
                pltpu.VMEM((tok, dm), BF16),
                pltpu.VMEM((tok, ff), BF16),
                pltpu.VMEM((2, tok, BLOCK), BF16),
                pltpu.VMEM((tok, dm), F32),
                pltpu.VMEM((tok, dm), BF16),
                pltpu.VMEM((tok, dm), BF16),
                pltpu.VMEM((n_layers, tok, dm), BF16),
                pltpu.VMEM((n_seq * n_pair, 2 * seq, seq), BF16),
                pltpu.VMEM((n_chunk, dm // 2, dm), F32),
                pltpu.VMEM((n_chunk, dm // 8, dm), F32),
                pltpu.VMEM((n_chunk, dm // 8, dm), F32),
                pltpu.VMEM((n_chunk, dm // 16, dm), F32),
                pltpu.VMEM((n_chunk, dm // 16, dm), F32),
                pltpu.SemaphoreType.DMA((8,)),
                pltpu.SemaphoreType.DMA((12, n_chunk)),
                pltpu.SemaphoreType.DMA((12, n_chunk)),
                pltpu.SemaphoreType.REGULAR,
            ],
            compiler_params=pltpu.CompilerParams(
                collective_id=0, has_side_effects=True, vmem_limit_bytes=VMEM_LIMIT),
        )(x_loc.reshape(tok, dm), g_loc.reshape(tok, dm), step_emb,
          *wts, w_o.reshape(n_heads * hd, dm), w_up, w_down)
        sq = jax.ShapeDtypeStruct((dm, dm), F32)
        gq, gk, gv, go, gup, gdn, gx = pl.pallas_call(
            store_kernel,
            out_shape=(sq, sq, sq, sq, jax.ShapeDtypeStruct((dm, ff), F32), jax.ShapeDtypeStruct((ff, dm), F32),
                       jax.ShapeDtypeStruct((tok, dm), BF16)),
            in_specs=[vm] * 2,
            out_specs=[hb] * 7,
            scratch_shapes=[pltpu.SemaphoreType.DMA((n_chunk + 1,))],
            compiler_params=pltpu.CompilerParams(vmem_limit_bytes=2 ** 20),
        )(acc, dx)
        heads = [a.reshape(n_heads, hd, dm).transpose(2, 0, 1) for a in (gq, gk, gv)]
        return (*heads, go.reshape(n_heads, hd, dm), gup, gdn, gx.reshape(n_seq, seq, dm))

    return jax.shard_map(per_device, mesh=mesh, in_specs=(batch_spec, batch_spec, P(), P(), P(), P(), P(), P(), P()), out_specs=(P(), P(), P(), P(), P(), P(), batch_spec), check_vma=False)
```

```python
import functools
import math

import jax
import jax.numpy as jnp
from jax import lax
from jax.experimental import pallas as pl
from jax.experimental.pallas import tpu as pltpu
from jax.sharding import PartitionSpec as P

EPS = 1e-6
F32 = jnp.float32
BF16 = jnp.bfloat16
MESH = pl.DeviceIdType.MESH
LOG2E = math.log2(math.e)
GC0 = math.sqrt(2.0 / math.pi)
GC1 = GC0 * 0.044715
NT = (((1,), (1,)), ((), ()))
TN = (((0,), (0,)), ((), ()))
VMEM_LIMIT = 58851328
BLOCK = 256


def mm(a, b):
    return jnp.dot(a, b, preferred_element_type=F32)


def mmg(a, b, dims):
    return lax.dot_general(a, b, dims, preferred_element_type=F32)


def blocks(total, size):
    return [(s, min(size, total - s)) for s in range(0, total, size)]


def rms_scale(xf):
    return lax.rsqrt(jnp.mean(xf * xf, axis=-1, keepdims=True) + EPS)


def norm_back(xf, r, dy):
    inner = jnp.mean(xf * dy, axis=-1, keepdims=True)
    return dy * r - xf * (r * r * r * inner)


def merge(*streams):
    plan = []
    for si, (start, steps) in enumerate(streams):
        at = start
        for cost, fn in steps:
            plan.append((at, si, fn))
            at += cost
    for _, _, fn in sorted(plan, key=lambda e: e[:2]):
        fn()


def block_kernel(n_seq, seq, n_layers, n_heads,
                 x_hbm, g_hbm, emb_ref, wq_hbm, wk_hbm, wv_hbm, wo_hbm, wup_hbm, wdn_hbm,
                 acc, dx_ref,
                 wqkv_s, wqkvt_s, wo_s, wot_s, wup_s, wupt_s, wdn_s, wdnt_s, emb_s,
                 x_s, qkv_s, p_s, mix_s, h_s, z_s,
                 u_s, g_s, da_s, dn_s, d_s, dmid_s, st_s,
                 r0, ra, rb, ra2, rb2, in_sem, ssem, rsem, free_sem):
    tok, dm = d_s.shape
    ff = wup_s.shape[1]
    fb = blocks(ff, BLOCK)
    hd = dm // n_heads
    pw = 2 * hd
    n_pair = n_heads // 2
    n_dn = ff // dm
    n_chunk = 2 * n_dn + 4
    k_o, k_q = 2 * n_dn, 2 * n_dn + 1
    scale = hd ** -0.5
    NB = BLOCK
    rows = blocks(tok, 64)
    rows_b = blocks(tok, 32)

    me = lax.axis_index('data')
    c = lax.rem(me, 2)
    x = lax.rem(lax.div(me, 2), 2)
    y = lax.div(me, 4)
    cp = me + 1 - 2 * c
    xp = me + 2 - 4 * x
    yp = me + 4 - 8 * y
    barrier = pltpu.get_barrier_semaphore()
    for p in (cp, xp, yp):
        pl.semaphore_signal(barrier, inc=1, device_id=(p,), device_id_type=MESH)

    loads = [pltpu.make_async_copy(src, dst, in_sem.at[i]) for i, (src, dst) in enumerate((
        (wq_hbm, wqkvt_s.at[0:dm, :]), (wk_hbm, wqkvt_s.at[dm:2 * dm, :]), (wv_hbm, wqkvt_s.at[2 * dm:3 * dm, :]),
        (x_hbm, d_s), (wo_hbm, wo_s), (wup_hbm, wup_s), (wdn_hbm, wdn_s), (g_hbm, dmid_s.at[0])))]
    for ld in loads:
        ld.start()
    emb = emb_ref[...].astype(F32)
    for l in range(n_layers):
        emb_s[l] = emb[l:l + 1]
    acc[0:n_dn] = jnp.zeros((n_dn, dm, dm), F32)
    for i in range(3):
        loads[i].wait()
        wqkv_s[:, i * dm:(i + 1) * dm] = wqkvt_s[i * dm:(i + 1) * dm, :].T
    for ld in loads[3:]:
        ld.wait()
    wot_s[...] = wo_s[...].T

    low = lax.broadcasted_iota(jnp.int32, (seq, pw), 1) < hd

    def stack(a):
        zero = jnp.zeros_like(a)
        return jnp.concatenate([jnp.where(low, a, zero), jnp.where(low, zero, a)], axis=0)

    def halves(a):
        return a[:seq], a[seq:]

    def beside(a):
        return jnp.concatenate(halves(a), axis=1)

    def seq_rows(s):
        return slice(s * seq, (s + 1) * seq)

    hrows = tok // 2
    hseq = n_seq // 2

    def sub_rows(h, rb):
        return [slice(h * hrows + r_0, h * hrows + r_0 + rn) for r_0, rn in blocks(hrows, rb)]

    def col_blocks(n):
        return [slice(n0, n0 + nn) for n0, nn in blocks(n, NB)]

    def fwd_half(l, h):
        hr = slice(h * hrows, (h + 1) * hrows)
        emb_l = emb_s[l]
        steps = []

        def start(rs):
            xb = (d_s[rs, :].astype(F32) + emb_l).astype(BF16)
            x_s[l, rs, :] = xb
            xf = xb.astype(F32)
            u_s[rs, :] = (xf * rms_scale(xf)).astype(BF16)

        def qkv(ns):
            qkv_s[l, hr, ns] = mm(u_s[hr, :], wqkv_s[:, ns]).astype(BF16)

        def scores(s, j):
            rs = seq_rows(s)
            cc = j * pw
            k = stack(qkv_s[l, rs, dm + cc:dm + cc + pw])
            st_s[s * n_pair + j] = mmg(k, qkv_s[l, rs, cc:cc + pw], NT).astype(BF16)

        def soft(s, j):
            for i, half in enumerate(halves(st_s[s * n_pair + j])):
                sf = half.astype(F32)
                top = jnp.max(sf, axis=0, keepdims=True)
                e = jnp.exp2((sf - top) * (scale * LOG2E))
                pr = e * (1.0 / jnp.sum(e, axis=0, keepdims=True))
                p_s[l, s * n_pair + j, i * seq:(i + 1) * seq, :] = pr

        def mix(s, j):
            rs = seq_rows(s)
            cc = j * pw
            v = stack(qkv_s[l, rs, 2 * dm + cc:2 * dm + cc + pw])
            pb = p_s[l, s * n_pair + j].astype(BF16)
            mix_s[l, rs, cc:cc + pw] = mmg(pb, v, TN).astype(BF16)

        def out(ns):
            o = mm(mix_s[l, hr, :], wo_s[:, ns]).astype(BF16)
            h_s[l, hr, ns] = (x_s[l, hr, ns].astype(F32) + o.astype(F32)).astype(BF16)

        def norm2(rs):
            hf = h_s[l, rs, :].astype(F32)
            u_s[rs, :] = (hf * rms_scale(hf)).astype(BF16)

        def up(ns):
            z_s[l, hr, ns] = mm(u_s[hr, :], wup_s[:, ns]).astype(BF16)

        def gelu(rs, ns):
            z = z_s[l, rs, ns].astype(F32)
            cdf = 0.5 + 0.5 * jnp.tanh(z * (GC0 + GC1 * (z * z)))
            g_s[rs, ns] = (z * cdf).astype(BF16)

        def down(ns):
            yd = mm(g_s[hr, :], wdn_s[:, ns]).astype(BF16)
            d_s[hr, ns] = (h_s[l, hr, ns].astype(F32) + yd.astype(F32)).astype(BF16)

        def step(cost, fn, *args):
            steps.append((cost, functools.partial(fn, *args)))

        for rs in sub_rows(h, 64):
            step(60, start, rs)
        for ns in col_blocks(3 * dm):
            step(120, qkv, ns)
        pairs = [(h * hseq + s, j) for s in range(hseq) for j in range(n_pair)]
        for t in range(len(pairs) + 3):
            if t < len(pairs):
                step(40, scores, *pairs[t])
            if 1 <= t <= len(pairs):
                step(70, soft, *pairs[t - 1])
            if t >= 3:
                step(50, mix, *pairs[t - 3])
        for ns in col_blocks(dm):
            step(100, out, ns)
        for rs in sub_rows(h, 64):
            step(70, norm2, rs)
        cols = col_blocks(ff)
        step(100, up, cols[0])
        for i, ns in enumerate(cols):
            if i + 1 < len(cols):
                step(20, up, cols[i + 1])
            for rs in sub_rows(h, 64):
                step(38, gelu, rs, ns)
        for ns in col_blocks(dm):
            step(380, down, ns)
        return steps

    def fwd(l, carry):
        tl = ff // n_layers
        ts = pl.ds(pl.multiple_of(l * tl, tl), tl)

        def wt():
            wupt_s[ts, :] = wup_s[:, ts].T
            wdnt_s[:, ts] = wdn_s[ts, :].T

        merge((0, fwd_half(l, 0)), (400, fwd_half(l, 1)), (2500, [(1, wt)]))
        return carry

    lax.fori_loop(0, n_layers, fwd, 0)
    d_s[...] = dmid_s[0]

    def gelu_phase(l, after):
        def dact(i):
            n0, nn = fb[i]
            da_s[i % 2] = mm(d_s[...], wdnt_s[:, n0:n0 + nn]).astype(BF16)

        def gelu_back(i):
            n0, nn = fb[i]
            ns = slice(n0, n0 + nn)
            for r_0, rn in rows_b:
                rs = slice(r_0, r_0 + rn)
                z = z_s[l, rs, ns].astype(F32)
                z2 = z * z
                cdf = 0.5 + 0.5 * jnp.tanh(z * (GC0 + GC1 * z2))
                g = z * cdf
                g_s[rs, ns] = g.astype(BF16)
                dg = cdf + (g * (1.0 - cdf)) * (2.0 * GC0 + 6.0 * GC1 * z2)
                z_s[l, rs, ns] = (da_s[i % 2, rs, :].astype(F32) * dg).astype(BF16)

        def wg_down(i):
            n0, nn = fb[i]
            res = mmg(g_s[:, n0:n0 + nn], d_s[...], TN)
            for t in range(0, nn, 128):
                r = n0 + t
                acc[r // dm, r % dm:r % dm + 128, :] += res[t:t + 128]

        dact(0)
        for i in range(len(fb)):
            if i + 1 < len(fb):
                dact(i + 1)
            gelu_back(i)
            if i >= 1:
                wg_down(i - 1)
                after(i - 1)
        wg_down(len(fb) - 1)
        after(len(fb) - 1)

    def mid_phase(l):
        for n0, nn in blocks(dm, NB):
            ns = slice(n0, n0 + nn)
            dn_s[:, ns] = mm(z_s[l], wupt_s[:, ns]).astype(BF16)
        for r_0, rn in rows_b:
            rs = slice(r_0, r_0 + rn)
            hf = h_s[l, rs, :].astype(F32)
            r = rms_scale(hf)
            dh = norm_back(hf, r, dn_s[rs, :].astype(F32)).astype(BF16)
            h_s[l, rs, :] = (hf * r).astype(BF16)
            dmid_s[l, rs, :] = (d_s[rs, :].astype(F32) + dh.astype(F32)).astype(BF16)

    def attn_phase(l):
        for n0, nn in blocks(dm, NB):
            ns = slice(n0, n0 + nn)
            dn_s[:, ns] = mm(dmid_s[l], wot_s[:, ns]).astype(BF16)

        def dprob(s):
            rs = seq_rows(s)
            for j in range(n_pair):
                cc = j * pw
                v = stack(qkv_s[l, rs, 2 * dm + cc:2 * dm + cc + pw])
                st_s[s * n_pair + j] = mmg(v, dn_s[rs, cc:cc + pw], NT).astype(BF16)

        def dscore(s):
            for j in range(n_pair):
                i = s * n_pair + j
                for hh in range(2):
                    hs = slice(hh * seq, (hh + 1) * seq)
                    pf = p_s[l, i, hs, :]
                    dp = st_s[i, hs, :].astype(F32)
                    inner = jnp.sum(pf * dp, axis=0, keepdims=True)
                    st_s[i, hs, :] = (pf * (dp - inner) * scale).astype(BF16)

        def dqkv(s):
            rs = seq_rows(s)
            for j in range(n_pair):
                i = s * n_pair + j
                cc = j * pw
                dst = st_s[i]
                q = stack(qkv_s[l, rs, cc:cc + pw])
                k = stack(qkv_s[l, rs, dm + cc:dm + cc + pw])
                dmx = stack(dn_s[rs, cc:cc + pw])
                qkv_s[l, rs, cc:cc + pw] = mmg(dst, k, TN).astype(BF16)
                qkv_s[l, rs, dm + cc:dm + cc + pw] = mm(beside(dst), q).astype(BF16)
                pb = p_s[l, i].astype(BF16)
                qkv_s[l, rs, 2 * dm + cc:2 * dm + cc + pw] = mm(beside(pb), dmx).astype(BF16)

        for s in range(n_seq + 2):
            if s < n_seq:
                dprob(s)
            if 1 <= s <= n_seq:
                dscore(s - 1)
            if s >= 2:
                dqkv(s - 2)

    def in_phase(l):
        for n0, nn in blocks(dm, NB):
            ns = slice(n0, n0 + nn)
            dn_s[:, ns] = mm(qkv_s[l], wqkvt_s[:, ns]).astype(BF16)
        for r_0, rn in rows_b:
            rs = slice(r_0, r_0 + rn)
            xf = x_s[l, rs, :].astype(F32)
            r = rms_scale(xf)
            dh = norm_back(xf, r, dn_s[rs, :].astype(F32)).astype(BF16)
            x_s[l, rs, :] = (xf * r).astype(BF16)
            d_s[rs, :] = (dmid_s[l, rs, :].astype(F32) + dh.astype(F32)).astype(BF16)

    def bwd_body(i, carry):
        l = n_layers - 1 - i
        gelu_phase(l, lambda n: None)
        mid_phase(l)
        attn_phase(l)
        in_phase(l)
        return carry

    lax.fori_loop(0, n_layers - 1, bwd_body, 0)
    pl.semaphore_wait(barrier, 3)

    h0, h1, h2, h3 = dm // 2, dm // 4, dm // 8, dm // 16
    own = c * h0
    oth = (1 - c) * h0
    a0, a0n = own + x * h2, own + (1 - x) * h2
    b0, b0n = own + h1 + y * h2, own + h1 + (1 - y) * h2
    a1, a1n = a0 + y * h3, a0 + (1 - y) * h3
    b1, b1n = b0 + x * h3, b0 + (1 - x) * h3

    def part(k, off, n):
        return acc.at[k, pl.ds(pl.multiple_of(off, 8), n), :]

    def send(j, src, dst, dev):
        def at(k):
            return pltpu.make_async_remote_copy(
                src_ref=src(k), dst_ref=dst(k), send_sem=ssem.at[j, k], recv_sem=rsem.at[j, k],
                device_id=(dev,), device_id_type=MESH)
        return at

    def rows_of(off, n):
        return lambda k: part(k, off, n)

    def slot(ref, n):
        return lambda k: ref.at[k, 0:n, :]

    cs = [
        send(0, rows_of(oth, h0), slot(r0, h0), cp),
        send(1, rows_of(a0n, h2), slot(ra, h2), xp),
        send(2, rows_of(b0n, h2), slot(rb, h2), yp),
        send(3, rows_of(a1n, h3), slot(ra2, h3), yp),
        send(4, rows_of(b1n, h3), slot(rb2, h3), xp),
        send(5, rows_of(a1, h3), slot(ra, h3), yp),
        send(6, rows_of(b1, h3), slot(rb, h3), xp),
        send(7, rows_of(a1, h3), rows_of(a1, h3), xp),
        send(8, rows_of(b1, h3), rows_of(b1, h3), yp),
        send(9, slot(ra, h3), rows_of(a1n, h3), xp),
        send(10, slot(rb, h3), rows_of(b1n, h3), yp),
        send(11, rows_of(own, h0), rows_of(own, h0), cp),
    ]

    def add(k, off, n, src):
        sl = pl.ds(pl.multiple_of(off, 8), n)
        acc[k, sl, :] = acc[k, sl, :] + src[k]

    def loop(fn, lo=0, hi=n_chunk):
        lax.fori_loop(lo, hi, lambda k, t: (fn(k), t)[1], 0)

    def s0(k):
        cs[0](k).start()

    def s1(k):
        cs[0](k).wait_recv()
        add(k, own, h0, r0)
        cs[1](k).start()
        cs[2](k).start()

    def s2(k):
        cs[1](k).wait()
        add(k, a0, h2, ra)
        cs[2](k).wait()
        add(k, b0, h2, rb)
        cs[3](k).start()
        cs[4](k).start()

    def g2(k, both=True):
        cs[3](k).wait_recv()
        add(k, a1, h3, ra2)
        cs[4](k).wait_recv()
        add(k, b1, h3, rb2)
        for j in (5, 6, 7, 8) if both else (5, 6):
            cs[j](k).start()

    def g2_own(k):
        cs[7](k).start()
        cs[8](k).start()

    def g1(k):
        cs[5](k).wait_recv()
        cs[9](k).start()
        cs[6](k).wait_recv()
        cs[10](k).start()
        cs[3](k).wait_send()
        acc[k, pl.ds(pl.multiple_of(a1n, 8), h3), :] = ra[k, 0:h3, :]
        cs[4](k).wait_send()
        acc[k, pl.ds(pl.multiple_of(b1n, 8), h3), :] = rb[k, 0:h3, :]

    def g0(k):
        for j in (7, 8, 9, 10):
            cs[j](k).wait_recv()
        cs[11](k).start()

    def finish(k):
        cs[11](k).wait_recv()
        for j in range(5, 12):
            cs[j](k).wait_send()

    first = n_layers - 1

    def put(l, k, sl, val):
        if l == first:
            acc[(k, *sl)] = val
        else:
            acc[(k, *sl)] += val

    def wg_up(l, m):
        for n0, nn in fb:
            res = mmg(m, z_s[l, :, n0:n0 + nn], TN)
            for t in range(0, nn, 128):
                r = n0 + t
                put(l, n_dn + r // dm, (slice(None), slice(r % dm, r % dm + 128)), res[:, t:t + 128])

    def wg_o(l):
        put(l, k_o, (slice(None), slice(None)), mmg(mix_s[l], dmid_s[l], TN))

    def wg_qkv(l):
        for i in range(3):
            put(l, k_q + i, (slice(None), slice(None)), mmg(qkv_s[l, :, i * dm:(i + 1) * dm], x_s[l], TN))

    def after(i):
        done = min((i + 1) * BLOCK // dm, n_dn)
        prev = i * BLOCK // dm
        for k in range(prev, done):
            s0(k)
        if i >= 1:
            for k in range((i - 1) * BLOCK // dm, prev):
                s1(k)

    for r_0, rn in rows:
        rs = slice(r_0, r_0 + rn)
        hf = h_s[0, rs, :].astype(F32)
        u_s[rs, :] = (hf * rms_scale(hf)).astype(BF16)
    gelu_phase(0, after)
    order = list(range(first, -1, -1))
    for i, l in enumerate(order):
        wg_up(l, h_s[l] if l else u_s[...])
        if i == 0:
            loop(s1, n_dn - 1, n_dn)
        if i >= 3:
            loop(s2, i - 3, i - 2)
    loop(s0, n_dn, 2 * n_dn)
    loop(s2, 3, n_dn)
    mid_phase(0)
    loop(s1, n_dn, 2 * n_dn)
    attn_phase(0)
    loop(g2, 0, n_dn)
    in_phase(0)
    dx_ref[...] = d_s[...]
    loop(s2, n_dn, 2 * n_dn)
    for l in order:
        wg_o(l)
    loop(s0, k_o, k_o + 1)
    loop(g1, 0, n_dn)
    for i, l in enumerate(order):
        wg_qkv(l)
        if i == 1:
            loop(s1, k_o, k_o + 1)
        if i == 3:
            loop(g2, n_dn, 2 * n_dn)
    loop(s0, k_q, n_chunk)
    loop(s1, k_q, n_chunk)
    loop(lambda k: cs[0](k).wait_send())
    pl.semaphore_signal(free_sem, inc=1, device_id=(cp,), device_id_type=MESH)
    loop(g1, n_dn, 2 * n_dn)
    loop(s2, 2 * n_dn, n_chunk)
    pl.semaphore_wait(free_sem, 1)
    loop(g0, 0, n_dn)
    loop(lambda k: g2(k, False), 2 * n_dn, n_chunk)
    loop(g2_own, 2 * n_dn, n_chunk)
    loop(g0, n_dn, 2 * n_dn)
    loop(g1, 2 * n_dn, n_chunk)
    loop(g0, 2 * n_dn, n_chunk)
    loop(finish)


def store_kernel(acc, dx_ref, oq, ok, ov, oo, oup, odn, odx, sem):
    dm = acc.shape[1]
    n = odn.shape[0] // dm
    dst = ([odn.at[i * dm:(i + 1) * dm, :] for i in range(n)]
           + [oup.at[:, i * dm:(i + 1) * dm] for i in range(n)] + [oo, oq, ok, ov])
    cps = [pltpu.make_async_copy(acc.at[i], d, sem.at[i]) for i, d in enumerate(dst)]
    cps.append(pltpu.make_async_copy(dx_ref, odx, sem.at[len(dst)]))
    for cc in cps:
        cc.start()
    for cc in cps:
        cc.wait()


def solution(mesh):
    batch_spec = P('data', None, None)

    def per_device(x_loc, g_loc, step_emb, w_q, w_k, w_v, w_o, w_up, w_down):
        n_seq, seq, dm = x_loc.shape
        n_layers = step_emb.shape[0]
        n_heads, hd = w_q.shape[1:]
        ff = w_up.shape[1]
        tok = n_seq * seq
        n_pair = n_heads // 2
        n_chunk = 4 + 2 * (ff // dm)
        wts = [w.transpose(1, 2, 0).reshape(n_heads * hd, dm) for w in (w_q, w_k, w_v)]
        vm = pl.BlockSpec(memory_space=pltpu.VMEM)
        hb = pl.BlockSpec(memory_space=pl.ANY)
        acc, dx = pl.pallas_call(
            functools.partial(block_kernel, n_seq, seq, n_layers, n_heads),
            out_shape=(pltpu.VMEM((n_chunk, dm, dm), F32), pltpu.VMEM((tok, dm), BF16)),
            in_specs=[hb, hb, vm] + [hb] * 6,
            out_specs=[vm] * 2,
            scratch_shapes=[
                pltpu.VMEM((dm, 3 * dm), BF16),
                pltpu.VMEM((3 * dm, dm), BF16),
                pltpu.VMEM((dm, dm), BF16),
                pltpu.VMEM((dm, dm), BF16),
                pltpu.VMEM((dm, ff), BF16),
                pltpu.VMEM((ff, dm), BF16),
                pltpu.VMEM((ff, dm), BF16),
                pltpu.VMEM((dm, ff), BF16),
                pltpu.VMEM((n_layers, 1, dm), F32),
                pltpu.VMEM((n_layers, tok, dm), BF16),
                pltpu.VMEM((n_layers, tok, 3 * dm), BF16),
                pltpu.VMEM((n_layers, n_seq * n_pair, 2 * seq, seq), F32),
                pltpu.VMEM((n_layers, tok, dm), BF16),
                pltpu.VMEM((n_layers, tok, dm), BF16),
                pltpu.VMEM((n_layers, tok, ff), BF16),
                pltpu.VMEM((tok, dm), BF16),
                pltpu.VMEM((tok, ff), BF16),
                pltpu.VMEM((2, tok, BLOCK), BF16),
                pltpu.VMEM((tok, dm), BF16),
                pltpu.VMEM((tok, dm), BF16),
                pltpu.VMEM((n_layers, tok, dm), BF16),
                pltpu.VMEM((n_seq * n_pair, 2 * seq, seq), BF16),
                pltpu.VMEM((n_chunk, dm // 2, dm), F32),
                pltpu.VMEM((n_chunk, dm // 8, dm), F32),
                pltpu.VMEM((n_chunk, dm // 8, dm), F32),
                pltpu.VMEM((n_chunk, dm // 16, dm), F32),
                pltpu.VMEM((n_chunk, dm // 16, dm), F32),
                pltpu.SemaphoreType.DMA((8,)),
                pltpu.SemaphoreType.DMA((12, n_chunk)),
                pltpu.SemaphoreType.DMA((12, n_chunk)),
                pltpu.SemaphoreType.REGULAR,
            ],
            compiler_params=pltpu.CompilerParams(
                collective_id=0, has_side_effects=True, vmem_limit_bytes=VMEM_LIMIT),
        )(x_loc.reshape(tok, dm), g_loc.reshape(tok, dm), step_emb,
          *wts, w_o.reshape(n_heads * hd, dm), w_up, w_down)
        sq = jax.ShapeDtypeStruct((dm, dm), F32)
        gq, gk, gv, go, gup, gdn, gx = pl.pallas_call(
            store_kernel,
            out_shape=(sq, sq, sq, sq, jax.ShapeDtypeStruct((dm, ff), F32), jax.ShapeDtypeStruct((ff, dm), F32),
                       jax.ShapeDtypeStruct((tok, dm), BF16)),
            in_specs=[vm] * 2,
            out_specs=[hb] * 7,
            scratch_shapes=[pltpu.SemaphoreType.DMA((n_chunk + 1,))],
            compiler_params=pltpu.CompilerParams(vmem_limit_bytes=2 ** 20),
        )(acc, dx)
        heads = [a.reshape(n_heads, hd, dm).transpose(2, 0, 1) for a in (gq, gk, gv)]
        return (*heads, go.reshape(n_heads, hd, dm), gup, gdn, gx.reshape(n_seq, seq, dm))

    return jax.shard_map(per_device, mesh=mesh, in_specs=(batch_spec, batch_spec, P(), P(), P(), P(), P(), P(), P()), out_specs=(P(), P(), P(), P(), P(), P(), batch_spec), check_vma=False)
```

```python
import functools
import math

import jax
import jax.numpy as jnp
from jax import lax
from jax.experimental import pallas as pl
from jax.experimental.pallas import tpu as pltpu
from jax.sharding import PartitionSpec as P

EPS = 1e-6
F32 = jnp.float32
BF16 = jnp.bfloat16
MESH = pl.DeviceIdType.MESH
LOG2E = math.log2(math.e)
GC0 = math.sqrt(2.0 / math.pi)
GC1 = GC0 * 0.044715
NT = (((1,), (1,)), ((), ()))
TN = (((0,), (0,)), ((), ()))
VMEM_LIMIT = 58851328
BLOCK = 256


def mm(a, b):
    return jnp.dot(a, b, preferred_element_type=F32)


def mmg(a, b, dims):
    return lax.dot_general(a, b, dims, preferred_element_type=F32)


def blocks(total, size):
    return [(s, min(size, total - s)) for s in range(0, total, size)]


def rms_scale(xf):
    return lax.rsqrt(jnp.mean(xf * xf, axis=-1, keepdims=True) + EPS)


def norm_back(xf, r, dy):
    inner = jnp.mean(xf * dy, axis=-1, keepdims=True)
    return dy * r - xf * (r * r * r * inner)


def merge(*streams):
    plan = []
    for si, (start, steps) in enumerate(streams):
        at = start
        for cost, fn in steps:
            plan.append((at, si, fn))
            at += cost
    for _, _, fn in sorted(plan, key=lambda e: e[:2]):
        fn()


def block_kernel(n_seq, seq, n_layers, n_heads,
                 x_hbm, g_hbm, emb_hbm, wq_hbm, wk_hbm, wv_hbm, wo_hbm, wup_hbm, wdn_hbm,
                 acc, dx_ref,
                 wqkv_s, wqkvt_s, wo_s, wot_s, wup_s, wupt_s, wdn_s, wdnt_s, emb_s, embb_s,
                 x_s, qkv_s, p_s, mix_s, h_s, z_s,
                 u_s, g_s, da_s, dn_s, d_s, dmid_s, st_s,
                 r0, ra, rb, ra2, rb2, in_sem, ssem, rsem, free_sem):
    tok, dm = d_s.shape
    ff = wup_s.shape[1]
    fb = blocks(ff, BLOCK)
    hd = dm // n_heads
    pw = 2 * hd
    n_pair = n_heads // 2
    n_dn = ff // dm
    n_chunk = 2 * n_dn + 4
    k_o, k_q = 2 * n_dn, 2 * n_dn + 1
    scale = hd ** -0.5
    NB = BLOCK
    rows = blocks(tok, 64)
    rows_b = blocks(tok, 32)

    me = lax.axis_index('data')
    c = lax.rem(me, 2)
    x = lax.rem(lax.div(me, 2), 2)
    y = lax.div(me, 4)
    cp = me + 1 - 2 * c
    xp = me + 2 - 4 * x
    yp = me + 4 - 8 * y
    barrier = pltpu.get_barrier_semaphore()
    for p in (cp, xp, yp):
        pl.semaphore_signal(barrier, inc=1, device_id=(p,), device_id_type=MESH)

    loads = [pltpu.make_async_copy(src, dst, in_sem.at[i]) for i, (src, dst) in enumerate((
        (wq_hbm, wqkvt_s.at[0:dm, :]), (wk_hbm, wqkvt_s.at[dm:2 * dm, :]), (wv_hbm, wqkvt_s.at[2 * dm:3 * dm, :]),
        (x_hbm, d_s), (wo_hbm, wo_s), (wup_hbm, wup_s), (wdn_hbm, wdn_s), (g_hbm, dmid_s.at[0]), (emb_hbm, embb_s)))]
    for ld in loads:
        ld.start()
    acc[0:n_dn] = jnp.zeros((n_dn, dm, dm), F32)
    for i in range(3):
        loads[i].wait()
        wqkv_s[:, i * dm:(i + 1) * dm] = wqkvt_s[i * dm:(i + 1) * dm, :].T
    for ld in loads[3:]:
        ld.wait()
    emb = embb_s[...].astype(F32)
    for l in range(n_layers):
        emb_s[l] = emb[l:l + 1]
    wot_s[...] = wo_s[...].T

    low = lax.broadcasted_iota(jnp.int32, (seq, pw), 1) < hd

    def stack(a):
        zero = jnp.zeros_like(a)
        return jnp.concatenate([jnp.where(low, a, zero), jnp.where(low, zero, a)], axis=0)

    def halves(a):
        return a[:seq], a[seq:]

    def beside(a):
        return jnp.concatenate(halves(a), axis=1)

    def seq_rows(s):
        return slice(s * seq, (s + 1) * seq)

    hrows = tok // 2
    hseq = n_seq // 2

    def sub_rows(h, rb):
        return [slice(h * hrows + r_0, h * hrows + r_0 + rn) for r_0, rn in blocks(hrows, rb)]

    def col_blocks(n):
        return [slice(n0, n0 + nn) for n0, nn in blocks(n, NB)]

    def fwd_half(l, h):
        hr = slice(h * hrows, (h + 1) * hrows)
        emb_l = emb_s[l]
        steps = []

        def start(rs):
            xb = (d_s[rs, :].astype(F32) + emb_l).astype(BF16)
            x_s[l, rs, :] = xb
            xf = xb.astype(F32)
            u_s[rs, :] = (xf * rms_scale(xf)).astype(BF16)

        def qkv(ns):
            qkv_s[l, hr, ns] = mm(u_s[hr, :], wqkv_s[:, ns]).astype(BF16)

        def scores(s, j):
            rs = seq_rows(s)
            cc = j * pw
            k = stack(qkv_s[l, rs, dm + cc:dm + cc + pw])
            st_s[s * n_pair + j] = mmg(k, qkv_s[l, rs, cc:cc + pw], NT).astype(BF16)

        def soft(s, j):
            for i, half in enumerate(halves(st_s[s * n_pair + j])):
                sf = half.astype(F32)
                top = jnp.max(sf, axis=0, keepdims=True)
                e = jnp.exp2((sf - top) * (scale * LOG2E))
                pr = e * (1.0 / jnp.sum(e, axis=0, keepdims=True))
                p_s[l, s * n_pair + j, i * seq:(i + 1) * seq, :] = pr

        def mix(s, j):
            rs = seq_rows(s)
            cc = j * pw
            v = stack(qkv_s[l, rs, 2 * dm + cc:2 * dm + cc + pw])
            pb = p_s[l, s * n_pair + j].astype(BF16)
            mix_s[l, rs, cc:cc + pw] = mmg(pb, v, TN).astype(BF16)

        def out(ns):
            o = mm(mix_s[l, hr, :], wo_s[:, ns]).astype(BF16)
            h_s[l, hr, ns] = (x_s[l, hr, ns].astype(F32) + o.astype(F32)).astype(BF16)

        def norm2(rs):
            hf = h_s[l, rs, :].astype(F32)
            u_s[rs, :] = (hf * rms_scale(hf)).astype(BF16)

        def up(ns):
            z_s[l, hr, ns] = mm(u_s[hr, :], wup_s[:, ns]).astype(BF16)

        def gelu(rs, ns):
            z = z_s[l, rs, ns].astype(F32)
            cdf = 0.5 + 0.5 * jnp.tanh(z * (GC0 + GC1 * (z * z)))
            g_s[rs, ns] = (z * cdf).astype(BF16)

        def down(ns):
            yd = mm(g_s[hr, :], wdn_s[:, ns]).astype(BF16)
            d_s[hr, ns] = (h_s[l, hr, ns].astype(F32) + yd.astype(F32)).astype(BF16)

        def step(cost, fn, *args):
            steps.append((cost, functools.partial(fn, *args)))

        for rs in sub_rows(h, 64):
            step(60, start, rs)
        for ns in col_blocks(3 * dm):
            step(120, qkv, ns)
        pairs = [(h * hseq + s, j) for s in range(hseq) for j in range(n_pair)]
        for t in range(len(pairs) + 3):
            if t < len(pairs):
                step(40, scores, *pairs[t])
            if 1 <= t <= len(pairs):
                step(70, soft, *pairs[t - 1])
            if t >= 3:
                step(50, mix, *pairs[t - 3])
        for ns in col_blocks(dm):
            step(100, out, ns)
        for rs in sub_rows(h, 64):
            step(70, norm2, rs)
        cols = col_blocks(ff)
        step(100, up, cols[0])
        for i, ns in enumerate(cols):
            if i + 1 < len(cols):
                step(20, up, cols[i + 1])
            for rs in sub_rows(h, 64):
                step(38, gelu, rs, ns)
        for ns in col_blocks(dm):
            step(380, down, ns)
        return steps

    def fwd(l, carry):
        tl = ff // n_layers
        ts = pl.ds(pl.multiple_of(l * tl, tl), tl)

        def wt():
            wupt_s[ts, :] = wup_s[:, ts].T
            wdnt_s[:, ts] = wdn_s[ts, :].T

        merge((0, fwd_half(l, 0)), (700, fwd_half(l, 1)), (2500, [(1, wt)]))
        return carry

    lax.fori_loop(0, n_layers, fwd, 0)
    d_s[...] = dmid_s[0]

    def gelu_phase(l, after):
        def dact(i):
            n0, nn = fb[i]
            da_s[i % 2] = mm(d_s[...], wdnt_s[:, n0:n0 + nn]).astype(BF16)

        def gelu_back(i):
            n0, nn = fb[i]
            ns = slice(n0, n0 + nn)
            for r_0, rn in blocks(tok, 32):
                rs = slice(r_0, r_0 + rn)
                z = z_s[l, rs, ns].astype(F32)
                z2 = z * z
                cdf = 0.5 + 0.5 * jnp.tanh(z * (GC0 + GC1 * z2))
                g = z * cdf
                g_s[rs, ns] = g.astype(BF16)
                dg = cdf + (g * (1.0 - cdf)) * (2.0 * GC0 + 6.0 * GC1 * z2)
                z_s[l, rs, ns] = (da_s[i % 2, rs, :].astype(F32) * dg).astype(BF16)

        def wg_down(i):
            n0, nn = fb[i]
            res = mmg(g_s[:, n0:n0 + nn], d_s[...], TN)
            for t in range(0, nn, 128):
                r = n0 + t
                acc[r // dm, r % dm:r % dm + 128, :] += res[t:t + 128]

        dact(0)
        for i in range(len(fb)):
            if i + 1 < len(fb):
                dact(i + 1)
            gelu_back(i)
            if i >= 1:
                wg_down(i - 1)
                after(i - 1)
        wg_down(len(fb) - 1)
        after(len(fb) - 1)

    def mid_phase(l):
        for n0, nn in blocks(dm, NB):
            ns = slice(n0, n0 + nn)
            dn_s[:, ns] = mm(z_s[l], wupt_s[:, ns]).astype(BF16)
        for r_0, rn in blocks(tok, 32):
            rs = slice(r_0, r_0 + rn)
            hf = h_s[l, rs, :].astype(F32)
            r = rms_scale(hf)
            dh = norm_back(hf, r, dn_s[rs, :].astype(F32)).astype(BF16)
            h_s[l, rs, :] = (hf * r).astype(BF16)
            dmid_s[l, rs, :] = (d_s[rs, :].astype(F32) + dh.astype(F32)).astype(BF16)

    def attn_phase(l):
        for n0, nn in blocks(dm, NB):
            ns = slice(n0, n0 + nn)
            dn_s[:tok // 2, ns] = mm(dmid_s[l, :tok // 2], wot_s[:, ns]).astype(BF16)
        for n0, nn in blocks(dm, NB):
            ns = slice(n0, n0 + nn)
            dn_s[tok // 2:, ns] = mm(dmid_s[l, tok // 2:], wot_s[:, ns]).astype(BF16)

        def dprob(s, j):
            rs = seq_rows(s)
            cc = j * pw
            v = stack(qkv_s[l, rs, 2 * dm + cc:2 * dm + cc + pw])
            st_s[s * n_pair + j] = mmg(v, dn_s[rs, cc:cc + pw], NT).astype(BF16)

        def dscore(s, j):
            i = s * n_pair + j
            for hh in range(2):
                hs = slice(hh * seq, (hh + 1) * seq)
                pf = p_s[l, i, hs, :]
                dp = st_s[i, hs, :].astype(F32)
                inner = jnp.sum(pf * dp, axis=0, keepdims=True)
                st_s[i, hs, :] = (pf * (dp - inner) * scale).astype(BF16)

        def dqkv(s, j):
            rs = seq_rows(s)
            i = s * n_pair + j
            cc = j * pw
            dst = st_s[i]
            q = stack(qkv_s[l, rs, cc:cc + pw])
            k = stack(qkv_s[l, rs, dm + cc:dm + cc + pw])
            dmx = stack(dn_s[rs, cc:cc + pw])
            qkv_s[l, rs, cc:cc + pw] = mmg(dst, k, TN).astype(BF16)
            qkv_s[l, rs, dm + cc:dm + cc + pw] = mm(beside(dst), q).astype(BF16)
            pb = p_s[l, i].astype(BF16)
            qkv_s[l, rs, 2 * dm + cc:2 * dm + cc + pw] = mm(beside(pb), dmx).astype(BF16)

        pairs = [(s, j) for s in range(n_seq) for j in range(n_pair)]
        for t in range(len(pairs) + 3):
            if t < len(pairs):
                dprob(*pairs[t])
            if 1 <= t < len(pairs) + 1:
                dscore(*pairs[t - 1])
            if t >= 3:
                dqkv(*pairs[t - 3])

    def in_phase(l):
        for n0, nn in blocks(dm, NB):
            ns = slice(n0, n0 + nn)
            dn_s[:tok // 2, ns] = mm(qkv_s[l, :tok // 2], wqkvt_s[:, ns]).astype(BF16)
        for n0, nn in blocks(dm, NB):
            ns = slice(n0, n0 + nn)
            dn_s[tok // 2:, ns] = mm(qkv_s[l, tok // 2:], wqkvt_s[:, ns]).astype(BF16)
        for r_0, rn in blocks(tok, 32):
            rs = slice(r_0, r_0 + rn)
            xf = x_s[l, rs, :].astype(F32)
            r = rms_scale(xf)
            dh = norm_back(xf, r, dn_s[rs, :].astype(F32)).astype(BF16)
            x_s[l, rs, :] = (xf * r).astype(BF16)
            d_s[rs, :] = (dmid_s[l, rs, :].astype(F32) + dh.astype(F32)).astype(BF16)

    def bwd_body(i, carry):
        l = n_layers - 1 - i
        gelu_phase(l, lambda n: None)
        mid_phase(l)
        attn_phase(l)
        in_phase(l)
        return carry

    lax.fori_loop(0, n_layers - 1, bwd_body, 0)
    pl.semaphore_wait(barrier, 3)

    h0, h1, h2, h3 = dm // 2, dm // 4, dm // 8, dm // 16
    own = c * h0
    oth = (1 - c) * h0
    a0, a0n = own + x * h2, own + (1 - x) * h2
    b0, b0n = own + h1 + y * h2, own + h1 + (1 - y) * h2
    a1, a1n = a0 + y * h3, a0 + (1 - y) * h3
    b1, b1n = b0 + x * h3, b0 + (1 - x) * h3

    def part(k, off, n):
        return acc.at[k, pl.ds(pl.multiple_of(off, 8), n), :]

    def send(j, src, dst, dev):
        def at(k):
            return pltpu.make_async_remote_copy(
                src_ref=src(k), dst_ref=dst(k), send_sem=ssem.at[j, k], recv_sem=rsem.at[j, k],
                device_id=(dev,), device_id_type=MESH)
        return at

    def rows_of(off, n):
        return lambda k: part(k, off, n)

    def slot(ref, n):
        return lambda k: ref.at[k, 0:n, :]

    cs = [
        send(0, rows_of(oth, h0), slot(r0, h0), cp),
        send(1, rows_of(a0n, h2), slot(ra, h2), xp),
        send(2, rows_of(b0n, h2), slot(rb, h2), yp),
        send(3, rows_of(a1n, h3), slot(ra2, h3), yp),
        send(4, rows_of(b1n, h3), slot(rb2, h3), xp),
        send(5, rows_of(a1, h3), slot(ra, h3), yp),
        send(6, rows_of(b1, h3), slot(rb, h3), xp),
        send(7, rows_of(a1, h3), rows_of(a1, h3), xp),
        send(8, rows_of(b1, h3), rows_of(b1, h3), yp),
        send(9, slot(ra, h3), rows_of(a1n, h3), xp),
        send(10, slot(rb, h3), rows_of(b1n, h3), yp),
        send(11, rows_of(own, h0), rows_of(own, h0), cp),
    ]

    def add(k, off, n, src):
        sl = pl.ds(pl.multiple_of(off, 8), n)
        acc[k, sl, :] = acc[k, sl, :] + src[k]

    def loop(fn, lo=0, hi=n_chunk):
        lax.fori_loop(lo, hi, lambda k, t: (fn(k), t)[1], 0)

    def s0(k):
        cs[0](k).start()

    def s1(k):
        cs[0](k).wait_recv()
        add(k, own, h0, r0)
        cs[1](k).start()
        cs[2](k).start()

    def s2(k):
        cs[1](k).wait()
        add(k, a0, h2, ra)
        cs[2](k).wait()
        add(k, b0, h2, rb)
        cs[3](k).start()
        cs[4](k).start()

    def g2(k, both=True):
        cs[3](k).wait_recv()
        add(k, a1, h3, ra2)
        cs[4](k).wait_recv()
        add(k, b1, h3, rb2)
        for j in (5, 6, 7, 8) if both else (5, 6):
            cs[j](k).start()

    def g2_own(k):
        cs[7](k).start()
        cs[8](k).start()

    def g1(k):
        cs[5](k).wait_recv()
        cs[9](k).start()
        cs[6](k).wait_recv()
        cs[10](k).start()
        cs[3](k).wait_send()
        acc[k, pl.ds(pl.multiple_of(a1n, 8), h3), :] = ra[k, 0:h3, :]
        cs[4](k).wait_send()
        acc[k, pl.ds(pl.multiple_of(b1n, 8), h3), :] = rb[k, 0:h3, :]

    def g0(k):
        for j in (7, 8, 9, 10):
            cs[j](k).wait_recv()
        cs[11](k).start()

    def finish(k):
        cs[11](k).wait_recv()
        for j in range(5, 12):
            cs[j](k).wait_send()

    first = n_layers - 1

    def put(l, k, sl, val):
        if l == first:
            acc[(k, *sl)] = val
        else:
            acc[(k, *sl)] += val

    def wg_up(l, m):
        for n0, nn in fb:
            res = mmg(m, z_s[l, :, n0:n0 + nn], TN)
            for t in range(0, nn, 128):
                r = n0 + t
                put(l, n_dn + r // dm, (slice(None), slice(r % dm, r % dm + 128)), res[:, t:t + 128])

    def wg_o(l):
        put(l, k_o, (slice(None), slice(None)), mmg(mix_s[l], dmid_s[l], TN))

    def wg_qkv(l):
        for i in range(3):
            put(l, k_q + i, (slice(None), slice(None)), mmg(qkv_s[l, :, i * dm:(i + 1) * dm], x_s[l], TN))

    def after(i):
        done = min((i + 1) * BLOCK // dm, n_dn)
        prev = i * BLOCK // dm
        for k in range(prev, done):
            s0(k)
        if i >= 1:
            for k in range((i - 1) * BLOCK // dm, prev):
                s1(k)

    for r_0, rn in rows:
        rs = slice(r_0, r_0 + rn)
        hf = h_s[0, rs, :].astype(F32)
        u_s[rs, :] = (hf * rms_scale(hf)).astype(BF16)
    gelu_phase(0, after)
    order = list(range(first, -1, -1))
    for i, l in enumerate(order):
        wg_up(l, h_s[l] if l else u_s[...])
        if i == 0:
            loop(s1, n_dn - 1, n_dn)
        if i >= 3:
            loop(s2, i - 3, i - 2)
    loop(s0, n_dn, 2 * n_dn)
    loop(s2, 3, n_dn)
    mid_phase(0)
    loop(s1, n_dn, 2 * n_dn)
    attn_phase(0)
    loop(g2, 0, n_dn)
    in_phase(0)
    dx_ref[...] = d_s[...]
    loop(s2, n_dn, 2 * n_dn)
    for l in order:
        wg_o(l)
    loop(s0, k_o, k_o + 1)
    loop(g1, 0, n_dn)
    for i, l in enumerate(order):
        wg_qkv(l)
        if i == 1:
            loop(s1, k_o, k_o + 1)
        if i == 3:
            loop(g2, n_dn, 2 * n_dn)
    loop(s0, k_q, n_chunk)
    loop(s1, k_q, n_chunk)
    loop(lambda k: cs[0](k).wait_send())
    pl.semaphore_signal(free_sem, inc=1, device_id=(cp,), device_id_type=MESH)
    loop(g1, n_dn, 2 * n_dn)
    loop(s2, 2 * n_dn, n_chunk)
    pl.semaphore_wait(free_sem, 1)
    loop(g0, 0, n_dn)
    loop(lambda k: g2(k, False), 2 * n_dn, n_chunk)
    loop(g2_own, 2 * n_dn, n_chunk)
    loop(g0, n_dn, 2 * n_dn)
    loop(g1, 2 * n_dn, n_chunk)
    loop(g0, 2 * n_dn, n_chunk)
    loop(finish)


def store_kernel(acc, dx_ref, oq, ok, ov, oo, oup, odn, odx, sem):
    dm = acc.shape[1]
    n = odn.shape[0] // dm
    dst = ([odn.at[i * dm:(i + 1) * dm, :] for i in range(n)]
           + [oup.at[:, i * dm:(i + 1) * dm] for i in range(n)] + [oo, oq, ok, ov])
    cps = [pltpu.make_async_copy(acc.at[i], d, sem.at[i]) for i, d in enumerate(dst)]
    cps.append(pltpu.make_async_copy(dx_ref, odx, sem.at[len(dst)]))
    for cc in cps:
        cc.start()
    for cc in cps:
        cc.wait()


def solution(mesh):
    batch_spec = P('data', None, None)

    def per_device(x_loc, g_loc, step_emb, w_q, w_k, w_v, w_o, w_up, w_down):
        n_seq, seq, dm = x_loc.shape
        n_layers = step_emb.shape[0]
        n_heads, hd = w_q.shape[1:]
        ff = w_up.shape[1]
        tok = n_seq * seq
        n_pair = n_heads // 2
        n_chunk = 4 + 2 * (ff // dm)
        wts = [w.transpose(1, 2, 0).reshape(n_heads * hd, dm) for w in (w_q, w_k, w_v)]
        vm = pl.BlockSpec(memory_space=pltpu.VMEM)
        hb = pl.BlockSpec(memory_space=pl.ANY)
        acc, dx = pl.pallas_call(
            functools.partial(block_kernel, n_seq, seq, n_layers, n_heads),
            out_shape=(pltpu.VMEM((n_chunk, dm, dm), F32), pltpu.VMEM((tok, dm), BF16)),
            in_specs=[hb] * 9,
            out_specs=[vm] * 2,
            scratch_shapes=[
                pltpu.VMEM((dm, 3 * dm), BF16),
                pltpu.VMEM((3 * dm, dm), BF16),
                pltpu.VMEM((dm, dm), BF16),
                pltpu.VMEM((dm, dm), BF16),
                pltpu.VMEM((dm, ff), BF16),
                pltpu.VMEM((ff, dm), BF16),
                pltpu.VMEM((ff, dm), BF16),
                pltpu.VMEM((dm, ff), BF16),
                pltpu.VMEM((n_layers, 1, dm), F32),
                pltpu.VMEM((n_layers, dm), BF16),
                pltpu.VMEM((n_layers, tok, dm), BF16),
                pltpu.VMEM((n_layers, tok, 3 * dm), BF16),
                pltpu.VMEM((n_layers, n_seq * n_pair, 2 * seq, seq), F32),
                pltpu.VMEM((n_layers, tok, dm), BF16),
                pltpu.VMEM((n_layers, tok, dm), BF16),
                pltpu.VMEM((n_layers, tok, ff), BF16),
                pltpu.VMEM((tok, dm), BF16),
                pltpu.VMEM((tok, ff), BF16),
                pltpu.VMEM((2, tok, BLOCK), BF16),
                pltpu.VMEM((tok, dm), BF16),
                pltpu.VMEM((tok, dm), BF16),
                pltpu.VMEM((n_layers, tok, dm), BF16),
                pltpu.VMEM((n_seq * n_pair, 2 * seq, seq), BF16),
                pltpu.VMEM((n_chunk, dm // 2, dm), F32),
                pltpu.VMEM((n_chunk, dm // 8, dm), F32),
                pltpu.VMEM((n_chunk, dm // 8, dm), F32),
                pltpu.VMEM((n_chunk, dm // 16, dm), F32),
                pltpu.VMEM((n_chunk, dm // 16, dm), F32),
                pltpu.SemaphoreType.DMA((9,)),
                pltpu.SemaphoreType.DMA((12, n_chunk)),
                pltpu.SemaphoreType.DMA((12, n_chunk)),
                pltpu.SemaphoreType.REGULAR,
            ],
            compiler_params=pltpu.CompilerParams(
                collective_id=0, has_side_effects=True, vmem_limit_bytes=VMEM_LIMIT),
        )(x_loc.reshape(tok, dm), g_loc.reshape(tok, dm), step_emb,
          *wts, w_o.reshape(n_heads * hd, dm), w_up, w_down)
        sq = jax.ShapeDtypeStruct((dm, dm), F32)
        gq, gk, gv, go, gup, gdn, gx = pl.pallas_call(
            store_kernel,
            out_shape=(sq, sq, sq, sq, jax.ShapeDtypeStruct((dm, ff), F32), jax.ShapeDtypeStruct((ff, dm), F32),
                       jax.ShapeDtypeStruct((tok, dm), BF16)),
            in_specs=[vm] * 2,
            out_specs=[hb] * 7,
            scratch_shapes=[pltpu.SemaphoreType.DMA((n_chunk + 1,))],
            compiler_params=pltpu.CompilerParams(vmem_limit_bytes=2 ** 20),
        )(acc, dx)
        heads = [a.reshape(n_heads, hd, dm).transpose(2, 0, 1) for a in (gq, gk, gv)]
        return (*heads, go.reshape(n_heads, hd, dm), gup, gdn, gx.reshape(n_seq, seq, dm))

    return jax.shard_map(per_device, mesh=mesh, in_specs=(batch_spec, batch_spec, P(), P(), P(), P(), P(), P(), P()), out_specs=(P(), P(), P(), P(), P(), P(), batch_spec), check_vma=False)
```

```python
import functools
import math

import jax
import jax.numpy as jnp
from jax import lax
from jax.experimental import pallas as pl
from jax.experimental.pallas import tpu as pltpu
from jax.sharding import PartitionSpec as P

EPS = 1e-6
F32 = jnp.float32
BF16 = jnp.bfloat16
MESH = pl.DeviceIdType.MESH
LOG2E = math.log2(math.e)
GC0 = math.sqrt(2.0 / math.pi)
GC1 = GC0 * 0.044715
NT = (((1,), (1,)), ((), ()))
TN = (((0,), (0,)), ((), ()))
VMEM_LIMIT = 58851328
BLOCK = 256


def mm(a, b):
    return jnp.dot(a, b, preferred_element_type=F32)


def mmg(a, b, dims):
    return lax.dot_general(a, b, dims, preferred_element_type=F32)


def blocks(total, size):
    return [(s, min(size, total - s)) for s in range(0, total, size)]


def rms_scale(xf):
    return lax.rsqrt(jnp.mean(xf * xf, axis=-1, keepdims=True) + EPS)


def norm_back(xf, r, dy):
    inner = jnp.mean(xf * dy, axis=-1, keepdims=True)
    return dy * r - xf * (r * r * r * inner)


def merge(*streams):
    plan = []
    for si, (start, steps) in enumerate(streams):
        at = start
        for cost, fn in steps:
            plan.append((at, si, fn))
            at += cost
    for _, _, fn in sorted(plan, key=lambda e: e[:2]):
        fn()


def block_kernel(n_seq, seq, n_layers, n_heads,
                 x_hbm, g_hbm, emb_hbm, wq_hbm, wk_hbm, wv_hbm, wo_hbm, wup_hbm, wdn_hbm,
                 acc, dx_ref,
                 wqkv_s, wqkvt_s, wo_s, wot_s, wup_s, wupt_s, wdn_s, wdnt_s, emb_s, embb_s,
                 x_s, qkv_s, p_s, mix_s, h_s, z_s,
                 u_s, g_s, da_s, dn_s, d_s, dmid_s, st_s,
                 r0, ra, rb, ra2, rb2, in_sem, ssem, rsem, free_sem):
    tok, dm = d_s.shape
    ff = wup_s.shape[1]
    fb = blocks(ff, BLOCK)
    hd = dm // n_heads
    pw = 2 * hd
    n_pair = n_heads // 2
    n_dn = ff // dm
    n_chunk = 2 * n_dn + 4
    k_o, k_q = 2 * n_dn, 2 * n_dn + 1
    scale = hd ** -0.5
    NB = BLOCK
    rows = blocks(tok, 64)
    rows_b = blocks(tok, 32)

    me = lax.axis_index('data')
    c = lax.rem(me, 2)
    x = lax.rem(lax.div(me, 2), 2)
    y = lax.div(me, 4)
    cp = me + 1 - 2 * c
    xp = me + 2 - 4 * x
    yp = me + 4 - 8 * y
    barrier = pltpu.get_barrier_semaphore()
    for p in (cp, xp, yp):
        pl.semaphore_signal(barrier, inc=1, device_id=(p,), device_id_type=MESH)

    loads = [pltpu.make_async_copy(src, dst, in_sem.at[i]) for i, (src, dst) in enumerate((
        (wq_hbm, wqkvt_s.at[0:dm, :]), (wk_hbm, wqkvt_s.at[dm:2 * dm, :]), (wv_hbm, wqkvt_s.at[2 * dm:3 * dm, :]),
        (x_hbm, d_s), (wo_hbm, wo_s), (wup_hbm, wup_s), (wdn_hbm, wdn_s), (g_hbm, dmid_s.at[0]), (emb_hbm, embb_s)))]
    for ld in loads:
        ld.start()
    acc[0:n_dn] = jnp.zeros((n_dn, dm, dm), F32)
    for i in range(3):
        loads[i].wait()
        wqkv_s[:, i * dm:(i + 1) * dm] = wqkvt_s[i * dm:(i + 1) * dm, :].T
    for ld in loads[3:]:
        ld.wait()
    emb = embb_s[...].astype(F32)
    for l in range(n_layers):
        emb_s[l] = emb[l:l + 1]
    wot_s[...] = wo_s[...].T

    low = lax.broadcasted_iota(jnp.int32, (seq, pw), 1) < hd

    def stack(a):
        zero = jnp.zeros_like(a)
        return jnp.concatenate([jnp.where(low, a, zero), jnp.where(low, zero, a)], axis=0)

    def halves(a):
        return a[:seq], a[seq:]

    def beside(a):
        return jnp.concatenate(halves(a), axis=1)

    def seq_rows(s):
        return slice(s * seq, (s + 1) * seq)

    hrows = tok // 2
    hseq = n_seq // 2

    def sub_rows(h, rb):
        return [slice(h * hrows + r_0, h * hrows + r_0 + rn) for r_0, rn in blocks(hrows, rb)]

    def col_blocks(n):
        return [slice(n0, n0 + nn) for n0, nn in blocks(n, NB)]

    def fwd_half(l, h):
        hr = slice(h * hrows, (h + 1) * hrows)
        emb_l = emb_s[l]
        steps = []

        def start(rs):
            xb = (d_s[rs, :].astype(F32) + emb_l).astype(BF16)
            x_s[l, rs, :] = xb
            xf = xb.astype(F32)
            u_s[rs, :] = (xf * rms_scale(xf)).astype(BF16)

        def qkv(ns):
            qkv_s[l, hr, ns] = mm(u_s[hr, :], wqkv_s[:, ns]).astype(BF16)

        def scores(s, j):
            rs = seq_rows(s)
            cc = j * pw
            k = stack(qkv_s[l, rs, dm + cc:dm + cc + pw])
            st_s[s * n_pair + j] = mmg(k, qkv_s[l, rs, cc:cc + pw], NT).astype(BF16)

        def soft(s, j):
            for i, half in enumerate(halves(st_s[s * n_pair + j])):
                sf = half.astype(F32)
                top = jnp.max(sf, axis=0, keepdims=True)
                e = jnp.exp2((sf - top) * (scale * LOG2E))
                pr = e * (1.0 / jnp.sum(e, axis=0, keepdims=True))
                p_s[l, s * n_pair + j, i * seq:(i + 1) * seq, :] = pr

        def mix(s, j):
            rs = seq_rows(s)
            cc = j * pw
            v = stack(qkv_s[l, rs, 2 * dm + cc:2 * dm + cc + pw])
            pb = p_s[l, s * n_pair + j].astype(BF16)
            mix_s[l, rs, cc:cc + pw] = mmg(pb, v, TN).astype(BF16)

        def out(ns):
            o = mm(mix_s[l, hr, :], wo_s[:, ns]).astype(BF16)
            h_s[l, hr, ns] = (x_s[l, hr, ns].astype(F32) + o.astype(F32)).astype(BF16)

        def norm2(rs):
            hf = h_s[l, rs, :].astype(F32)
            u_s[rs, :] = (hf * rms_scale(hf)).astype(BF16)

        def up(ns):
            z_s[l, hr, ns] = mm(u_s[hr, :], wup_s[:, ns]).astype(BF16)

        def gelu(rs, ns):
            z = z_s[l, rs, ns].astype(F32)
            cdf = 0.5 + 0.5 * jnp.tanh(z * (GC0 + GC1 * (z * z)))
            g_s[rs, ns] = (z * cdf).astype(BF16)

        def down(ns):
            yd = mm(g_s[hr, :], wdn_s[:, ns]).astype(BF16)
            d_s[hr, ns] = (h_s[l, hr, ns].astype(F32) + yd.astype(F32)).astype(BF16)

        def step(cost, fn, *args):
            steps.append((cost, functools.partial(fn, *args)))

        for rs in sub_rows(h, 64):
            step(60, start, rs)
        for ns in col_blocks(3 * dm):
            step(120, qkv, ns)
        pairs = [(h * hseq + s, j) for s in range(hseq) for j in range(n_pair)]
        for t in range(len(pairs) + 3):
            if t < len(pairs):
                step(40, scores, *pairs[t])
            if 1 <= t <= len(pairs):
                step(70, soft, *pairs[t - 1])
            if t >= 3:
                step(50, mix, *pairs[t - 3])
        for ns in [slice(0, dm)]:
            step(100, out, ns)
        for rs in sub_rows(h, 64):
            step(70, norm2, rs)
        cols = col_blocks(ff)
        step(100, up, cols[0])
        for i, ns in enumerate(cols):
            if i + 1 < len(cols):
                step(120, up, cols[i + 1])
            for rs in sub_rows(h, 64):
                step(38, gelu, rs, ns)
        for ns in [slice(0, dm)]:
            step(380, down, ns)
        return steps

    def fwd(l, carry):
        tl = ff // n_layers
        ts = pl.ds(pl.multiple_of(l * tl, tl), tl)

        def wt():
            wupt_s[ts, :] = wup_s[:, ts].T
            wdnt_s[:, ts] = wdn_s[ts, :].T

        merge((0, fwd_half(l, 0)), (700, fwd_half(l, 1)), (2500, [(1, wt)]))
        return carry

    lax.fori_loop(0, n_layers, fwd, 0)
    d_s[...] = dmid_s[0]

    def gelu_phase(l, after, lag=1):
        def dact(i):
            n0, nn = fb[i]
            da_s[i % 2] = mm(d_s[...], wdnt_s[:, n0:n0 + nn]).astype(BF16)

        def gelu_back(i):
            n0, nn = fb[i]
            ns = slice(n0, n0 + nn)
            for r_0, rn in blocks(tok, 32):
                rs = slice(r_0, r_0 + rn)
                z = z_s[l, rs, ns].astype(F32)
                z2 = z * z
                cdf = 0.5 + 0.5 * jnp.tanh(z * (GC0 + GC1 * z2))
                g = z * cdf
                g_s[rs, ns] = g.astype(BF16)
                dg = cdf + (g * (1.0 - cdf)) * (2.0 * GC0 + 6.0 * GC1 * z2)
                z_s[l, rs, ns] = (da_s[i % 2, rs, :].astype(F32) * dg).astype(BF16)

        def wg_down(i):
            n0, nn = fb[i]
            res = mmg(g_s[:, n0:n0 + nn], d_s[...], TN)
            for t in range(0, nn, 128):
                r = n0 + t
                acc[r // dm, r % dm:r % dm + 128, :] += res[t:t + 128]

        dact(0)
        for i in range(len(fb)):
            if i + 1 < len(fb):
                dact(i + 1)
            gelu_back(i)
            if i >= lag:
                wg_down(i - lag)
                after(i - lag)
        for i in range(len(fb) - lag, len(fb)):
            wg_down(i)
            after(i)

    def mid_phase(l):
        for n0, nn in blocks(dm, dm):
            ns = slice(n0, n0 + nn)
            dn_s[:, ns] = mm(z_s[l], wupt_s[:, ns]).astype(BF16)
        for r_0, rn in blocks(tok, 32):
            rs = slice(r_0, r_0 + rn)
            hf = h_s[l, rs, :].astype(F32)
            r = rms_scale(hf)
            dh = norm_back(hf, r, dn_s[rs, :].astype(F32)).astype(BF16)
            h_s[l, rs, :] = (hf * r).astype(BF16)
            dmid_s[l, rs, :] = (d_s[rs, :].astype(F32) + dh.astype(F32)).astype(BF16)

    def attn_phase(l):
        for n0, nn in blocks(dm, dm):
            ns = slice(n0, n0 + nn)
            dn_s[:tok // 2, ns] = mm(dmid_s[l, :tok // 2], wot_s[:, ns]).astype(BF16)
        for n0, nn in blocks(dm, dm):
            ns = slice(n0, n0 + nn)
            dn_s[tok // 2:, ns] = mm(dmid_s[l, tok // 2:], wot_s[:, ns]).astype(BF16)

        def dprob(s, j):
            rs = seq_rows(s)
            cc = j * pw
            v = stack(qkv_s[l, rs, 2 * dm + cc:2 * dm + cc + pw])
            st_s[s * n_pair + j] = mmg(v, dn_s[rs, cc:cc + pw], NT).astype(BF16)

        def dscore(s, j):
            i = s * n_pair + j
            for hh in range(2):
                hs = slice(hh * seq, (hh + 1) * seq)
                pf = p_s[l, i, hs, :]
                dp = st_s[i, hs, :].astype(F32)
                inner = jnp.sum(pf * dp, axis=0, keepdims=True)
                st_s[i, hs, :] = (pf * (dp - inner) * scale).astype(BF16)

        def dqkv(s, j):
            rs = seq_rows(s)
            i = s * n_pair + j
            cc = j * pw
            dst = st_s[i]
            q = stack(qkv_s[l, rs, cc:cc + pw])
            k = stack(qkv_s[l, rs, dm + cc:dm + cc + pw])
            dmx = stack(dn_s[rs, cc:cc + pw])
            qkv_s[l, rs, cc:cc + pw] = mmg(dst, k, TN).astype(BF16)
            qkv_s[l, rs, dm + cc:dm + cc + pw] = mm(beside(dst), q).astype(BF16)
            pb = p_s[l, i].astype(BF16)
            qkv_s[l, rs, 2 * dm + cc:2 * dm + cc + pw] = mm(beside(pb), dmx).astype(BF16)

        pairs = [(s, j) for s in range(n_seq) for j in range(n_pair)]
        for t in range(len(pairs) + 4):
            if t < len(pairs):
                dprob(*pairs[t])
            if 1 <= t < len(pairs) + 1:
                dscore(*pairs[t - 1])
            if t >= 4:
                dqkv(*pairs[t - 4])

    def in_phase(l):
        for n0, nn in blocks(dm, dm):
            ns = slice(n0, n0 + nn)
            dn_s[:tok // 2, ns] = mm(qkv_s[l, :tok // 2], wqkvt_s[:, ns]).astype(BF16)
        for n0, nn in blocks(dm, dm):
            ns = slice(n0, n0 + nn)
            dn_s[tok // 2:, ns] = mm(qkv_s[l, tok // 2:], wqkvt_s[:, ns]).astype(BF16)
        for r_0, rn in blocks(tok, 32):
            rs = slice(r_0, r_0 + rn)
            xf = x_s[l, rs, :].astype(F32)
            r = rms_scale(xf)
            dh = norm_back(xf, r, dn_s[rs, :].astype(F32)).astype(BF16)
            x_s[l, rs, :] = (xf * r).astype(BF16)
            d_s[rs, :] = (dmid_s[l, rs, :].astype(F32) + dh.astype(F32)).astype(BF16)

    def bwd_body(i, carry):
        l = n_layers - 1 - i
        gelu_phase(l, lambda n: None)
        mid_phase(l)
        attn_phase(l)
        in_phase(l)
        return carry

    lax.fori_loop(0, n_layers - 1, bwd_body, 0)
    pl.semaphore_wait(barrier, 3)

    h0, h1, h2, h3 = dm // 2, dm // 4, dm // 8, dm // 16
    own = c * h0
    oth = (1 - c) * h0
    a0, a0n = own + x * h2, own + (1 - x) * h2
    b0, b0n = own + h1 + y * h2, own + h1 + (1 - y) * h2
    a1, a1n = a0 + y * h3, a0 + (1 - y) * h3
    b1, b1n = b0 + x * h3, b0 + (1 - x) * h3

    def part(k, off, n):
        return acc.at[k, pl.ds(pl.multiple_of(off, 8), n), :]

    def send(j, src, dst, dev):
        def at(k):
            return pltpu.make_async_remote_copy(
                src_ref=src(k), dst_ref=dst(k), send_sem=ssem.at[j, k], recv_sem=rsem.at[j, k],
                device_id=(dev,), device_id_type=MESH)
        return at

    def rows_of(off, n):
        return lambda k: part(k, off, n)

    def slot(ref, n):
        return lambda k: ref.at[k, 0:n, :]

    cs = [
        send(0, rows_of(oth, h0), slot(r0, h0), cp),
        send(1, rows_of(a0n, h2), slot(ra, h2), xp),
        send(2, rows_of(b0n, h2), slot(rb, h2), yp),
        send(3, rows_of(a1n, h3), slot(ra2, h3), yp),
        send(4, rows_of(b1n, h3), slot(rb2, h3), xp),
        send(5, rows_of(a1, h3), slot(ra, h3), yp),
        send(6, rows_of(b1, h3), slot(rb, h3), xp),
        send(7, rows_of(a1, h3), rows_of(a1, h3), xp),
        send(8, rows_of(b1, h3), rows_of(b1, h3), yp),
        send(9, slot(ra, h3), rows_of(a1n, h3), xp),
        send(10, slot(rb, h3), rows_of(b1n, h3), yp),
        send(11, rows_of(own, h0), rows_of(own, h0), cp),
    ]

    def add(k, off, n, src):
        sl = pl.ds(pl.multiple_of(off, 8), n)
        acc[k, sl, :] = acc[k, sl, :] + src[k]

    def loop(fn, lo=0, hi=n_chunk):
        lax.fori_loop(lo, hi, lambda k, t: (fn(k), t)[1], 0)

    def s0(k):
        cs[0](k).start()

    def s1(k):
        cs[0](k).wait_recv()
        add(k, own, h0, r0)
        cs[1](k).start()
        cs[2](k).start()

    def s2(k):
        cs[1](k).wait()
        add(k, a0, h2, ra)
        cs[2](k).wait()
        add(k, b0, h2, rb)
        cs[3](k).start()
        cs[4](k).start()

    def g2(k, both=True):
        cs[3](k).wait_recv()
        add(k, a1, h3, ra2)
        cs[4](k).wait_recv()
        add(k, b1, h3, rb2)
        for j in (5, 6, 7, 8) if both else (5, 6):
            cs[j](k).start()

    def g2_own(k):
        cs[7](k).start()
        cs[8](k).start()

    def g1(k):
        cs[5](k).wait_recv()
        cs[9](k).start()
        cs[6](k).wait_recv()
        cs[10](k).start()
        cs[3](k).wait_send()
        acc[k, pl.ds(pl.multiple_of(a1n, 8), h3), :] = ra[k, 0:h3, :]
        cs[4](k).wait_send()
        acc[k, pl.ds(pl.multiple_of(b1n, 8), h3), :] = rb[k, 0:h3, :]

    def g0(k):
        for j in (7, 8, 9, 10):
            cs[j](k).wait_recv()
        cs[11](k).start()

    def finish(k):
        cs[11](k).wait_recv()
        for j in range(5, 12):
            cs[j](k).wait_send()

    first = n_layers - 1

    def put(l, k, sl, val):
        if l == first:
            acc[(k, *sl)] = val
        else:
            acc[(k, *sl)] += val

    def wg_up(l, m):
        for n0, nn in fb:
            res = mmg(m, z_s[l, :, n0:n0 + nn], TN)
            for t in range(0, nn, 128):
                r = n0 + t
                put(l, n_dn + r // dm, (slice(None), slice(r % dm, r % dm + 128)), res[:, t:t + 128])

    def wg_o(l):
        put(l, k_o, (slice(None), slice(None)), mmg(mix_s[l], dmid_s[l], TN))

    def wg_qkv(l):
        for i in range(3):
            put(l, k_q + i, (slice(None), slice(None)), mmg(qkv_s[l, :, i * dm:(i + 1) * dm], x_s[l], TN))

    def after(i):
        done = min((i + 1) * BLOCK // dm, n_dn)
        prev = i * BLOCK // dm
        for k in range(prev, done):
            s0(k)
        if i == len(fb) - 1:
            s1(0)

    gelu_phase(0, after, 0)
    for r_0, rn in rows:
        rs = slice(r_0, r_0 + rn)
        hf = h_s[0, rs, :].astype(F32)
        u_s[rs, :] = (hf * rms_scale(hf)).astype(BF16)
    s1(1)
    order = list(range(first, -1, -1))
    for i, l in enumerate(order):
        wg_up(l, h_s[l] if l else u_s[...])
        if i == 0:
            loop(s1, 2, n_dn)
        if i >= 3:
            loop(s2, i - 3, i - 2)
    loop(s0, n_dn, 2 * n_dn)
    loop(s2, 3, n_dn)
    mid_phase(0)
    loop(s1, n_dn, 2 * n_dn)
    attn_phase(0)
    loop(g2, 0, n_dn)
    in_phase(0)
    dx_ref[...] = d_s[...]
    loop(s2, n_dn, 2 * n_dn)
    for l in order:
        wg_o(l)
    loop(s0, k_o, k_o + 1)
    loop(g1, 0, n_dn)
    for i, l in enumerate(order):
        wg_qkv(l)
        if i == 1:
            loop(s1, k_o, k_o + 1)
        if i == 3:
            loop(g2, n_dn, 2 * n_dn)
    loop(s0, k_q, n_chunk)
    loop(s1, k_q, n_chunk)
    loop(lambda k: cs[0](k).wait_send())
    pl.semaphore_signal(free_sem, inc=1, device_id=(cp,), device_id_type=MESH)
    loop(g1, n_dn, 2 * n_dn)
    loop(s2, 2 * n_dn, n_chunk)
    pl.semaphore_wait(free_sem, 1)
    loop(g0, 0, n_dn)
    loop(lambda k: g2(k, False), 2 * n_dn, n_chunk)
    loop(g2_own, 2 * n_dn, n_chunk)
    loop(g0, n_dn, 2 * n_dn)
    loop(g1, 2 * n_dn, n_chunk)
    loop(g0, 2 * n_dn, n_chunk)
    loop(finish)


def store_kernel(acc, dx_ref, oq, ok, ov, oo, oup, odn, odx, sem):
    dm = acc.shape[1]
    n = odn.shape[0] // dm
    dst = ([odn.at[i * dm:(i + 1) * dm, :] for i in range(n)]
           + [oup.at[:, i * dm:(i + 1) * dm] for i in range(n)] + [oo, oq, ok, ov])
    cps = [pltpu.make_async_copy(acc.at[i], d, sem.at[i]) for i, d in enumerate(dst)]
    cps.append(pltpu.make_async_copy(dx_ref, odx, sem.at[len(dst)]))
    for cc in cps:
        cc.start()
    for cc in cps:
        cc.wait()


def solution(mesh):
    batch_spec = P('data', None, None)

    def per_device(x_loc, g_loc, step_emb, w_q, w_k, w_v, w_o, w_up, w_down):
        n_seq, seq, dm = x_loc.shape
        n_layers = step_emb.shape[0]
        n_heads, hd = w_q.shape[1:]
        ff = w_up.shape[1]
        tok = n_seq * seq
        n_pair = n_heads // 2
        n_chunk = 4 + 2 * (ff // dm)
        wts = [w.transpose(1, 2, 0).reshape(n_heads * hd, dm) for w in (w_q, w_k, w_v)]
        vm = pl.BlockSpec(memory_space=pltpu.VMEM)
        hb = pl.BlockSpec(memory_space=pl.ANY)
        acc, dx = pl.pallas_call(
            functools.partial(block_kernel, n_seq, seq, n_layers, n_heads),
            out_shape=(pltpu.VMEM((n_chunk, dm, dm), F32), pltpu.VMEM((tok, dm), BF16)),
            in_specs=[hb] * 9,
            out_specs=[vm] * 2,
            scratch_shapes=[
                pltpu.VMEM((dm, 3 * dm), BF16),
                pltpu.VMEM((3 * dm, dm), BF16),
                pltpu.VMEM((dm, dm), BF16),
                pltpu.VMEM((dm, dm), BF16),
                pltpu.VMEM((dm, ff), BF16),
                pltpu.VMEM((ff, dm), BF16),
                pltpu.VMEM((ff, dm), BF16),
                pltpu.VMEM((dm, ff), BF16),
                pltpu.VMEM((n_layers, 1, dm), F32),
                pltpu.VMEM((n_layers, dm), BF16),
                pltpu.VMEM((n_layers, tok, dm), BF16),
                pltpu.VMEM((n_layers, tok, 3 * dm), BF16),
                pltpu.VMEM((n_layers, n_seq * n_pair, 2 * seq, seq), F32),
                pltpu.VMEM((n_layers, tok, dm), BF16),
                pltpu.VMEM((n_layers, tok, dm), BF16),
                pltpu.VMEM((n_layers, tok, ff), BF16),
                pltpu.VMEM((tok, dm), BF16),
                pltpu.VMEM((tok, ff), BF16),
                pltpu.VMEM((2, tok, BLOCK), BF16),
                pltpu.VMEM((tok, dm), BF16),
                pltpu.VMEM((tok, dm), BF16),
                pltpu.VMEM((n_layers, tok, dm), BF16),
                pltpu.VMEM((n_seq * n_pair, 2 * seq, seq), BF16),
                pltpu.VMEM((n_chunk, dm // 2, dm), F32),
                pltpu.VMEM((n_chunk, dm // 8, dm), F32),
                pltpu.VMEM((n_chunk, dm // 8, dm), F32),
                pltpu.VMEM((n_chunk, dm // 16, dm), F32),
                pltpu.VMEM((n_chunk, dm // 16, dm), F32),
                pltpu.SemaphoreType.DMA((9,)),
                pltpu.SemaphoreType.DMA((12, n_chunk)),
                pltpu.SemaphoreType.DMA((12, n_chunk)),
                pltpu.SemaphoreType.REGULAR,
            ],
            compiler_params=pltpu.CompilerParams(
                collective_id=0, has_side_effects=True, vmem_limit_bytes=VMEM_LIMIT),
        )(x_loc.reshape(tok, dm), g_loc.reshape(tok, dm), step_emb,
          *wts, w_o.reshape(n_heads * hd, dm), w_up, w_down)
        sq = jax.ShapeDtypeStruct((dm, dm), F32)
        gq, gk, gv, go, gup, gdn, gx = pl.pallas_call(
            store_kernel,
            out_shape=(sq, sq, sq, sq, jax.ShapeDtypeStruct((dm, ff), F32), jax.ShapeDtypeStruct((ff, dm), F32),
                       jax.ShapeDtypeStruct((tok, dm), BF16)),
            in_specs=[vm] * 2,
            out_specs=[hb] * 7,
            scratch_shapes=[pltpu.SemaphoreType.DMA((n_chunk + 1,))],
            compiler_params=pltpu.CompilerParams(vmem_limit_bytes=2 ** 20),
        )(acc, dx)
        heads = [a.reshape(n_heads, hd, dm).transpose(2, 0, 1) for a in (gq, gk, gv)]
        return (*heads, go.reshape(n_heads, hd, dm), gup, gdn, gx.reshape(n_seq, seq, dm))

    return jax.shard_map(per_device, mesh=mesh, in_specs=(batch_spec, batch_spec, P(), P(), P(), P(), P(), P(), P()), out_specs=(P(), P(), P(), P(), P(), P(), batch_spec), check_vma=False)
```

```python
import functools
import math

import jax
import jax.numpy as jnp
from jax import lax
from jax.experimental import pallas as pl
from jax.experimental.pallas import tpu as pltpu
from jax.sharding import PartitionSpec as P

EPS = 1e-6
F32 = jnp.float32
BF16 = jnp.bfloat16
MESH = pl.DeviceIdType.MESH
LOG2E = math.log2(math.e)
GC0 = math.sqrt(2.0 / math.pi)
GC1 = GC0 * 0.044715
NT = (((1,), (1,)), ((), ()))
TN = (((0,), (0,)), ((), ()))
VMEM_LIMIT = 58851328
BLOCK = 512


def mm(a, b):
    return jnp.dot(a, b, preferred_element_type=F32)


def mmg(a, b, dims):
    return lax.dot_general(a, b, dims, preferred_element_type=F32)


def blocks(total, size):
    return [(s, min(size, total - s)) for s in range(0, total, size)]


def rms_scale(xf):
    return lax.rsqrt(jnp.mean(xf * xf, axis=-1, keepdims=True) + EPS)


def norm_back(xf, r, dy):
    inner = jnp.mean(xf * dy, axis=-1, keepdims=True)
    return dy * r - xf * (r * r * r * inner)


def merge(*streams):
    plan = []
    for si, (start, steps) in enumerate(streams):
        at = start
        for cost, fn in steps:
            plan.append((at, si, fn))
            at += cost
    for _, _, fn in sorted(plan, key=lambda e: e[:2]):
        fn()


def block_kernel(n_seq, seq, n_layers, n_heads,
                 x_hbm, g_hbm, emb_hbm, wq_hbm, wk_hbm, wv_hbm, wo_hbm, wup_hbm, wdn_hbm,
                 acc, dx_ref,
                 wqkv_s, wqkvt_s, wo_s, wot_s, wup_s, wupt_s, wdn_s, wdnt_s, emb_s, embb_s,
                 x_s, qkv_s, p_s, mix_s, h_s, z_s,
                 u_s, g_s, da_s, dn_s, d_s, dmid_s, st_s,
                 r0, ra, rb, ra2, rb2, in_sem, ssem, rsem, free_sem):
    tok, dm = d_s.shape
    ff = wup_s.shape[1]
    fb = blocks(ff, BLOCK)
    hd = dm // n_heads
    pw = 2 * hd
    n_pair = n_heads // 2
    n_dn = ff // dm
    n_chunk = 2 * n_dn + 4
    k_o, k_q = 2 * n_dn, 2 * n_dn + 1
    scale = hd ** -0.5
    NB = 256
    rows = blocks(tok, 64)
    rows_b = blocks(tok, 32)

    me = lax.axis_index('data')
    c = lax.rem(me, 2)
    x = lax.rem(lax.div(me, 2), 2)
    y = lax.div(me, 4)
    cp = me + 1 - 2 * c
    xp = me + 2 - 4 * x
    yp = me + 4 - 8 * y
    barrier = pltpu.get_barrier_semaphore()
    for p in (cp, xp, yp):
        pl.semaphore_signal(barrier, inc=1, device_id=(p,), device_id_type=MESH)

    loads = [pltpu.make_async_copy(src, dst, in_sem.at[i]) for i, (src, dst) in enumerate((
        (wq_hbm, wqkvt_s.at[0:dm, :]), (wk_hbm, wqkvt_s.at[dm:2 * dm, :]), (wv_hbm, wqkvt_s.at[2 * dm:3 * dm, :]),
        (x_hbm, d_s), (wo_hbm, wo_s), (wup_hbm, wup_s), (wdn_hbm, wdn_s), (g_hbm, dmid_s.at[0]), (emb_hbm, embb_s)))]
    for ld in loads:
        ld.start()
    acc[0:n_dn] = jnp.zeros((n_dn, dm, dm), F32)
    for i in range(3):
        loads[i].wait()
        wqkv_s[:, i * dm:(i + 1) * dm] = wqkvt_s[i * dm:(i + 1) * dm, :].T
    for ld in loads[3:]:
        ld.wait()
    emb = embb_s[...].astype(F32)
    for l in range(n_layers):
        emb_s[l] = emb[l:l + 1]
    wot_s[...] = wo_s[...].T

    low = lax.broadcasted_iota(jnp.int32, (seq, pw), 1) < hd

    def stack(a):
        zero = jnp.zeros_like(a)
        return jnp.concatenate([jnp.where(low, a, zero), jnp.where(low, zero, a)], axis=0)

    def halves(a):
        return a[:seq], a[seq:]

    def beside(a):
        return jnp.concatenate(halves(a), axis=1)

    def seq_rows(s):
        return slice(s * seq, (s + 1) * seq)

    hrows = tok // 2
    hseq = n_seq // 2

    def sub_rows(h, rb):
        return [slice(h * hrows + r_0, h * hrows + r_0 + rn) for r_0, rn in blocks(hrows, rb)]

    def col_blocks(n):
        return [slice(n0, n0 + nn) for n0, nn in blocks(n, NB)]

    def fwd_half(l, h):
        hr = slice(h * hrows, (h + 1) * hrows)
        emb_l = emb_s[l]
        steps = []

        def start(rs):
            xb = (d_s[rs, :].astype(F32) + emb_l).astype(BF16)
            x_s[l, rs, :] = xb
            xf = xb.astype(F32)
            u_s[rs, :] = (xf * rms_scale(xf)).astype(BF16)

        def qkv(ns):
            qkv_s[l, hr, ns] = mm(u_s[hr, :], wqkv_s[:, ns]).astype(BF16)

        def scores(s, j):
            rs = seq_rows(s)
            cc = j * pw
            k = stack(qkv_s[l, rs, dm + cc:dm + cc + pw])
            st_s[s * n_pair + j] = mmg(k, qkv_s[l, rs, cc:cc + pw], NT).astype(BF16)

        def soft(s, j):
            for i, half in enumerate(halves(st_s[s * n_pair + j])):
                sf = half.astype(F32)
                top = jnp.max(sf, axis=0, keepdims=True)
                e = jnp.exp2((sf - top) * (scale * LOG2E))
                pr = e * (1.0 / jnp.sum(e, axis=0, keepdims=True))
                p_s[l, s * n_pair + j, i * seq:(i + 1) * seq, :] = pr

        def mix(s, j):
            rs = seq_rows(s)
            cc = j * pw
            v = stack(qkv_s[l, rs, 2 * dm + cc:2 * dm + cc + pw])
            pb = p_s[l, s * n_pair + j].astype(BF16)
            mix_s[l, rs, cc:cc + pw] = mmg(pb, v, TN).astype(BF16)

        def out(ns):
            o = mm(mix_s[l, hr, :], wo_s[:, ns]).astype(BF16)
            h_s[l, hr, ns] = (x_s[l, hr, ns].astype(F32) + o.astype(F32)).astype(BF16)

        def norm2(rs):
            hf = h_s[l, rs, :].astype(F32)
            u_s[rs, :] = (hf * rms_scale(hf)).astype(BF16)

        def up(ns):
            z_s[l, hr, ns] = mm(u_s[hr, :], wup_s[:, ns]).astype(BF16)

        def gelu(rs, ns):
            z = z_s[l, rs, ns].astype(F32)
            cdf = 0.5 + 0.5 * jnp.tanh(z * (GC0 + GC1 * (z * z)))
            g_s[rs, ns] = (z * cdf).astype(BF16)

        def down(ns):
            yd = mm(g_s[hr, :], wdn_s[:, ns]).astype(BF16)
            d_s[hr, ns] = (h_s[l, hr, ns].astype(F32) + yd.astype(F32)).astype(BF16)

        def step(cost, fn, *args):
            steps.append((cost, functools.partial(fn, *args)))

        for rs in sub_rows(h, 64):
            step(60, start, rs)
        for ns in col_blocks(3 * dm):
            step(120, qkv, ns)
        pairs = [(h * hseq + s, j) for s in range(hseq) for j in range(n_pair)]
        for t in range(len(pairs) + 3):
            if t < len(pairs):
                step(40, scores, *pairs[t])
            if 1 <= t <= len(pairs):
                step(70, soft, *pairs[t - 1])
            if t >= 3:
                step(50, mix, *pairs[t - 3])
        for ns in [slice(0, dm)]:
            step(100, out, ns)
        for rs in sub_rows(h, 64):
            step(70, norm2, rs)
        cols = col_blocks(ff)
        step(100, up, cols[0])
        for i, ns in enumerate(cols):
            if i + 1 < len(cols):
                step(120, up, cols[i + 1])
            for rs in sub_rows(h, 64):
                step(38, gelu, rs, ns)
        for ns in [slice(0, dm)]:
            step(380, down, ns)
        return steps

    def fwd(l, carry):
        tl = ff // n_layers
        ts = pl.ds(pl.multiple_of(l * tl, tl), tl)

        def wt():
            wupt_s[ts, :] = wup_s[:, ts].T
            wdnt_s[:, ts] = wdn_s[ts, :].T

        merge((0, fwd_half(l, 0)), (700, fwd_half(l, 1)), (2500, [(1, wt)]))
        return carry

    lax.fori_loop(0, n_layers, fwd, 0)
    d_s[...] = dmid_s[0]

    def gelu_phase(l, after, lag=1):
        def dact(i):
            n0, nn = fb[i]
            da_s[i % 2] = mm(d_s[...], wdnt_s[:, n0:n0 + nn]).astype(BF16)

        def gelu_back(i):
            n0, nn = fb[i]
            ns = slice(n0, n0 + nn)
            for r_0, rn in blocks(tok, 32):
                rs = slice(r_0, r_0 + rn)
                z = z_s[l, rs, ns].astype(F32)
                z2 = z * z
                cdf = 0.5 + 0.5 * jnp.tanh(z * (GC0 + GC1 * z2))
                g = z * cdf
                g_s[rs, ns] = g.astype(BF16)
                dg = cdf + (g * (1.0 - cdf)) * (2.0 * GC0 + 6.0 * GC1 * z2)
                z_s[l, rs, ns] = (da_s[i % 2, rs, :].astype(F32) * dg).astype(BF16)

        def wg_down(i):
            n0, nn = fb[i]
            res = mmg(g_s[:, n0:n0 + nn], d_s[...], TN)
            for t in range(0, nn, 128):
                r = n0 + t
                acc[r // dm, r % dm:r % dm + 128, :] += res[t:t + 128]

        dact(0)
        for i in range(len(fb)):
            if i + 1 < len(fb):
                dact(i + 1)
            gelu_back(i)
            if i >= lag:
                wg_down(i - lag)
                after(i - lag)
        for i in range(len(fb) - lag, len(fb)):
            wg_down(i)
            after(i)

    def mid_phase(l):
        for n0, nn in blocks(dm, dm):
            ns = slice(n0, n0 + nn)
            dn_s[:, ns] = mm(z_s[l], wupt_s[:, ns]).astype(BF16)
        for r_0, rn in blocks(tok, 32):
            rs = slice(r_0, r_0 + rn)
            hf = h_s[l, rs, :].astype(F32)
            r = rms_scale(hf)
            dh = norm_back(hf, r, dn_s[rs, :].astype(F32)).astype(BF16)
            h_s[l, rs, :] = (hf * r).astype(BF16)
            dmid_s[l, rs, :] = (d_s[rs, :].astype(F32) + dh.astype(F32)).astype(BF16)

    def attn_phase(l):
        for n0, nn in blocks(dm, dm):
            ns = slice(n0, n0 + nn)
            dn_s[:tok // 2, ns] = mm(dmid_s[l, :tok // 2], wot_s[:, ns]).astype(BF16)
        for n0, nn in blocks(dm, dm):
            ns = slice(n0, n0 + nn)
            dn_s[tok // 2:, ns] = mm(dmid_s[l, tok // 2:], wot_s[:, ns]).astype(BF16)

        def dprob(s, j):
            rs = seq_rows(s)
            cc = j * pw
            v = stack(qkv_s[l, rs, 2 * dm + cc:2 * dm + cc + pw])
            st_s[s * n_pair + j] = mmg(v, dn_s[rs, cc:cc + pw], NT).astype(BF16)

        def dscore(s, j):
            i = s * n_pair + j
            for hh in range(2):
                hs = slice(hh * seq, (hh + 1) * seq)
                pf = p_s[l, i, hs, :]
                dp = st_s[i, hs, :].astype(F32)
                inner = jnp.sum(pf * dp, axis=0, keepdims=True)
                st_s[i, hs, :] = (pf * (dp - inner) * scale).astype(BF16)

        def dqkv(s, j):
            rs = seq_rows(s)
            i = s * n_pair + j
            cc = j * pw
            dst = st_s[i]
            q = stack(qkv_s[l, rs, cc:cc + pw])
            k = stack(qkv_s[l, rs, dm + cc:dm + cc + pw])
            dmx = stack(dn_s[rs, cc:cc + pw])
            qkv_s[l, rs, cc:cc + pw] = mmg(dst, k, TN).astype(BF16)
            qkv_s[l, rs, dm + cc:dm + cc + pw] = mm(beside(dst), q).astype(BF16)
            pb = p_s[l, i].astype(BF16)
            qkv_s[l, rs, 2 * dm + cc:2 * dm + cc + pw] = mm(beside(pb), dmx).astype(BF16)

        pairs = [(s, j) for s in range(n_seq) for j in range(n_pair)]
        for t in range(len(pairs) + 4):
            if t < len(pairs):
                dprob(*pairs[t])
            if 1 <= t < len(pairs) + 1:
                dscore(*pairs[t - 1])
            if t >= 4:
                dqkv(*pairs[t - 4])

    def in_phase(l):
        for n0, nn in blocks(dm, dm):
            ns = slice(n0, n0 + nn)
            dn_s[:tok // 2, ns] = mm(qkv_s[l, :tok // 2], wqkvt_s[:, ns]).astype(BF16)
        for n0, nn in blocks(dm, dm):
            ns = slice(n0, n0 + nn)
            dn_s[tok // 2:, ns] = mm(qkv_s[l, tok // 2:], wqkvt_s[:, ns]).astype(BF16)
        for r_0, rn in blocks(tok, 32):
            rs = slice(r_0, r_0 + rn)
            xf = x_s[l, rs, :].astype(F32)
            r = rms_scale(xf)
            dh = norm_back(xf, r, dn_s[rs, :].astype(F32)).astype(BF16)
            x_s[l, rs, :] = (xf * r).astype(BF16)
            d_s[rs, :] = (dmid_s[l, rs, :].astype(F32) + dh.astype(F32)).astype(BF16)

    def bwd_body(i, carry):
        l = n_layers - 1 - i
        gelu_phase(l, lambda n: None)
        mid_phase(l)
        attn_phase(l)
        in_phase(l)
        return carry

    lax.fori_loop(0, n_layers - 1, bwd_body, 0)
    pl.semaphore_wait(barrier, 3)

    h0, h1, h2, h3 = dm // 2, dm // 4, dm // 8, dm // 16
    own = c * h0
    oth = (1 - c) * h0
    a0, a0n = own + x * h2, own + (1 - x) * h2
    b0, b0n = own + h1 + y * h2, own + h1 + (1 - y) * h2
    a1, a1n = a0 + y * h3, a0 + (1 - y) * h3
    b1, b1n = b0 + x * h3, b0 + (1 - x) * h3

    def part(k, off, n):
        return acc.at[k, pl.ds(pl.multiple_of(off, 8), n), :]

    def send(j, src, dst, dev):
        def at(k):
            return pltpu.make_async_remote_copy(
                src_ref=src(k), dst_ref=dst(k), send_sem=ssem.at[j, k], recv_sem=rsem.at[j, k],
                device_id=(dev,), device_id_type=MESH)
        return at

    def rows_of(off, n):
        return lambda k: part(k, off, n)

    def slot(ref, n):
        return lambda k: ref.at[k, 0:n, :]

    cs = [
        send(0, rows_of(oth, h0), slot(r0, h0), cp),
        send(1, rows_of(a0n, h2), slot(ra, h2), xp),
        send(2, rows_of(b0n, h2), slot(rb, h2), yp),
        send(3, rows_of(a1n, h3), slot(ra2, h3), yp),
        send(4, rows_of(b1n, h3), slot(rb2, h3), xp),
        send(5, rows_of(a1, h3), slot(ra, h3), yp),
        send(6, rows_of(b1, h3), slot(rb, h3), xp),
        send(7, rows_of(a1, h3), rows_of(a1, h3), xp),
        send(8, rows_of(b1, h3), rows_of(b1, h3), yp),
        send(9, slot(ra, h3), rows_of(a1n, h3), xp),
        send(10, slot(rb, h3), rows_of(b1n, h3), yp),
        send(11, rows_of(own, h0), rows_of(own, h0), cp),
    ]

    def add(k, off, n, src):
        sl = pl.ds(pl.multiple_of(off, 8), n)
        acc[k, sl, :] = acc[k, sl, :] + src[k]

    def loop(fn, lo=0, hi=n_chunk):
        lax.fori_loop(lo, hi, lambda k, t: (fn(k), t)[1], 0)

    def s0(k):
        cs[0](k).start()

    def s1(k):
        cs[0](k).wait_recv()
        add(k, own, h0, r0)
        cs[1](k).start()
        cs[2](k).start()

    def s2(k):
        cs[1](k).wait()
        add(k, a0, h2, ra)
        cs[2](k).wait()
        add(k, b0, h2, rb)
        cs[3](k).start()
        cs[4](k).start()

    def g2(k, both=True):
        cs[3](k).wait_recv()
        add(k, a1, h3, ra2)
        cs[4](k).wait_recv()
        add(k, b1, h3, rb2)
        for j in (5, 6, 7, 8) if both else (5, 6):
            cs[j](k).start()

    def g2_own(k):
        cs[7](k).start()
        cs[8](k).start()

    def g1(k):
        cs[5](k).wait_recv()
        cs[9](k).start()
        cs[6](k).wait_recv()
        cs[10](k).start()
        cs[3](k).wait_send()
        acc[k, pl.ds(pl.multiple_of(a1n, 8), h3), :] = ra[k, 0:h3, :]
        cs[4](k).wait_send()
        acc[k, pl.ds(pl.multiple_of(b1n, 8), h3), :] = rb[k, 0:h3, :]

    def g0(k):
        for j in (7, 8, 9, 10):
            cs[j](k).wait_recv()
        cs[11](k).start()

    def finish(k):
        cs[11](k).wait_recv()
        for j in range(5, 12):
            cs[j](k).wait_send()

    first = n_layers - 1

    def put(l, k, sl, val):
        if l == first:
            acc[(k, *sl)] = val
        else:
            acc[(k, *sl)] += val

    def wg_up(l, m):
        for n0, nn in fb:
            res = mmg(m, z_s[l, :, n0:n0 + nn], TN)
            for t in range(0, nn, 128):
                r = n0 + t
                put(l, n_dn + r // dm, (slice(None), slice(r % dm, r % dm + 128)), res[:, t:t + 128])

    def wg_o(l):
        put(l, k_o, (slice(None), slice(None)), mmg(mix_s[l], dmid_s[l], TN))

    def wg_qkv(l):
        for i in range(3):
            put(l, k_q + i, (slice(None), slice(None)), mmg(qkv_s[l, :, i * dm:(i + 1) * dm], x_s[l], TN))

    def after(i):
        done = min((i + 1) * BLOCK // dm, n_dn)
        prev = i * BLOCK // dm
        for k in range(prev, done):
            s0(k)
        if i == len(fb) - 1:
            s1(0)

    gelu_phase(0, after, 0)
    for r_0, rn in rows:
        rs = slice(r_0, r_0 + rn)
        hf = h_s[0, rs, :].astype(F32)
        u_s[rs, :] = (hf * rms_scale(hf)).astype(BF16)
    s1(1)
    order = list(range(first, -1, -1))
    for i, l in enumerate(order):
        wg_up(l, h_s[l] if l else u_s[...])
        if i == 0:
            loop(s1, 2, n_dn)
        if i >= 3:
            loop(s2, i - 3, i - 2)
    loop(s0, n_dn, 2 * n_dn)
    loop(s2, 3, n_dn)
    mid_phase(0)
    loop(s1, n_dn, 2 * n_dn)
    attn_phase(0)
    loop(g2, 0, n_dn)
    in_phase(0)
    dx_ref[...] = d_s[...]
    loop(s2, n_dn, 2 * n_dn)
    for l in order:
        wg_o(l)
    loop(s0, k_o, k_o + 1)
    loop(g1, 0, n_dn)
    for i, l in enumerate(order):
        wg_qkv(l)
        if i == 1:
            loop(s1, k_o, k_o + 1)
        if i == 3:
            loop(g2, n_dn, 2 * n_dn)
    loop(s0, k_q, n_chunk)
    loop(s1, k_q, n_chunk)
    loop(lambda k: cs[0](k).wait_send())
    pl.semaphore_signal(free_sem, inc=1, device_id=(cp,), device_id_type=MESH)
    loop(g1, n_dn, 2 * n_dn)
    loop(s2, 2 * n_dn, n_chunk)
    pl.semaphore_wait(free_sem, 1)
    loop(g0, 0, n_dn)
    loop(lambda k: g2(k, False), 2 * n_dn, n_chunk)
    loop(g2_own, 2 * n_dn, n_chunk)
    loop(g0, n_dn, 2 * n_dn)
    loop(g1, 2 * n_dn, n_chunk)
    loop(g0, 2 * n_dn, n_chunk)
    loop(finish)


def store_kernel(acc, dx_ref, oq, ok, ov, oo, oup, odn, odx, sem):
    dm = acc.shape[1]
    n = odn.shape[0] // dm
    dst = ([odn.at[i * dm:(i + 1) * dm, :] for i in range(n)]
           + [oup.at[:, i * dm:(i + 1) * dm] for i in range(n)] + [oo, oq, ok, ov])
    cps = [pltpu.make_async_copy(acc.at[i], d, sem.at[i]) for i, d in enumerate(dst)]
    cps.append(pltpu.make_async_copy(dx_ref, odx, sem.at[len(dst)]))
    for cc in cps:
        cc.start()
    for cc in cps:
        cc.wait()


def solution(mesh):
    batch_spec = P('data', None, None)

    def per_device(x_loc, g_loc, step_emb, w_q, w_k, w_v, w_o, w_up, w_down):
        n_seq, seq, dm = x_loc.shape
        n_layers = step_emb.shape[0]
        n_heads, hd = w_q.shape[1:]
        ff = w_up.shape[1]
        tok = n_seq * seq
        n_pair = n_heads // 2
        n_chunk = 4 + 2 * (ff // dm)
        wts = [w.transpose(1, 2, 0).reshape(n_heads * hd, dm) for w in (w_q, w_k, w_v)]
        vm = pl.BlockSpec(memory_space=pltpu.VMEM)
        hb = pl.BlockSpec(memory_space=pl.ANY)
        acc, dx = pl.pallas_call(
            functools.partial(block_kernel, n_seq, seq, n_layers, n_heads),
            out_shape=(pltpu.VMEM((n_chunk, dm, dm), F32), pltpu.VMEM((tok, dm), BF16)),
            in_specs=[hb] * 9,
            out_specs=[vm] * 2,
            scratch_shapes=[
                pltpu.VMEM((dm, 3 * dm), BF16),
                pltpu.VMEM((3 * dm, dm), BF16),
                pltpu.VMEM((dm, dm), BF16),
                pltpu.VMEM((dm, dm), BF16),
                pltpu.VMEM((dm, ff), BF16),
                pltpu.VMEM((ff, dm), BF16),
                pltpu.VMEM((ff, dm), BF16),
                pltpu.VMEM((dm, ff), BF16),
                pltpu.VMEM((n_layers, 1, dm), F32),
                pltpu.VMEM((n_layers, dm), BF16),
                pltpu.VMEM((n_layers, tok, dm), BF16),
                pltpu.VMEM((n_layers, tok, 3 * dm), BF16),
                pltpu.VMEM((n_layers, n_seq * n_pair, 2 * seq, seq), F32),
                pltpu.VMEM((n_layers, tok, dm), BF16),
                pltpu.VMEM((n_layers, tok, dm), BF16),
                pltpu.VMEM((n_layers, tok, ff), BF16),
                pltpu.VMEM((tok, dm), BF16),
                pltpu.VMEM((tok, ff), BF16),
                pltpu.VMEM((2, tok, BLOCK), BF16),
                pltpu.VMEM((tok, dm), BF16),
                pltpu.VMEM((tok, dm), BF16),
                pltpu.VMEM((n_layers, tok, dm), BF16),
                pltpu.VMEM((n_seq * n_pair, 2 * seq, seq), BF16),
                pltpu.VMEM((n_chunk, dm // 2, dm), F32),
                pltpu.VMEM((n_chunk, dm // 8, dm), F32),
                pltpu.VMEM((n_chunk, dm // 8, dm), F32),
                pltpu.VMEM((n_chunk, dm // 16, dm), F32),
                pltpu.VMEM((n_chunk, dm // 16, dm), F32),
                pltpu.SemaphoreType.DMA((9,)),
                pltpu.SemaphoreType.DMA((12, n_chunk)),
                pltpu.SemaphoreType.DMA((12, n_chunk)),
                pltpu.SemaphoreType.REGULAR,
            ],
            compiler_params=pltpu.CompilerParams(
                collective_id=0, has_side_effects=True, vmem_limit_bytes=VMEM_LIMIT),
        )(x_loc.reshape(tok, dm), g_loc.reshape(tok, dm), step_emb,
          *wts, w_o.reshape(n_heads * hd, dm), w_up, w_down)
        sq = jax.ShapeDtypeStruct((dm, dm), F32)
        gq, gk, gv, go, gup, gdn, gx = pl.pallas_call(
            store_kernel,
            out_shape=(sq, sq, sq, sq, jax.ShapeDtypeStruct((dm, ff), F32), jax.ShapeDtypeStruct((ff, dm), F32),
                       jax.ShapeDtypeStruct((tok, dm), BF16)),
            in_specs=[vm] * 2,
            out_specs=[hb] * 7,
            scratch_shapes=[pltpu.SemaphoreType.DMA((n_chunk + 1,))],
            compiler_params=pltpu.CompilerParams(vmem_limit_bytes=2 ** 20),
        )(acc, dx)
        heads = [a.reshape(n_heads, hd, dm).transpose(2, 0, 1) for a in (gq, gk, gv)]
        return (*heads, go.reshape(n_heads, hd, dm), gup, gdn, gx.reshape(n_seq, seq, dm))

    return jax.shard_map(per_device, mesh=mesh, in_specs=(batch_spec, batch_spec, P(), P(), P(), P(), P(), P(), P()), out_specs=(P(), P(), P(), P(), P(), P(), batch_spec), check_vma=False)
```

```python
import functools
import math

import jax
import jax.numpy as jnp
from jax import lax
from jax.experimental import pallas as pl
from jax.experimental.pallas import tpu as pltpu
from jax.sharding import PartitionSpec as P

EPS = 1e-6
F32 = jnp.float32
BF16 = jnp.bfloat16
MESH = pl.DeviceIdType.MESH
LOG2E = math.log2(math.e)
GC0 = math.sqrt(2.0 / math.pi)
GC1 = GC0 * 0.044715
NT = (((1,), (1,)), ((), ()))
TN = (((0,), (0,)), ((), ()))
VMEM_LIMIT = 58851328
BLOCK = 256


def mm(a, b):
    return jnp.dot(a, b, preferred_element_type=F32)


def mmg(a, b, dims):
    return lax.dot_general(a, b, dims, preferred_element_type=F32)


def blocks(total, size):
    return [(s, min(size, total - s)) for s in range(0, total, size)]


def rms_scale(xf):
    return lax.rsqrt(jnp.mean(xf * xf, axis=-1, keepdims=True) + EPS)


def norm_back(xf, r, dy):
    inner = jnp.mean(xf * dy, axis=-1, keepdims=True)
    return dy * r - xf * (r * r * r * inner)


def merge(*streams):
    plan = []
    for si, (start, steps) in enumerate(streams):
        at = start
        for cost, fn in steps:
            plan.append((at, si, fn))
            at += cost
    for _, _, fn in sorted(plan, key=lambda e: e[:2]):
        fn()


def block_kernel(n_seq, seq, n_layers, n_heads,
                 x_hbm, g_hbm, emb_hbm, wq_hbm, wk_hbm, wv_hbm, wo_hbm, wup_hbm, wdn_hbm,
                 acc, dx_ref,
                 wqkv_s, wqkvt_s, wo_s, wot_s, wup_s, wupt_s, wdn_s, wdnt_s, emb_s, embb_s,
                 x_s, qkv_s, p_s, mix_s, h_s, z_s,
                 u_s, g_s, da_s, dn_s, d_s, dmid_s, st_s,
                 r0, ra, rb, ra2, rb2, in_sem, ssem, rsem, free_sem):
    tok, dm = d_s.shape
    ff = wup_s.shape[1]
    fb = blocks(ff, BLOCK)
    hd = dm // n_heads
    pw = 2 * hd
    n_pair = n_heads // 2
    n_dn = ff // dm
    n_chunk = 2 * n_dn + 4
    k_o, k_q = 2 * n_dn, 2 * n_dn + 1
    scale = hd ** -0.5
    NB = BLOCK
    rows = blocks(tok, 64)
    rows_b = blocks(tok, 32)

    me = lax.axis_index('data')
    c = lax.rem(me, 2)
    x = lax.rem(lax.div(me, 2), 2)
    y = lax.div(me, 4)
    cp = me + 1 - 2 * c
    xp = me + 2 - 4 * x
    yp = me + 4 - 8 * y
    barrier = pltpu.get_barrier_semaphore()
    for p in (cp, xp, yp):
        pl.semaphore_signal(barrier, inc=1, device_id=(p,), device_id_type=MESH)

    loads = [pltpu.make_async_copy(src, dst, in_sem.at[i]) for i, (src, dst) in enumerate((
        (wq_hbm, wqkvt_s.at[0:dm, :]), (wk_hbm, wqkvt_s.at[dm:2 * dm, :]), (wv_hbm, wqkvt_s.at[2 * dm:3 * dm, :]),
        (x_hbm, d_s), (wo_hbm, wo_s), (wup_hbm, wup_s), (wdn_hbm, wdn_s), (g_hbm, dmid_s.at[0]), (emb_hbm, embb_s)))]
    for ld in loads:
        ld.start()
    acc[0:n_dn] = jnp.zeros((n_dn, dm, dm), F32)
    for i in range(3):
        loads[i].wait()
        wqkv_s[:, i * dm:(i + 1) * dm] = wqkvt_s[i * dm:(i + 1) * dm, :].T
    for ld in loads[3:]:
        ld.wait()
    emb = embb_s[...].astype(F32)
    for l in range(n_layers):
        emb_s[l] = emb[l:l + 1]
    wot_s[...] = wo_s[...].T

    low = lax.broadcasted_iota(jnp.int32, (seq, pw), 1) < hd

    def stack(a):
        zero = jnp.zeros_like(a)
        return jnp.concatenate([jnp.where(low, a, zero), jnp.where(low, zero, a)], axis=0)

    def halves(a):
        return a[:seq], a[seq:]

    def beside(a):
        return jnp.concatenate(halves(a), axis=1)

    def seq_rows(s):
        return slice(s * seq, (s + 1) * seq)

    hrows = tok // 2
    hseq = n_seq // 2

    def sub_rows(h, rb):
        return [slice(h * hrows + r_0, h * hrows + r_0 + rn) for r_0, rn in blocks(hrows, rb)]

    def col_blocks(n):
        return [slice(n0, n0 + nn) for n0, nn in blocks(n, NB)]

    def fwd_half(l, h):
        hr = slice(h * hrows, (h + 1) * hrows)
        emb_l = emb_s[l]
        steps = []

        def start(rs):
            xb = (d_s[rs, :].astype(F32) + emb_l).astype(BF16)
            x_s[l, rs, :] = xb
            xf = xb.astype(F32)
            u_s[rs, :] = (xf * rms_scale(xf)).astype(BF16)

        def qkv(ns):
            qkv_s[l, hr, ns] = mm(u_s[hr, :], wqkv_s[:, ns]).astype(BF16)

        def scores(s, j):
            rs = seq_rows(s)
            cc = j * pw
            k = stack(qkv_s[l, rs, dm + cc:dm + cc + pw])
            st_s[s * n_pair + j] = mmg(k, qkv_s[l, rs, cc:cc + pw], NT).astype(BF16)

        def soft(s, j):
            for i, half in enumerate(halves(st_s[s * n_pair + j])):
                sf = half.astype(F32)
                top = jnp.max(sf, axis=0, keepdims=True)
                e = jnp.exp2((sf - top) * (scale * LOG2E))
                pr = e * (1.0 / jnp.sum(e, axis=0, keepdims=True))
                p_s[l, s * n_pair + j, i * seq:(i + 1) * seq, :] = pr

        def mix(s, j):
            rs = seq_rows(s)
            cc = j * pw
            v = stack(qkv_s[l, rs, 2 * dm + cc:2 * dm + cc + pw])
            pb = p_s[l, s * n_pair + j].astype(BF16)
            mix_s[l, rs, cc:cc + pw] = mmg(pb, v, TN).astype(BF16)

        def out(ns):
            o = mm(mix_s[l, hr, :], wo_s[:, ns]).astype(BF16)
            h_s[l, hr, ns] = (x_s[l, hr, ns].astype(F32) + o.astype(F32)).astype(BF16)

        def norm2(rs):
            hf = h_s[l, rs, :].astype(F32)
            u_s[rs, :] = (hf * rms_scale(hf)).astype(BF16)

        def up(ns):
            z_s[l, hr, ns] = mm(u_s[hr, :], wup_s[:, ns]).astype(BF16)

        def gelu(rs, ns):
            z = z_s[l, rs, ns].astype(F32)
            cdf = 0.5 + 0.5 * jnp.tanh(z * (GC0 + GC1 * (z * z)))
            g_s[rs, ns] = (z * cdf).astype(BF16)

        def down(ns):
            yd = mm(g_s[hr, :], wdn_s[:, ns]).astype(BF16)
            d_s[hr, ns] = (h_s[l, hr, ns].astype(F32) + yd.astype(F32)).astype(BF16)

        def step(cost, fn, *args):
            steps.append((cost, functools.partial(fn, *args)))

        for rs in sub_rows(h, 64):
            step(60, start, rs)
        for ns in col_blocks(3 * dm):
            step(120, qkv, ns)
        pairs = [(h * hseq + s, j) for s in range(hseq) for j in range(n_pair)]
        for t in range(len(pairs) + 3):
            if t < len(pairs):
                step(40, scores, *pairs[t])
            if 1 <= t <= len(pairs):
                step(70, soft, *pairs[t - 1])
            if t >= 3:
                step(50, mix, *pairs[t - 3])
        for ns in [slice(0, dm)]:
            step(100, out, ns)
        for rs in sub_rows(h, 64):
            step(70, norm2, rs)
        cols = col_blocks(ff)
        step(100, up, cols[0])
        for i, ns in enumerate(cols):
            if i + 1 < len(cols):
                step(120, up, cols[i + 1])
            for rs in sub_rows(h, 64):
                step(38, gelu, rs, ns)
        for ns in [slice(0, dm)]:
            step(380, down, ns)
        return steps

    def fwd(l, carry):
        tl = ff // n_layers
        ts = pl.ds(pl.multiple_of(l * tl, tl), tl)

        def wt():
            wupt_s[ts, :] = wup_s[:, ts].T
            wdnt_s[:, ts] = wdn_s[ts, :].T

        merge((0, fwd_half(l, 0)), (700, fwd_half(l, 1)), (2500, [(1, wt)]))
        return carry

    lax.fori_loop(0, n_layers, fwd, 0)
    d_s[...] = dmid_s[0]

    def gelu_phase(l, after, lag=1):
        def dact(i):
            n0, nn = fb[i]
            da_s[i % 2] = mm(d_s[...], wdnt_s[:, n0:n0 + nn]).astype(BF16)

        def gelu_back(i):
            n0, nn = fb[i]
            ns = slice(n0, n0 + nn)
            for r_0, rn in blocks(tok, 32):
                rs = slice(r_0, r_0 + rn)
                z = z_s[l, rs, ns].astype(F32)
                z2 = z * z
                cdf = 0.5 + 0.5 * jnp.tanh(z * (GC0 + GC1 * z2))
                g = z * cdf
                g_s[rs, ns] = g.astype(BF16)
                dg = cdf + (g * (1.0 - cdf)) * (2.0 * GC0 + 6.0 * GC1 * z2)
                z_s[l, rs, ns] = (da_s[i % 2, rs, :].astype(F32) * dg).astype(BF16)

        def wg_down(i):
            n0, nn = fb[i]
            res = mmg(g_s[:, n0:n0 + nn], d_s[...], TN)
            for t in range(0, nn, 128):
                r = n0 + t
                acc[r // dm, r % dm:r % dm + 128, :] += res[t:t + 128]

        dact(0)
        for i in range(len(fb)):
            if i + 1 < len(fb):
                dact(i + 1)
            gelu_back(i)
            if i >= lag:
                wg_down(i - lag)
                after(i - lag)
        for i in range(len(fb) - lag, len(fb)):
            wg_down(i)
            after(i)

    def mid_phase(l):
        for n0, nn in blocks(dm, dm):
            ns = slice(n0, n0 + nn)
            dn_s[:, ns] = mm(z_s[l], wupt_s[:, ns]).astype(BF16)
        for r_0, rn in blocks(tok, 32):
            rs = slice(r_0, r_0 + rn)
            hf = h_s[l, rs, :].astype(F32)
            r = rms_scale(hf)
            dh = norm_back(hf, r, dn_s[rs, :].astype(F32)).astype(BF16)
            h_s[l, rs, :] = (hf * r).astype(BF16)
            dmid_s[l, rs, :] = (d_s[rs, :].astype(F32) + dh.astype(F32)).astype(BF16)

    def attn_phase(l):
        for n0, nn in blocks(dm, dm):
            ns = slice(n0, n0 + nn)
            dn_s[:tok // 2, ns] = mm(dmid_s[l, :tok // 2], wot_s[:, ns]).astype(BF16)
        for n0, nn in blocks(dm, dm):
            ns = slice(n0, n0 + nn)
            dn_s[tok // 2:, ns] = mm(dmid_s[l, tok // 2:], wot_s[:, ns]).astype(BF16)

        def dprob(s, j):
            rs = seq_rows(s)
            cc = j * pw
            v = stack(qkv_s[l, rs, 2 * dm + cc:2 * dm + cc + pw])
            st_s[s * n_pair + j] = mmg(v, dn_s[rs, cc:cc + pw], NT).astype(BF16)

        def dscore(s, j):
            i = s * n_pair + j
            for hh in range(2):
                hs = slice(hh * seq, (hh + 1) * seq)
                pf = p_s[l, i, hs, :]
                dp = st_s[i, hs, :].astype(F32)
                inner = jnp.sum(pf * dp, axis=0, keepdims=True)
                st_s[i, hs, :] = (pf * (dp - inner) * scale).astype(BF16)

        def dqkv(s, j):
            rs = seq_rows(s)
            i = s * n_pair + j
            cc = j * pw
            dst = st_s[i]
            q = stack(qkv_s[l, rs, cc:cc + pw])
            k = stack(qkv_s[l, rs, dm + cc:dm + cc + pw])
            dmx = stack(dn_s[rs, cc:cc + pw])
            qkv_s[l, rs, cc:cc + pw] = mmg(dst, k, TN).astype(BF16)
            qkv_s[l, rs, dm + cc:dm + cc + pw] = mm(beside(dst), q).astype(BF16)
            pb = p_s[l, i].astype(BF16)
            qkv_s[l, rs, 2 * dm + cc:2 * dm + cc + pw] = mm(beside(pb), dmx).astype(BF16)

        pairs = [(s, j) for s in range(n_seq) for j in range(n_pair)]
        for t in range(len(pairs) + 4):
            if t < len(pairs):
                dprob(*pairs[t])
            if 1 <= t < len(pairs) + 1:
                dscore(*pairs[t - 1])
            if t >= 4:
                dqkv(*pairs[t - 4])

    def in_phase(l):
        for n0, nn in blocks(dm, dm):
            ns = slice(n0, n0 + nn)
            dn_s[:tok // 2, ns] = mm(qkv_s[l, :tok // 2], wqkvt_s[:, ns]).astype(BF16)
        for n0, nn in blocks(dm, dm):
            ns = slice(n0, n0 + nn)
            dn_s[tok // 2:, ns] = mm(qkv_s[l, tok // 2:], wqkvt_s[:, ns]).astype(BF16)
        for r_0, rn in blocks(tok, 32):
            rs = slice(r_0, r_0 + rn)
            xf = x_s[l, rs, :].astype(F32)
            r = rms_scale(xf)
            dh = norm_back(xf, r, dn_s[rs, :].astype(F32)).astype(BF16)
            x_s[l, rs, :] = (xf * r).astype(BF16)
            d_s[rs, :] = (dmid_s[l, rs, :].astype(F32) + dh.astype(F32)).astype(BF16)

    def bwd_body(i, carry):
        l = n_layers - 1 - i
        gelu_phase(l, lambda n: None)
        mid_phase(l)
        attn_phase(l)
        in_phase(l)
        return carry

    lax.fori_loop(0, n_layers - 1, bwd_body, 0)
    pl.semaphore_wait(barrier, 3)

    h0, h1, h2, h3 = dm // 2, dm // 4, dm // 8, dm // 16
    own = c * h0
    oth = (1 - c) * h0
    a0, a0n = own + x * h2, own + (1 - x) * h2
    b0, b0n = own + h1 + y * h2, own + h1 + (1 - y) * h2
    a1, a1n = a0 + y * h3, a0 + (1 - y) * h3
    b1, b1n = b0 + x * h3, b0 + (1 - x) * h3

    def part(k, off, n):
        return acc.at[k, pl.ds(pl.multiple_of(off, 8), n), :]

    def send(j, src, dst, dev):
        def at(k):
            return pltpu.make_async_remote_copy(
                src_ref=src(k), dst_ref=dst(k), send_sem=ssem.at[j, k], recv_sem=rsem.at[j, k],
                device_id=(dev,), device_id_type=MESH)
        return at

    def rows_of(off, n):
        return lambda k: part(k, off, n)

    def slot(ref, n):
        return lambda k: ref.at[k, 0:n, :]

    cs = [
        send(0, rows_of(oth, h0), slot(r0, h0), cp),
        send(1, rows_of(a0n, h2), slot(ra, h2), xp),
        send(2, rows_of(b0n, h2), slot(rb, h2), yp),
        send(3, rows_of(a1n, h3), slot(ra2, h3), yp),
        send(4, rows_of(b1n, h3), slot(rb2, h3), xp),
        send(5, rows_of(a1, h3), slot(ra, h3), yp),
        send(6, rows_of(b1, h3), slot(rb, h3), xp),
        send(7, rows_of(a1, h3), rows_of(a1, h3), xp),
        send(8, rows_of(b1, h3), rows_of(b1, h3), yp),
        send(9, slot(ra, h3), rows_of(a1n, h3), xp),
        send(10, slot(rb, h3), rows_of(b1n, h3), yp),
        send(11, rows_of(own, h0), rows_of(own, h0), cp),
    ]

    def add(k, off, n, src):
        sl = pl.ds(pl.multiple_of(off, 8), n)
        acc[k, sl, :] = acc[k, sl, :] + src[k]

    def loop(fn, lo=0, hi=n_chunk):
        lax.fori_loop(lo, hi, lambda k, t: (fn(k), t)[1], 0)

    def s0(k):
        cs[0](k).start()

    def s1(k):
        cs[0](k).wait_recv()
        add(k, own, h0, r0)
        cs[1](k).start()
        cs[2](k).start()

    def s2(k):
        cs[1](k).wait()
        add(k, a0, h2, ra)
        cs[2](k).wait()
        add(k, b0, h2, rb)
        cs[3](k).start()
        cs[4](k).start()

    def g2(k, both=True):
        cs[3](k).wait_recv()
        add(k, a1, h3, ra2)
        cs[4](k).wait_recv()
        add(k, b1, h3, rb2)
        for j in (5, 6, 7, 8) if both else (5, 6):
            cs[j](k).start()

    def g2_own(k):
        cs[7](k).start()
        cs[8](k).start()

    def g1(k):
        cs[5](k).wait_recv()
        cs[9](k).start()
        cs[6](k).wait_recv()
        cs[10](k).start()
        cs[3](k).wait_send()
        acc[k, pl.ds(pl.multiple_of(a1n, 8), h3), :] = ra[k, 0:h3, :]
        cs[4](k).wait_send()
        acc[k, pl.ds(pl.multiple_of(b1n, 8), h3), :] = rb[k, 0:h3, :]

    def g0(k):
        for j in (7, 8, 9, 10):
            cs[j](k).wait_recv()
        cs[11](k).start()

    def finish(k):
        cs[11](k).wait_recv()
        for j in range(5, 12):
            cs[j](k).wait_send()

    first = n_layers - 1

    def put(l, k, sl, val):
        if l == first:
            acc[(k, *sl)] = val
        else:
            acc[(k, *sl)] += val

    def wg_up(l, m):
        for n0, nn in fb:
            res = mmg(m, z_s[l, :, n0:n0 + nn], TN)
            for t in range(0, nn, 128):
                r = n0 + t
                put(l, n_dn + r // dm, (slice(None), slice(r % dm, r % dm + 128)), res[:, t:t + 128])

    def wg_o(l):
        put(l, k_o, (slice(None), slice(None)), mmg(mix_s[l], dmid_s[l], TN))

    def wg_qkv(l):
        for i in range(3):
            put(l, k_q + i, (slice(None), slice(None)), mmg(qkv_s[l, :, i * dm:(i + 1) * dm], x_s[l], TN))

    def after(i):
        done = min((i + 1) * BLOCK // dm, n_dn)
        prev = i * BLOCK // dm
        for k in range(prev, done):
            s0(k)
        if i == len(fb) - 1:
            s1(0)

    gelu_phase(0, after, 1)
    for r_0, rn in rows:
        rs = slice(r_0, r_0 + rn)
        hf = h_s[0, rs, :].astype(F32)
        u_s[rs, :] = (hf * rms_scale(hf)).astype(BF16)
    s1(1)
    order = list(range(first, -1, -1))
    for i, l in enumerate(order):
        wg_up(l, h_s[l] if l else u_s[...])
        if i == 0:
            loop(s1, 2, n_dn)
        if i >= 3:
            loop(s2, i - 3, i - 2)
    loop(s0, n_dn, 2 * n_dn)
    loop(s2, 3, n_dn)
    mid_phase(0)
    loop(s1, n_dn, 2 * n_dn)
    attn_phase(0)
    loop(g2, 0, n_dn)
    in_phase(0)
    dx_ref[...] = d_s[...]
    loop(s2, n_dn, 2 * n_dn)
    for l in order:
        wg_o(l)
    loop(s0, k_o, k_o + 1)
    loop(g1, 0, n_dn)
    for i, l in enumerate(order):
        wg_qkv(l)
        if i == 1:
            loop(s1, k_o, k_o + 1)
        if i == 3:
            loop(g2, n_dn, 2 * n_dn)
    loop(s0, k_q, n_chunk)
    loop(s1, k_q, n_chunk)
    loop(lambda k: cs[0](k).wait_send())
    pl.semaphore_signal(free_sem, inc=1, device_id=(cp,), device_id_type=MESH)
    loop(g1, n_dn, 2 * n_dn)
    loop(s2, 2 * n_dn, n_chunk)
    pl.semaphore_wait(free_sem, 1)
    loop(g0, 0, n_dn)
    loop(lambda k: g2(k, False), 2 * n_dn, n_chunk)
    loop(g2_own, 2 * n_dn, n_chunk)
    loop(g0, n_dn, 2 * n_dn)
    loop(g1, 2 * n_dn, n_chunk)
    loop(g0, 2 * n_dn, n_chunk)
    loop(finish)


def store_kernel(acc, dx_ref, oq, ok, ov, oo, oup, odn, odx, sem):
    dm = acc.shape[1]
    n = odn.shape[0] // dm
    dst = ([odn.at[i * dm:(i + 1) * dm, :] for i in range(n)]
           + [oup.at[:, i * dm:(i + 1) * dm] for i in range(n)] + [oo, oq, ok, ov])
    cps = [pltpu.make_async_copy(acc.at[i], d, sem.at[i]) for i, d in enumerate(dst)]
    cps.append(pltpu.make_async_copy(dx_ref, odx, sem.at[len(dst)]))
    for cc in cps:
        cc.start()
    for cc in cps:
        cc.wait()


def solution(mesh):
    batch_spec = P('data', None, None)

    def per_device(x_loc, g_loc, step_emb, w_q, w_k, w_v, w_o, w_up, w_down):
        n_seq, seq, dm = x_loc.shape
        n_layers = step_emb.shape[0]
        n_heads, hd = w_q.shape[1:]
        ff = w_up.shape[1]
        tok = n_seq * seq
        n_pair = n_heads // 2
        n_chunk = 4 + 2 * (ff // dm)
        wts = [w.transpose(1, 2, 0).reshape(n_heads * hd, dm) for w in (w_q, w_k, w_v)]
        vm = pl.BlockSpec(memory_space=pltpu.VMEM)
        hb = pl.BlockSpec(memory_space=pl.ANY)
        acc, dx = pl.pallas_call(
            functools.partial(block_kernel, n_seq, seq, n_layers, n_heads),
            out_shape=(pltpu.VMEM((n_chunk, dm, dm), F32), pltpu.VMEM((tok, dm), BF16)),
            in_specs=[hb] * 9,
            out_specs=[vm] * 2,
            scratch_shapes=[
                pltpu.VMEM((dm, 3 * dm), BF16),
                pltpu.VMEM((3 * dm, dm), BF16),
                pltpu.VMEM((dm, dm), BF16),
                pltpu.VMEM((dm, dm), BF16),
                pltpu.VMEM((dm, ff), BF16),
                pltpu.VMEM((ff, dm), BF16),
                pltpu.VMEM((ff, dm), BF16),
                pltpu.VMEM((dm, ff), BF16),
                pltpu.VMEM((n_layers, 1, dm), F32),
                pltpu.VMEM((n_layers, dm), BF16),
                pltpu.VMEM((n_layers, tok, dm), BF16),
                pltpu.VMEM((n_layers, tok, 3 * dm), BF16),
                pltpu.VMEM((n_layers, n_seq * n_pair, 2 * seq, seq), F32),
                pltpu.VMEM((n_layers, tok, dm), BF16),
                pltpu.VMEM((n_layers, tok, dm), BF16),
                pltpu.VMEM((n_layers, tok, ff), BF16),
                pltpu.VMEM((tok, dm), BF16),
                pltpu.VMEM((tok, ff), BF16),
                pltpu.VMEM((2, tok, BLOCK), BF16),
                pltpu.VMEM((tok, dm), BF16),
                pltpu.VMEM((tok, dm), BF16),
                pltpu.VMEM((n_layers, tok, dm), BF16),
                pltpu.VMEM((n_seq * n_pair, 2 * seq, seq), BF16),
                pltpu.VMEM((n_chunk, dm // 2, dm), F32),
                pltpu.VMEM((n_chunk, dm // 8, dm), F32),
                pltpu.VMEM((n_chunk, dm // 8, dm), F32),
                pltpu.VMEM((n_chunk, dm // 16, dm), F32),
                pltpu.VMEM((n_chunk, dm // 16, dm), F32),
                pltpu.SemaphoreType.DMA((9,)),
                pltpu.SemaphoreType.DMA((12, n_chunk)),
                pltpu.SemaphoreType.DMA((12, n_chunk)),
                pltpu.SemaphoreType.REGULAR,
            ],
            compiler_params=pltpu.CompilerParams(
                collective_id=0, has_side_effects=True, vmem_limit_bytes=VMEM_LIMIT),
        )(x_loc.reshape(tok, dm), g_loc.reshape(tok, dm), step_emb,
          *wts, w_o.reshape(n_heads * hd, dm), w_up, w_down)
        sq = jax.ShapeDtypeStruct((dm, dm), F32)
        gq, gk, gv, go, gup, gdn, gx = pl.pallas_call(
            store_kernel,
            out_shape=(sq, sq, sq, sq, jax.ShapeDtypeStruct((dm, ff), F32), jax.ShapeDtypeStruct((ff, dm), F32),
                       jax.ShapeDtypeStruct((tok, dm), BF16)),
            in_specs=[vm] * 2,
            out_specs=[hb] * 7,
            scratch_shapes=[pltpu.SemaphoreType.DMA((n_chunk + 1,))],
            compiler_params=pltpu.CompilerParams(vmem_limit_bytes=2 ** 20),
        )(acc, dx)
        heads = [a.reshape(n_heads, hd, dm).transpose(2, 0, 1) for a in (gq, gk, gv)]
        return (*heads, go.reshape(n_heads, hd, dm), gup, gdn, gx.reshape(n_seq, seq, dm))

    return jax.shard_map(per_device, mesh=mesh, in_specs=(batch_spec, batch_spec, P(), P(), P(), P(), P(), P(), P()), out_specs=(P(), P(), P(), P(), P(), P(), batch_spec), check_vma=False)
```

```python
import functools
import math

import jax
import jax.numpy as jnp
from jax import lax
from jax.experimental import pallas as pl
from jax.experimental.pallas import tpu as pltpu
from jax.sharding import PartitionSpec as P

EPS = 1e-6
F32 = jnp.float32
BF16 = jnp.bfloat16
MESH = pl.DeviceIdType.MESH
LOG2E = math.log2(math.e)
GC0 = math.sqrt(2.0 / math.pi)
GC1 = GC0 * 0.044715
NT = (((1,), (1,)), ((), ()))
TN = (((0,), (0,)), ((), ()))
VMEM_LIMIT = 58851328
BLOCK = 256


def mm(a, b):
    return jnp.dot(a, b, preferred_element_type=F32)


def mmg(a, b, dims):
    return lax.dot_general(a, b, dims, preferred_element_type=F32)


def blocks(total, size):
    return [(s, min(size, total - s)) for s in range(0, total, size)]


def rms_scale(xf):
    return lax.rsqrt(jnp.mean(xf * xf, axis=-1, keepdims=True) + EPS)


def norm_back(xf, r, dy):
    inner = jnp.mean(xf * dy, axis=-1, keepdims=True)
    return dy * r - xf * (r * r * r * inner)


def merge(*streams):
    plan = []
    for si, (start, steps) in enumerate(streams):
        at = start
        for cost, fn in steps:
            plan.append((at, si, fn))
            at += cost
    for _, _, fn in sorted(plan, key=lambda e: e[:2]):
        fn()


def block_kernel(n_seq, seq, n_layers, n_heads,
                 x_hbm, g_hbm, emb_hbm, wq_hbm, wk_hbm, wv_hbm, wo_hbm, wup_hbm, wdn_hbm,
                 acc, dx_ref,
                 wqkv_s, wqkvt_s, wo_s, wot_s, wup_s, wupt_s, wdn_s, wdnt_s, emb_s, embb_s,
                 x_s, qkv_s, p_s, mix_s, h_s, z_s,
                 u_s, g_s, da_s, dn_s, d_s, dmid_s, st_s,
                 r0, ra, rb, ra2, rb2, in_sem, ssem, rsem, free_sem):
    tok, dm = d_s.shape
    ff = wup_s.shape[1]
    fb = blocks(ff, BLOCK)
    hd = dm // n_heads
    pw = 2 * hd
    n_pair = n_heads // 2
    n_dn = ff // dm
    n_chunk = 2 * n_dn + 4
    k_o, k_q = 2 * n_dn, 2 * n_dn + 1
    scale = hd ** -0.5
    NB = BLOCK
    rows = blocks(tok, 64)
    rows_b = blocks(tok, 32)

    me = lax.axis_index('data')
    c = lax.rem(me, 2)
    x = lax.rem(lax.div(me, 2), 2)
    y = lax.div(me, 4)
    cp = me + 1 - 2 * c
    xp = me + 2 - 4 * x
    yp = me + 4 - 8 * y
    barrier = pltpu.get_barrier_semaphore()
    for p in (cp, xp, yp):
        pl.semaphore_signal(barrier, inc=1, device_id=(p,), device_id_type=MESH)

    loads = [pltpu.make_async_copy(src, dst, in_sem.at[i]) for i, (src, dst) in enumerate((
        (wq_hbm, wqkvt_s.at[0:dm, :]), (wk_hbm, wqkvt_s.at[dm:2 * dm, :]), (wv_hbm, wqkvt_s.at[2 * dm:3 * dm, :]),
        (x_hbm, d_s), (emb_hbm, embb_s), (wo_hbm, wo_s), (wup_hbm, wup_s), (wdn_hbm, wdn_s), (g_hbm, dmid_s.at[0])))]
    for ld in loads:
        ld.start()
    acc[0:n_dn] = jnp.zeros((n_dn, dm, dm), F32)
    for i in range(3):
        loads[i].wait()
        wqkv_s[:, i * dm:(i + 1) * dm] = wqkvt_s[i * dm:(i + 1) * dm, :].T
    for ld in loads[3:-1]:
        ld.wait()
    emb = embb_s[...].astype(F32)
    for l in range(n_layers):
        emb_s[l] = emb[l:l + 1]
    wot_s[...] = wo_s[...].T

    low = lax.broadcasted_iota(jnp.int32, (seq, pw), 1) < hd

    def stack(a):
        zero = jnp.zeros_like(a)
        return jnp.concatenate([jnp.where(low, a, zero), jnp.where(low, zero, a)], axis=0)

    def halves(a):
        return a[:seq], a[seq:]

    def beside(a):
        return jnp.concatenate(halves(a), axis=1)

    def seq_rows(s):
        return slice(s * seq, (s + 1) * seq)

    hrows = tok // 2
    hseq = n_seq // 2

    def sub_rows(h, rb):
        return [slice(h * hrows + r_0, h * hrows + r_0 + rn) for r_0, rn in blocks(hrows, rb)]

    def col_blocks(n):
        return [slice(n0, n0 + nn) for n0, nn in blocks(n, NB)]

    def fwd_half(l, h):
        hr = slice(h * hrows, (h + 1) * hrows)
        emb_l = emb_s[l]
        steps = []

        def start(rs):
            xb = (d_s[rs, :].astype(F32) + emb_l).astype(BF16)
            x_s[l, rs, :] = xb
            xf = xb.astype(F32)
            u_s[rs, :] = (xf * rms_scale(xf)).astype(BF16)

        def qkv(ns):
            qkv_s[l, hr, ns] = mm(u_s[hr, :], wqkv_s[:, ns]).astype(BF16)

        def scores(s, j):
            rs = seq_rows(s)
            cc = j * pw
            k = stack(qkv_s[l, rs, dm + cc:dm + cc + pw])
            st_s[s * n_pair + j] = mmg(k, qkv_s[l, rs, cc:cc + pw], NT).astype(BF16)

        def soft(s, j):
            for i, half in enumerate(halves(st_s[s * n_pair + j])):
                sf = half.astype(F32)
                top = jnp.max(sf, axis=0, keepdims=True)
                e = jnp.exp2((sf - top) * (scale * LOG2E))
                pr = e * (1.0 / jnp.sum(e, axis=0, keepdims=True))
                p_s[l, s * n_pair + j, i * seq:(i + 1) * seq, :] = pr

        def mix(s, j):
            rs = seq_rows(s)
            cc = j * pw
            v = stack(qkv_s[l, rs, 2 * dm + cc:2 * dm + cc + pw])
            pb = p_s[l, s * n_pair + j].astype(BF16)
            mix_s[l, rs, cc:cc + pw] = mmg(pb, v, TN).astype(BF16)

        def out(ns):
            o = mm(mix_s[l, hr, :], wo_s[:, ns]).astype(BF16)
            h_s[l, hr, ns] = (x_s[l, hr, ns].astype(F32) + o.astype(F32)).astype(BF16)

        def norm2(rs):
            hf = h_s[l, rs, :].astype(F32)
            u_s[rs, :] = (hf * rms_scale(hf)).astype(BF16)

        def up(ns):
            z_s[l, hr, ns] = mm(u_s[hr, :], wup_s[:, ns]).astype(BF16)

        def gelu(rs, ns):
            z = z_s[l, rs, ns].astype(F32)
            cdf = 0.5 + 0.5 * jnp.tanh(z * (GC0 + GC1 * (z * z)))
            g_s[rs, ns] = (z * cdf).astype(BF16)

        def down(ns):
            yd = mm(g_s[hr, :], wdn_s[:, ns]).astype(BF16)
            d_s[hr, ns] = (h_s[l, hr, ns].astype(F32) + yd.astype(F32)).astype(BF16)

        def step(cost, fn, *args):
            steps.append((cost, functools.partial(fn, *args)))

        for rs in sub_rows(h, 64):
            step(60, start, rs)
        for ns in col_blocks(3 * dm):
            step(120, qkv, ns)
        pairs = [(h * hseq + s, j) for s in range(hseq) for j in range(n_pair)]
        for t in range(len(pairs) + 3):
            if t < len(pairs):
                step(40, scores, *pairs[t])
            if 1 <= t <= len(pairs):
                step(70, soft, *pairs[t - 1])
            if t >= 3:
                step(50, mix, *pairs[t - 3])
        for ns in [slice(0, dm)]:
            step(100, out, ns)
        for rs in sub_rows(h, 64):
            step(70, norm2, rs)
        cols = col_blocks(ff)
        step(100, up, cols[0])
        for i, ns in enumerate(cols):
            if i + 1 < len(cols):
                step(120, up, cols[i + 1])
            for rs in sub_rows(h, 64):
                step(38, gelu, rs, ns)
        for ns in [slice(0, dm)]:
            step(380, down, ns)
        return steps

    def fwd(l, carry):
        tl = ff // n_layers
        ts = pl.ds(pl.multiple_of(l * tl, tl), tl)

        def wt():
            wupt_s[ts, :] = wup_s[:, ts].T
            wdnt_s[:, ts] = wdn_s[ts, :].T

        merge((0, fwd_half(l, 0)), (700, fwd_half(l, 1)), (2500, [(1, wt)]))
        return carry

    lax.fori_loop(0, n_layers, fwd, 0)
    loads[-1].wait()
    d_s[...] = dmid_s[0]

    def gelu_phase(l, after, lag=1):
        def dact(i):
            n0, nn = fb[i]
            da_s[i % 2] = mm(d_s[...], wdnt_s[:, n0:n0 + nn]).astype(BF16)

        def gelu_back(i):
            n0, nn = fb[i]
            ns = slice(n0, n0 + nn)
            for r_0, rn in blocks(tok, 32):
                rs = slice(r_0, r_0 + rn)
                z = z_s[l, rs, ns].astype(F32)
                z2 = z * z
                cdf = 0.5 + 0.5 * jnp.tanh(z * (GC0 + GC1 * z2))
                g = z * cdf
                g_s[rs, ns] = g.astype(BF16)
                dg = cdf + (g * (1.0 - cdf)) * (2.0 * GC0 + 6.0 * GC1 * z2)
                z_s[l, rs, ns] = (da_s[i % 2, rs, :].astype(F32) * dg).astype(BF16)

        def wg_down(i):
            n0, nn = fb[i]
            res = mmg(g_s[:, n0:n0 + nn], d_s[...], TN)
            for t in range(0, nn, 128):
                r = n0 + t
                acc[r // dm, r % dm:r % dm + 128, :] += res[t:t + 128]

        dact(0)
        for i in range(len(fb)):
            if i + 1 < len(fb):
                dact(i + 1)
            gelu_back(i)
            if i >= lag:
                wg_down(i - lag)
                after(i - lag)
        for i in range(len(fb) - lag, len(fb)):
            wg_down(i)
            after(i)

    def mid_phase(l):
        for n0, nn in blocks(dm, dm):
            ns = slice(n0, n0 + nn)
            dn_s[:, ns] = mm(z_s[l], wupt_s[:, ns]).astype(BF16)
        for r_0, rn in blocks(tok, 32):
            rs = slice(r_0, r_0 + rn)
            hf = h_s[l, rs, :].astype(F32)
            r = rms_scale(hf)
            dh = norm_back(hf, r, dn_s[rs, :].astype(F32)).astype(BF16)
            h_s[l, rs, :] = (hf * r).astype(BF16)
            dmid_s[l, rs, :] = (d_s[rs, :].astype(F32) + dh.astype(F32)).astype(BF16)

    def attn_phase(l):
        for n0, nn in blocks(dm, dm):
            ns = slice(n0, n0 + nn)
            dn_s[:tok // 2, ns] = mm(dmid_s[l, :tok // 2], wot_s[:, ns]).astype(BF16)
        for n0, nn in blocks(dm, dm):
            ns = slice(n0, n0 + nn)
            dn_s[tok // 2:, ns] = mm(dmid_s[l, tok // 2:], wot_s[:, ns]).astype(BF16)

        def dprob(s, j):
            rs = seq_rows(s)
            cc = j * pw
            v = stack(qkv_s[l, rs, 2 * dm + cc:2 * dm + cc + pw])
            st_s[s * n_pair + j] = mmg(v, dn_s[rs, cc:cc + pw], NT).astype(BF16)

        def dscore(s, j):
            i = s * n_pair + j
            for hh in range(2):
                hs = slice(hh * seq, (hh + 1) * seq)
                pf = p_s[l, i, hs, :]
                dp = st_s[i, hs, :].astype(F32)
                inner = jnp.sum(pf * dp, axis=0, keepdims=True)
                st_s[i, hs, :] = (pf * (dp - inner) * scale).astype(BF16)

        def dqkv(s, j):
            rs = seq_rows(s)
            i = s * n_pair + j
            cc = j * pw
            dst = st_s[i]
            q = stack(qkv_s[l, rs, cc:cc + pw])
            k = stack(qkv_s[l, rs, dm + cc:dm + cc + pw])
            dmx = stack(dn_s[rs, cc:cc + pw])
            qkv_s[l, rs, cc:cc + pw] = mmg(dst, k, TN).astype(BF16)
            qkv_s[l, rs, dm + cc:dm + cc + pw] = mm(beside(dst), q).astype(BF16)
            pb = p_s[l, i].astype(BF16)
            qkv_s[l, rs, 2 * dm + cc:2 * dm + cc + pw] = mm(beside(pb), dmx).astype(BF16)

        pairs = [(s, j) for s in range(n_seq) for j in range(n_pair)]
        for t in range(len(pairs) + 4):
            if t < len(pairs):
                dprob(*pairs[t])
            if 1 <= t < len(pairs) + 1:
                dscore(*pairs[t - 1])
            if t >= 4:
                dqkv(*pairs[t - 4])

    def in_phase(l):
        for n0, nn in blocks(dm, dm):
            ns = slice(n0, n0 + nn)
            dn_s[:tok // 2, ns] = mm(qkv_s[l, :tok // 2], wqkvt_s[:, ns]).astype(BF16)
        for n0, nn in blocks(dm, dm):
            ns = slice(n0, n0 + nn)
            dn_s[tok // 2:, ns] = mm(qkv_s[l, tok // 2:], wqkvt_s[:, ns]).astype(BF16)
        for r_0, rn in blocks(tok, 32):
            rs = slice(r_0, r_0 + rn)
            xf = x_s[l, rs, :].astype(F32)
            r = rms_scale(xf)
            dh = norm_back(xf, r, dn_s[rs, :].astype(F32)).astype(BF16)
            x_s[l, rs, :] = (xf * r).astype(BF16)
            d_s[rs, :] = (dmid_s[l, rs, :].astype(F32) + dh.astype(F32)).astype(BF16)

    def bwd_body(i, carry):
        l = n_layers - 1 - i
        gelu_phase(l, lambda n: None)
        mid_phase(l)
        attn_phase(l)
        in_phase(l)
        return carry

    lax.fori_loop(0, n_layers - 1, bwd_body, 0)
    pl.semaphore_wait(barrier, 3)

    h0, h1, h2, h3 = dm // 2, dm // 4, dm // 8, dm // 16
    own = c * h0
    oth = (1 - c) * h0
    a0, a0n = own + x * h2, own + (1 - x) * h2
    b0, b0n = own + h1 + y * h2, own + h1 + (1 - y) * h2
    a1, a1n = a0 + y * h3, a0 + (1 - y) * h3
    b1, b1n = b0 + x * h3, b0 + (1 - x) * h3

    def part(k, off, n):
        return acc.at[k, pl.ds(pl.multiple_of(off, 8), n), :]

    def send(j, src, dst, dev):
        def at(k):
            return pltpu.make_async_remote_copy(
                src_ref=src(k), dst_ref=dst(k), send_sem=ssem.at[j, k], recv_sem=rsem.at[j, k],
                device_id=(dev,), device_id_type=MESH)
        return at

    def rows_of(off, n):
        return lambda k: part(k, off, n)

    def slot(ref, n):
        return lambda k: ref.at[k, 0:n, :]

    cs = [
        send(0, rows_of(oth, h0), slot(r0, h0), cp),
        send(1, rows_of(a0n, h2), slot(ra, h2), xp),
        send(2, rows_of(b0n, h2), slot(rb, h2), yp),
        send(3, rows_of(a1n, h3), slot(ra2, h3), yp),
        send(4, rows_of(b1n, h3), slot(rb2, h3), xp),
        send(5, rows_of(a1, h3), slot(ra, h3), yp),
        send(6, rows_of(b1, h3), slot(rb, h3), xp),
        send(7, rows_of(a1, h3), rows_of(a1, h3), xp),
        send(8, rows_of(b1, h3), rows_of(b1, h3), yp),
        send(9, slot(ra, h3), rows_of(a1n, h3), xp),
        send(10, slot(rb, h3), rows_of(b1n, h3), yp),
        send(11, rows_of(own, h0), rows_of(own, h0), cp),
    ]

    def add(k, off, n, src):
        sl = pl.ds(pl.multiple_of(off, 8), n)
        acc[k, sl, :] = acc[k, sl, :] + src[k]

    def loop(fn, lo=0, hi=n_chunk):
        lax.fori_loop(lo, hi, lambda k, t: (fn(k), t)[1], 0)

    def s0(k):
        cs[0](k).start()

    def s1(k):
        cs[0](k).wait_recv()
        add(k, own, h0, r0)
        cs[1](k).start()
        cs[2](k).start()

    def s2(k):
        cs[1](k).wait()
        add(k, a0, h2, ra)
        cs[2](k).wait()
        add(k, b0, h2, rb)
        cs[3](k).start()
        cs[4](k).start()

    def g2(k, both=True):
        cs[3](k).wait_recv()
        add(k, a1, h3, ra2)
        cs[4](k).wait_recv()
        add(k, b1, h3, rb2)
        for j in (5, 6, 7, 8) if both else (5, 6):
            cs[j](k).start()

    def g2_own(k):
        cs[7](k).start()
        cs[8](k).start()

    def g1(k):
        cs[5](k).wait_recv()
        cs[9](k).start()
        cs[6](k).wait_recv()
        cs[10](k).start()
        cs[3](k).wait_send()
        acc[k, pl.ds(pl.multiple_of(a1n, 8), h3), :] = ra[k, 0:h3, :]
        cs[4](k).wait_send()
        acc[k, pl.ds(pl.multiple_of(b1n, 8), h3), :] = rb[k, 0:h3, :]

    def g0(k):
        for j in (7, 8, 9, 10):
            cs[j](k).wait_recv()
        cs[11](k).start()

    def finish(k):
        cs[11](k).wait_recv()
        for j in range(5, 12):
            cs[j](k).wait_send()

    first = n_layers - 1

    def put(l, k, sl, val):
        if l == first:
            acc[(k, *sl)] = val
        else:
            acc[(k, *sl)] += val

    def wg_up(l, m):
        for n0, nn in fb:
            res = mmg(m, z_s[l, :, n0:n0 + nn], TN)
            for t in range(0, nn, 128):
                r = n0 + t
                put(l, n_dn + r // dm, (slice(None), slice(r % dm, r % dm + 128)), res[:, t:t + 128])

    def wg_o(l):
        put(l, k_o, (slice(None), slice(None)), mmg(mix_s[l], dmid_s[l], TN))

    def wg_qkv(l):
        for i in range(3):
            put(l, k_q + i, (slice(None), slice(None)), mmg(qkv_s[l, :, i * dm:(i + 1) * dm], x_s[l], TN))

    def after(i):
        done = min((i + 1) * BLOCK // dm, n_dn)
        prev = i * BLOCK // dm
        for k in range(prev, done):
            s0(k)
        if i == len(fb) - 1:
            s1(0)

    gelu_phase(0, after, 0)
    for r_0, rn in rows:
        rs = slice(r_0, r_0 + rn)
        hf = h_s[0, rs, :].astype(F32)
        u_s[rs, :] = (hf * rms_scale(hf)).astype(BF16)
    s1(1)
    order = list(range(first, -1, -1))
    for i, l in enumerate(order):
        wg_up(l, h_s[l] if l else u_s[...])
        if i == 0:
            loop(s1, 2, n_dn)
        if i >= 3:
            loop(s2, i - 3, i - 2)
    loop(s0, n_dn, 2 * n_dn)
    loop(s2, 3, n_dn)
    mid_phase(0)
    loop(s1, n_dn, 2 * n_dn)
    attn_phase(0)
    loop(g2, 0, n_dn)
    in_phase(0)
    dx_ref[...] = d_s[...]
    loop(s2, n_dn, 2 * n_dn)
    for l in order:
        wg_o(l)
    loop(s0, k_o, k_o + 1)
    loop(g1, 0, n_dn)
    for i, l in enumerate(order):
        wg_qkv(l)
        if i == 1:
            loop(s1, k_o, k_o + 1)
        if i == 3:
            loop(g2, n_dn, 2 * n_dn)
    loop(s0, k_q, n_chunk)
    loop(s1, k_q, n_chunk)
    loop(lambda k: cs[0](k).wait_send())
    pl.semaphore_signal(free_sem, inc=1, device_id=(cp,), device_id_type=MESH)
    loop(g1, n_dn, 2 * n_dn)
    loop(s2, 2 * n_dn, n_chunk)
    pl.semaphore_wait(free_sem, 1)
    loop(g0, 0, n_dn)
    loop(lambda k: g2(k, False), 2 * n_dn, n_chunk)
    loop(g2_own, 2 * n_dn, n_chunk)
    loop(g0, n_dn, 2 * n_dn)
    loop(g1, 2 * n_dn, n_chunk)
    loop(g0, 2 * n_dn, n_chunk)
    loop(finish)


def store_kernel(acc, dx_ref, oq, ok, ov, oo, oup, odn, odx, sem):
    dm = acc.shape[1]
    n = odn.shape[0] // dm
    dst = ([odn.at[i * dm:(i + 1) * dm, :] for i in range(n)]
           + [oup.at[:, i * dm:(i + 1) * dm] for i in range(n)] + [oo, oq, ok, ov])
    cps = [pltpu.make_async_copy(acc.at[i], d, sem.at[i]) for i, d in enumerate(dst)]
    cps.append(pltpu.make_async_copy(dx_ref, odx, sem.at[len(dst)]))
    for cc in cps:
        cc.start()
    for cc in cps:
        cc.wait()


def solution(mesh):
    batch_spec = P('data', None, None)

    def per_device(x_loc, g_loc, step_emb, w_q, w_k, w_v, w_o, w_up, w_down):
        n_seq, seq, dm = x_loc.shape
        n_layers = step_emb.shape[0]
        n_heads, hd = w_q.shape[1:]
        ff = w_up.shape[1]
        tok = n_seq * seq
        n_pair = n_heads // 2
        n_chunk = 4 + 2 * (ff // dm)
        wts = [w.transpose(1, 2, 0).reshape(n_heads * hd, dm) for w in (w_q, w_k, w_v)]
        vm = pl.BlockSpec(memory_space=pltpu.VMEM)
        hb = pl.BlockSpec(memory_space=pl.ANY)
        acc, dx = pl.pallas_call(
            functools.partial(block_kernel, n_seq, seq, n_layers, n_heads),
            out_shape=(pltpu.VMEM((n_chunk, dm, dm), F32), pltpu.VMEM((tok, dm), BF16)),
            in_specs=[hb] * 9,
            out_specs=[vm] * 2,
            scratch_shapes=[
                pltpu.VMEM((dm, 3 * dm), BF16),
                pltpu.VMEM((3 * dm, dm), BF16),
                pltpu.VMEM((dm, dm), BF16),
                pltpu.VMEM((dm, dm), BF16),
                pltpu.VMEM((dm, ff), BF16),
                pltpu.VMEM((ff, dm), BF16),
                pltpu.VMEM((ff, dm), BF16),
                pltpu.VMEM((dm, ff), BF16),
                pltpu.VMEM((n_layers, 1, dm), F32),
                pltpu.VMEM((n_layers, dm), BF16),
                pltpu.VMEM((n_layers, tok, dm), BF16),
                pltpu.VMEM((n_layers, tok, 3 * dm), BF16),
                pltpu.VMEM((n_layers, n_seq * n_pair, 2 * seq, seq), F32),
                pltpu.VMEM((n_layers, tok, dm), BF16),
                pltpu.VMEM((n_layers, tok, dm), BF16),
                pltpu.VMEM((n_layers, tok, ff), BF16),
                pltpu.VMEM((tok, dm), BF16),
                pltpu.VMEM((tok, ff), BF16),
                pltpu.VMEM((2, tok, BLOCK), BF16),
                pltpu.VMEM((tok, dm), BF16),
                pltpu.VMEM((tok, dm), BF16),
                pltpu.VMEM((n_layers, tok, dm), BF16),
                pltpu.VMEM((n_seq * n_pair, 2 * seq, seq), BF16),
                pltpu.VMEM((n_chunk, dm // 2, dm), F32),
                pltpu.VMEM((n_chunk, dm // 8, dm), F32),
                pltpu.VMEM((n_chunk, dm // 8, dm), F32),
                pltpu.VMEM((n_chunk, dm // 16, dm), F32),
                pltpu.VMEM((n_chunk, dm // 16, dm), F32),
                pltpu.SemaphoreType.DMA((9,)),
                pltpu.SemaphoreType.DMA((12, n_chunk)),
                pltpu.SemaphoreType.DMA((12, n_chunk)),
                pltpu.SemaphoreType.REGULAR,
            ],
            compiler_params=pltpu.CompilerParams(
                collective_id=0, has_side_effects=True, vmem_limit_bytes=VMEM_LIMIT),
        )(x_loc.reshape(tok, dm), g_loc.reshape(tok, dm), step_emb,
          *wts, w_o.reshape(n_heads * hd, dm), w_up, w_down)
        sq = jax.ShapeDtypeStruct((dm, dm), F32)
        gq, gk, gv, go, gup, gdn, gx = pl.pallas_call(
            store_kernel,
            out_shape=(sq, sq, sq, sq, jax.ShapeDtypeStruct((dm, ff), F32), jax.ShapeDtypeStruct((ff, dm), F32),
                       jax.ShapeDtypeStruct((tok, dm), BF16)),
            in_specs=[vm] * 2,
            out_specs=[hb] * 7,
            scratch_shapes=[pltpu.SemaphoreType.DMA((n_chunk + 1,))],
            compiler_params=pltpu.CompilerParams(vmem_limit_bytes=2 ** 20),
        )(acc, dx)
        heads = [a.reshape(n_heads, hd, dm).transpose(2, 0, 1) for a in (gq, gk, gv)]
        return (*heads, go.reshape(n_heads, hd, dm), gup, gdn, gx.reshape(n_seq, seq, dm))

    return jax.shard_map(per_device, mesh=mesh, in_specs=(batch_spec, batch_spec, P(), P(), P(), P(), P(), P(), P()), out_specs=(P(), P(), P(), P(), P(), P(), batch_spec), check_vma=False)
```
